64 devices in a mesh: data: 4 (over x, y), expert: 16 (over z, core).
Axes of the slice: x: 2, y: 2, z: 8, core: 2. Of those that a mesh axis runs over, the one named last changes fastest.
The devices are a block of a 4x4x8 slice.
Arguments:
- x_in: bfloat16 [8192, 1024], P(('data', 'expert')), parts along dimension 0
- expert_idx: int32 [8192, 8], P(('data', 'expert')), parts along dimension 0
- gate_weight: float32 [8192, 8], P(('data', 'expert')), parts along dimension 0
- grad_y: bfloat16 [8192, 1024], P(('data', 'expert')), parts along dimension 0
- w_in: bfloat16 [64, 1024, 512], P('expert')
- w_out: bfloat16 [64, 512, 1024], P('expert')
Outputs:
- output 1: bfloat16 [8192, 1024], P(('data', 'expert')), parts along dimension 0
- output 2: bfloat16 [8192, 1024], P(('data', 'expert')), parts along dimension 0
- output 3: float32 [8192, 8], P(('data', 'expert')), parts along dimension 0
- output 4: bfloat16 [256, 1024, 512], P(('data', 'expert')), parts along dimension 0
- output 5: bfloat16 [256, 512, 1024], P(('data', 'expert')), parts along dimension 0
There are 4 independent parts. The reference program is written for one: setup_inputs(seed, part) draws one part's arguments, and reference() takes and returns one part's arrays. A program takes and returns all parts, laid end to end along the dimension named above; an argument that names none is the same for every part.
All inputs are finite; a program needn't handle non-finite values.
Results may differ from the reference program's by a relative error of at most 0.0100943.
Values are sent between devices in bfloat16 or wider.
A program may use at most 768 MiB of HBM per device.

```python
import jax
import jax.numpy as jnp
from jax import lax

TOKENS = 128
GROUP_SIZE = 16
D_MODEL = 1024
D_FF = 512
EXPERTS = 64
TOP_K = 8
CAPACITY = 320

LOCAL_EXPERTS = EXPERTS // GROUP_SIZE
DEVICE_PAIRS = TOKENS * TOP_K
FAIR_SHARE = DEVICE_PAIRS // GROUP_SIZE
GROUP_ROWS = GROUP_SIZE * TOKENS
GROUP_PAIRS = GROUP_ROWS * TOP_K


def route_device(rng_key, hot_offset):
    key_perm, key_shift, key_quartet, key_pick, key_shuffle = jax.random.split(rng_key, 5)
    owner_perm = jax.random.permutation(key_perm, GROUP_SIZE)
    shift_size = jax.random.randint(key_shift, (GROUP_SIZE // 2,), 0, FAIR_SHARE + 1)
    shift_size = shift_size.at[0].set(FAIR_SHARE)
    per_owner = jnp.full((GROUP_SIZE,), FAIR_SHARE, jnp.int32)
    per_owner = per_owner.at[owner_perm[0::2]].add(shift_size).at[owner_perm[1::2]].add(-shift_size)
    owner_dev = jnp.searchsorted(jnp.cumsum(per_owner), jnp.arange(DEVICE_PAIRS, dtype=jnp.int32), side='right')
    quartet = jax.random.randint(key_quartet, (DEVICE_PAIRS,), 0, LOCAL_EXPERTS // 4)
    pick_draw = jax.random.randint(key_pick, (DEVICE_PAIRS,), 0, 8)
    hot_slot = hot_offset[owner_dev, quartet]
    within = jnp.where(pick_draw < 5, hot_slot, (hot_slot + pick_draw - 4) % 4)
    expert_id = owner_dev * LOCAL_EXPERTS + quartet * 4 + within
    return expert_id[jax.random.permutation(key_shuffle, DEVICE_PAIRS)].astype(jnp.int32)


def setup_inputs(seed: int = 0, part: int = 0) -> dict:
    part_key = jax.random.fold_in(jax.random.key(seed), part)
    key_x, key_gate, key_dy, key_hot, key_route = jax.random.split(part_key, 5)
    key_in, key_out = jax.random.split(jax.random.key(seed + 1), 2)
    hot_offset = jax.random.randint(key_hot, (GROUP_SIZE, LOCAL_EXPERTS // 4), 0, 4)
    route_keys = jax.random.split(key_route, GROUP_SIZE)
    expert_idx = jax.vmap(route_device, in_axes=(0, None))(route_keys, hot_offset).reshape(GROUP_ROWS, TOP_K)
    x_in = jax.random.normal(key_x, (GROUP_ROWS, D_MODEL), jnp.float32).astype(jnp.bfloat16)
    gate_weight = jax.random.uniform(key_gate, (GROUP_ROWS, TOP_K), jnp.float32, 0.5, 1.5) * TOP_K ** -0.5
    grad_y = jax.random.normal(key_dy, (GROUP_ROWS, D_MODEL), jnp.float32).astype(jnp.bfloat16)
    w_in = (jax.random.normal(key_in, (EXPERTS, D_MODEL, D_FF), jnp.float32) * D_MODEL ** -0.5).astype(jnp.bfloat16)
    w_out = (jax.random.normal(key_out, (EXPERTS, D_FF, D_MODEL), jnp.float32) * D_FF ** -0.5).astype(jnp.bfloat16)
    return {'x_in': x_in, 'expert_idx': expert_idx, 'gate_weight': gate_weight, 'grad_y': grad_y, 'w_in': w_in, 'w_out': w_out}


def reference(x_in, expert_idx, gate_weight, grad_y, w_in, w_out):
    flat_idx = expert_idx.reshape(GROUP_PAIRS)
    pair_ids = jnp.arange(GROUP_PAIRS, dtype=jnp.int32)
    sort_order = jnp.argsort(flat_idx, stable=True)
    counts = jnp.zeros((EXPERTS,), jnp.int32).at[flat_idx].add(1)
    starts = jnp.cumsum(counts) - counts
    sorted_rank = pair_ids - starts[flat_idx[sort_order]]
    pair_slot = jnp.zeros((GROUP_PAIRS,), jnp.int32).at[sort_order].set(sorted_rank)
    dest_row = jnp.where(pair_slot < CAPACITY, flat_idx * CAPACITY + pair_slot, EXPERTS * CAPACITY)
    source_pair = jnp.full((EXPERTS * CAPACITY,), GROUP_PAIRS, jnp.int32).at[dest_row].set(pair_ids, mode='drop')
    exp_rows = jnp.take(x_in, source_pair // TOP_K, axis=0, mode='fill', fill_value=0).reshape(EXPERTS, CAPACITY, D_MODEL)
    scaled_grad = (gate_weight[:, :, None] * grad_y[:, None, :].astype(jnp.float32)).astype(jnp.bfloat16).reshape(GROUP_PAIRS, D_MODEL)
    grad_rows = jnp.take(scaled_grad, source_pair, axis=0, mode='fill', fill_value=0).reshape(EXPERTS, CAPACITY, D_MODEL)

    def expert_pass(operands):
        rows_in, rows_grad, weight_in, weight_out = operands
        pre_act = jnp.dot(rows_in, weight_in, preferred_element_type=jnp.float32)
        act_full, gelu_pull = jax.vjp(jax.nn.gelu, pre_act)
        act_bf = act_full.astype(jnp.bfloat16)
        rows_out = jnp.dot(act_bf, weight_out, preferred_element_type=jnp.float32).astype(jnp.bfloat16)
        grad_act = jnp.dot(rows_grad, weight_out.T, preferred_element_type=jnp.float32).astype(jnp.bfloat16)
        grad_pre = gelu_pull(grad_act.astype(jnp.float32))[0].astype(jnp.bfloat16)
        grad_weight_out = jnp.dot(act_bf.T, rows_grad, preferred_element_type=jnp.float32).astype(jnp.bfloat16)
        grad_weight_in = jnp.dot(rows_in.T, grad_pre, preferred_element_type=jnp.float32).astype(jnp.bfloat16)
        grad_in = jnp.dot(grad_pre, weight_in.T, preferred_element_type=jnp.float32).astype(jnp.bfloat16)
        return rows_out, grad_in, grad_weight_in, grad_weight_out

    out_rows, grad_in_rows, grad_w_in, grad_w_out = lax.map(expert_pass, (exp_rows, grad_rows, w_in, w_out))
    out_pair = jnp.take(out_rows.reshape(EXPERTS * CAPACITY, D_MODEL), dest_row, axis=0, mode='fill', fill_value=0).reshape(GROUP_ROWS, TOP_K, D_MODEL).astype(jnp.float32)
    grad_pair = jnp.take(grad_in_rows.reshape(EXPERTS * CAPACITY, D_MODEL), dest_row, axis=0, mode='fill', fill_value=0).reshape(GROUP_ROWS, TOP_K, D_MODEL).astype(jnp.float32)
    y_out = (x_in.astype(jnp.float32) + jnp.sum(gate_weight[:, :, None] * out_pair, axis=1)).astype(jnp.bfloat16)
    grad_gate = jnp.sum(grad_y.astype(jnp.float32)[:, None, :] * out_pair, axis=2)
    grad_x = (grad_y.astype(jnp.float32) + jnp.sum(grad_pair, axis=1)).astype(jnp.bfloat16)
    return y_out, grad_x, grad_gate, grad_w_in, grad_w_out
```

```python
import jax
import jax.numpy as jnp
from jax import lax
from jax.sharding import PartitionSpec as P

CAP_NUM = 5
CAP_DEN = 4
BIG = 3.3e38
F32 = jnp.float32
BF16 = jnp.bfloat16
K0 = 0.7978845608028654
K1 = 0.044715


def split3(v):
    hi = jnp.clip(v, -BIG, BIG).astype(BF16)
    rest = v - hi.astype(F32)
    mid = rest.astype(BF16)
    lo = (rest - mid.astype(F32)).astype(BF16)
    return hi, mid, lo


def gelu_and_slope(a):
    t = jnp.tanh(K0 * (a + K1 * (a * a * a)))
    cdf = 0.5 * (1.0 + t)
    return a * cdf, cdf + a * (0.5 * (1.0 - t * t)) * (K0 * (1.0 + 3.0 * K1 * (a * a)))


def solution(mesh):
    groups = mesh.shape['expert']
    tok_spec = P(('data', 'expert'), None)
    weight_spec = P('expert', None, None)
    grad_spec = P(('data', 'expert'), None, None)

    def device_pass(x_in, expert_idx, gate_weight, grad_y, w_in, w_out):
        n_tokens, top_k = expert_idx.shape
        local_experts, d_model = w_in.shape[0], w_in.shape[1]
        num_experts = local_experts * groups
        n_pairs = n_tokens * top_k
        capacity = (CAP_NUM * n_pairs * groups) // (CAP_DEN * num_experts)
        rows = groups * n_tokens
        me = lax.axis_index('expert')
        idx = lax.all_gather(expert_idx, 'expert', tiled=True)
        gate = lax.all_gather(gate_weight, 'expert', tiled=True)
        x_all = lax.all_gather(x_in, 'expert', tiled=True)
        dy_all = lax.all_gather(grad_y, 'expert', tiled=True)
        local = idx - me * local_experts
        match = (local[:, None, :] == jnp.arange(local_experts)[None, :, None]).astype(F32)
        cnt = jnp.sum(match, axis=2)
        blocks = cnt.reshape(groups, n_tokens, local_experts)
        tri = (jnp.arange(n_tokens)[:, None] > jnp.arange(n_tokens)[None, :]).astype(BF16)
        within = jnp.einsum('tu,sue->ste', tri, blocks.astype(BF16), preferred_element_type=F32)
        totals = jnp.sum(blocks, axis=1)
        tri_g = (jnp.arange(groups)[:, None] > jnp.arange(groups)[None, :]).astype(F32)
        base = jnp.sum(tri_g[:, :, None] * totals[None], axis=1)
        start = (within + base[:, None, :]).reshape(rows, local_experts)
        tri_k = (jnp.arange(top_k)[:, None] > jnp.arange(top_k)[None, :]).astype(F32)
        before_j = jnp.sum(tri_k[None, None] * match[:, :, None, :], axis=3)
        row_of = jnp.sum(match * (start[:, :, None] + before_j), axis=1)
        slot_ids = jnp.arange(capacity, dtype=F32)[None, :, None]
        pick = ((slot_ids >= start.T[:, None, :]) & (slot_ids < (start + cnt).T[:, None, :])).astype(BF16)
        mine = jnp.sum(match, axis=1) > 0
        kept = mine & (row_of < capacity)
        slot_code = jnp.where(kept, row_of - capacity // 2, 255.0).astype(BF16)
        exp_code = jnp.where(kept, local, 255).astype(BF16)
        hi, mid, lo = split3(gate)
        table = jnp.concatenate([hi, mid, lo, slot_code, exp_code], axis=1)
        feat = jnp.einsum('ert,tf->erf', pick, table, preferred_element_type=F32)
        f_hi, f_mid, f_lo, f_slot, f_exp = jnp.split(feat, 5, axis=2)
        is_pair = (f_slot == (jnp.arange(capacity) - capacity // 2).astype(F32)[None, :, None]) & (
            f_exp == jnp.arange(local_experts, dtype=F32)[:, None, None])
        filled = jnp.sum(pick.astype(F32), axis=2, keepdims=True) > 0
        is_pair = is_pair & filled
        g_row = jnp.sum(jnp.where(is_pair, f_hi + f_mid + f_lo, 0.0), axis=2, keepdims=True)
        exp_rows = jnp.einsum('ert,td->erd', pick, x_all, preferred_element_type=F32).astype(BF16)
        pre_act = jnp.einsum('lcd,ldf->lcf', exp_rows, w_in, preferred_element_type=F32)
        act, slope = gelu_and_slope(pre_act)
        act_bf = act.astype(BF16)
        out_rows = jnp.einsum('lcf,lfd->lcd', act_bf, w_out, preferred_element_type=F32).astype(BF16)
        g3 = split3(g_row)
        part_y = sum(jnp.einsum('ert,erd->td', pick * g, out_rows, preferred_element_type=F32) for g in g3)
        y_out = (x_in.astype(F32) + lax.psum_scatter(part_y, 'expert', tiled=True)).astype(BF16)
        dy_rows = jnp.einsum('ert,td->erd', pick, dy_all, preferred_element_type=F32)
        dg_row = jnp.sum(dy_rows * out_rows.astype(F32), axis=2, keepdims=True)
        dg3 = split3(jnp.where(is_pair, dg_row, 0.0))
        part_g = sum(jnp.einsum('ert,erj->tj', pick, d, preferred_element_type=F32) for d in dg3)
        grad_gate = lax.psum_scatter(part_g, 'expert', tiled=True)
        grad_rows = (g_row * dy_rows).astype(BF16)
        grad_act = jnp.einsum('lcd,lfd->lcf', grad_rows, w_out, preferred_element_type=F32).astype(BF16)
        grad_pre = (grad_act.astype(F32) * slope).astype(BF16)
        grad_w_out = jnp.einsum('lcf,lcd->lfd', act_bf, grad_rows, preferred_element_type=F32).astype(BF16)
        grad_w_in = jnp.einsum('lcd,lcf->ldf', exp_rows, grad_pre, preferred_element_type=F32).astype(BF16)
        grad_in = jnp.einsum('lcf,ldf->lcd', grad_pre, w_in, preferred_element_type=F32).astype(BF16)
        part_x = jnp.einsum('ert,erd->td', pick, grad_in, preferred_element_type=F32)
        grad_x = (grad_y.astype(F32) + lax.psum_scatter(part_x, 'expert', tiled=True)).astype(BF16)
        return y_out, grad_x, grad_gate, grad_w_in, grad_w_out

    return jax.shard_map(device_pass, mesh=mesh,
                         in_specs=(tok_spec, tok_spec, tok_spec, tok_spec, weight_spec, weight_spec),
                         out_specs=(tok_spec, tok_spec, tok_spec, grad_spec, grad_spec), check_vma=False)
```

```python
import functools

import jax
import jax.numpy as jnp
from jax import lax
from jax.experimental import pallas as pl
from jax.experimental.pallas import tpu as pltpu
from jax.sharding import PartitionSpec as P

CAP_NUM = 5
CAP_DEN = 4
BIG = 3.3e38
F32 = jnp.float32
BF16 = jnp.bfloat16
K0 = 0.7978845608028654
K1 = 0.044715
MESH = pl.DeviceIdType.MESH
VMEM_BYTES = 67_000_000


def split3(v):
    hi = jnp.clip(v, -BIG, BIG).astype(BF16).astype(F32)
    rest = v - hi
    mid = rest.astype(BF16).astype(F32)
    lo = (rest - mid).astype(BF16).astype(F32)
    return hi, mid, lo


def gelu_and_slope(a):
    t = jnp.tanh(K0 * (a + K1 * (a * a * a)))
    cdf = 0.5 * (1.0 + t)
    return a * cdf, cdf + a * (0.5 * (1.0 - t * t)) * (K0 * (1.0 + 3.0 * K1 * (a * a)))


def dot_nn(a, b):
    return lax.dot_general(a, b, (((1,), (0,)), ((), ())), preferred_element_type=F32)


def dot_nt(a, b):
    return lax.dot_general(a, b, (((1,), (1,)), ((), ())), preferred_element_type=F32)


def dot_tn(a, b):
    return lax.dot_general(a, b, (((0,), (0,)), ((), ())), preferred_element_type=F32)


def moe_kernel(chips, cap, n_exp,
               info, x_in, dy_in, w1_hbm, w2_hbm,
               y_out, dx_out, dg_out, dw1_hbm, dw2_hbm,
               info_all, xa, dya, vt, cnt, tab, bfeat, grow, brow, gy, hid, slope, orow, dact, lhs,
               part, sib, ring, mg, dgp, dgs, dgr, w1, w2,
               ag_s, ag_r, agb_s, agb_r, in_s, in_r, inb_s, inb_r, rs_s, rs_r, rsb_s, rsb_r,
               dg_s, dg_r, dgb_s, dgb_r, w_sem, o_sem):
    top_k = info.shape[0] // 2
    tok = info.shape[1]
    half = tok // 2
    rows = n_exp * cap
    me = lax.axis_index('expert')
    z = me // 2
    c = me % 2
    far = chips // 2

    def chip(d):
        return (z + d + chips) % chips

    def dev(q, k):
        return {'expert': q * 2 + k}

    right, left, twin = dev(chip(1), c), dev(chip(-1), c), {'expert': z * 2 + 1 - c}
    side = (right, left)
    pending = []

    def rcopy(src, dst, ss, rs, to):
        return pltpu.make_async_remote_copy(src_ref=src, dst_ref=dst, send_sem=ss, recv_sem=rs,
                                            device_id=to, device_id_type=MESH)

    def send(src, dst, ss, rs, to):
        cp = rcopy(src, dst, ss, rs, to)
        cp.start()
        return cp

    def landed(dst, ss, rs, to):
        rcopy(dst, dst, ss, rs, to).wait_recv()

    loads = []
    for e in range(n_exp):
        for k, (src, dst) in enumerate(((w1_hbm, w1), (w2_hbm, w2))):
            cp = pltpu.make_async_copy(src.at[e], dst.at[e], w_sem.at[k, e])
            cp.start()
            loads.append(cp)

    barrier = pltpu.get_barrier_semaphore()
    for d in range(1, chips):
        pl.semaphore_signal(barrier, inc=1, device_id=dev(chip(d), c), device_id_type=MESH)
    pl.semaphore_signal(barrier, inc=1, device_id=twin, device_id_type=MESH)
    pl.semaphore_wait(barrier, chips)

    bufs = (xa, dya)
    own = (x_in, dy_in)

    def item(k, h):
        return 2 * (k - 1) + h if k < far else 2 * (far - 1)

    def slot(a, q, h, k=None):
        kk = c if k is None else k
        return bufs[a].at[q, pl.ds(pl.multiple_of(kk * tok + h * half, half), half)]

    def twin_send(a, d, h, src):
        di = d % chips
        pending.append(send(src, slot(a, chip(d), h), agb_s.at[a, di, h], agb_r.at[a, di, h], twin))

    def twin_wait(a, d):
        di = d % chips
        for h in range(2):
            landed(slot(a, chip(d), h, 1 - c), agb_s.at[a, di, h], agb_r.at[a, di, h], twin)

    def first_send(a, h):
        src = own[a].at[pl.ds(h * half, half)]
        for r in range(2):
            i = item(1, h)
            pending.append(send(src, slot(a, z, h), ag_s.at[a, r, i], ag_r.at[a, r, i], side[r]))

    def poll(a, k, h, r):
        q = chip(-k) if r == 0 else chip(k)
        i = item(k, h)
        here = slot(a, q, h)
        landed(here, ag_s.at[a, r, i], ag_r.at[a, r, i], side[r])
        if k + 1 < far or (k + 1 == far and h == r):
            j = item(k + 1, h)
            pending.append(send(here, slot(a, q, h), ag_s.at[a, r, j], ag_r.at[a, r, j], side[r]))
        twin_send(a, (-k if r == 0 else k), h, here)

    def poll2(a, k, h):
        if k == far:
            poll(a, k, h, h)
        else:
            poll(a, k, h, 0)
            poll(a, k, h, 1)

    for d in range(1, chips):
        pending.append(send(info, info_all.at[c, z], in_s.at[d], in_r.at[d], dev(chip(d), c)))
    first_send(0, 0)
    first_send(0, 1)
    first_send(1, 0)
    info_all[c, z] = info[...]
    xa[z, pl.ds(pl.multiple_of(c * tok, tok), tok)] = x_in[...]
    dya[z, pl.ds(pl.multiple_of(c * tok, tok), tok)] = dy_in[...]
    for a in range(2):
        for h in range(2):
            twin_send(a, 0, h, own[a].at[pl.ds(h * half, half)])
    for d in range(1, chips):
        landed(info_all.at[c, chip(-d)], in_s.at[d], in_r.at[d], twin)
    pending.append(send(info_all.at[c], info_all.at[c], inb_s.at[0], inb_r.at[0], twin))
    poll2(0, 1, 0)
    landed(info_all.at[1 - c], inb_s.at[0], inb_r.at[0], twin)

    first_e = (me * n_exp).astype(F32)
    sub8 = lax.broadcasted_iota(jnp.int32, (8, tok), 0)

    def count_block(b, carry):
        k, q = b // chips, b % chips
        loc = info_all[k, q, 0:top_k, :] - first_e
        for e in range(n_exp):
            s = jnp.sum(jnp.where(loc == e, 1.0, 0.0), axis=0, keepdims=True)
            cnt[b, e:e + 1, :] = s
            cnt[b, n_exp + e:n_exp + e + 1, :] = s
        return carry

    lax.fori_loop(0, 2 * chips, count_block, 0)
    cmat = cnt[...].reshape(2 * chips * 8, tok)
    ri = lax.broadcasted_iota(jnp.int32, (tok, tok), 0)
    ci = lax.broadcasted_iota(jnp.int32, (tok, tok), 1)
    upper = jnp.where(ri < ci, 1.0, 0.0).astype(BF16)
    rb, cb = ri // 8, ci // 8
    r_ord, c_ord = 2 * (rb % chips) + rb // chips, 2 * (cb % chips) + cb // chips
    prior = jnp.where((c_ord < r_ord) & (ri % 8 == ci % 8), 1.0, 0.0).astype(BF16)
    cbf = cmat.astype(BF16)
    start = dot_nn(cbf, upper) + jnp.sum(dot_nn(prior, cbf), axis=1, keepdims=True)
    cnt[...] = start.reshape(2 * chips, 8, tok)
    row8 = ri % 8
    edge = jnp.where(row8 < n_exp, start, start + cmat)
    edge = jnp.minimum(edge, float(cap)) + (row8 % n_exp).astype(F32) * cap
    vt[...] = edge.reshape(2 * chips, 8, tok)
    poll2(0, 1, 1)

    def table_block(b, carry):
        k, q = b // chips, b % chips
        idx = info_all[k, q, 0:top_k, :]
        loc = idx - first_e
        at = jnp.zeros((top_k, tok), F32)
        for e in range(n_exp):
            at = at + jnp.where(loc == e, cnt[b, e:e + 1, :], 0.0)
        for j in range(top_k - 1):
            at = at + jnp.where((idx[j:j + 1, :] == idx) & (sub8 > j), 1.0, 0.0)
        ok = (loc >= 0.0) & (loc < n_exp) & (at < cap)
        rr = loc * cap + at
        coarse = jnp.floor(rr * 0.125)
        hi, mid, lo = split3(info_all[k, q, top_k:2 * top_k, :])
        code = jnp.where(ok, coarse - rows // 16, 200.0)
        fine = jnp.where(ok, rr - 8.0 * coarse, 0.0)
        tile = jnp.concatenate([hi, mid, lo, code, fine, jnp.zeros((tok - 40, tok), F32)], axis=0)
        tab[q, :, pl.ds(pl.multiple_of(k * tok, tok), tok)] = tile.astype(BF16)
        return carry

    lax.fori_loop(0, 2 * chips, table_block, 0)

    def esl(e):
        return pl.ds(pl.multiple_of(e * cap, cap), cap)

    def pick_rows(q, e):
        r = (lax.broadcasted_iota(jnp.int32, (cap, tok), 0) + e * cap).astype(F32)
        out = []
        for k in range(2):
            b = k * chips + q
            lo = vt[b, pl.ds(e, 1), :]
            hi = vt[b, pl.ds(e + n_exp, 1), :]
            out.append(jnp.where((r >= lo) & (r < hi), 1.0, 0.0).astype(BF16))
        return jnp.concatenate(out, axis=1)

    def gather_step(a, d):
        twin_wait(a, d)
        q = chip(d)
        dst = brow if a == 0 else gy

        def body(e, carry):
            p = pick_rows(q, e)
            g = dot_nn(p, bufs[a][q]).astype(BF16)
            if d == 0:
                dst[esl(e), :] = g
            else:
                dst[esl(e), :] = dst[esl(e), :] + g
            if a == 0:
                f = dot_nt(p, tab[q])
                bfeat[esl(e), :] = f if d == 0 else bfeat[esl(e), :] + f
            return carry

        lax.fori_loop(0, n_exp, body, 0)

    gather_step(0, 0)
    poll2(0, 2, 0)
    gather_step(0, -1)
    poll2(0, 2, 1)
    gather_step(0, 1)
    poll2(0, 3, 0)
    gather_step(0, -2)
    poll2(0, 3, 1)
    first_send(1, 1)
    poll2(1, 1, 0)
    gather_step(0, 2)
    poll2(0, 4, 0)
    poll2(0, 4, 1)
    gather_step(0, -3)
    gather_step(0, 3)
    poll2(1, 1, 1)
    gather_step(0, 4)

    for cp in loads:
        cp.wait()

    def forward(e):
        act, sl = gelu_and_slope(dot_nn(brow[esl(e), :], w1[e]))
        hb = act.astype(BF16)
        hid[esl(e), :] = hb
        slope[esl(e), :] = sl
        orow[esl(e), :] = dot_nn(hb, w2[e]).astype(BF16)

    def forward_pair(e0):
        def body(i, carry):
            forward(e0 + i)
            return carry
        lax.fori_loop(0, 2, body, 0)

    forward_pair(0)
    poll2(1, 2, 0)
    forward_pair(2)

    lane = lax.broadcasted_iota(jnp.int32, (tok, tok), 1)

    def gate_rows(i, carry):
        sl = pl.ds(pl.multiple_of(i * tok, tok), tok)
        f = bfeat[sl, :]
        r = ri + i * tok
        want_c = (r // 8 - rows // 16).astype(F32)
        want_f = (r % 8).astype(F32)
        hit = (pltpu.roll(f, tok - 24, 1) == want_c) & (pltpu.roll(f, tok - 32, 1) == want_f) & (lane < top_k)
        val = f + pltpu.roll(f, tok - 8, 1) + pltpu.roll(f, tok - 16, 1)
        g = jnp.sum(jnp.where(hit, val, 0.0), axis=1, keepdims=True)
        bfeat[sl, :] = jnp.where(lane == top_k, g, jnp.where(hit, 1.0, 0.0))
        hi, mid, lo = split3(g)
        cols = jnp.where(lane == 0, hi, jnp.where(lane == 1, mid, jnp.where(lane == 2, lo, 0.0)))
        grow[i] = jnp.transpose(cols)[0:8, :]
        return carry

    lax.fori_loop(0, rows // tok, gate_rows, 0)
    poll2(1, 2, 1)

    order = [far]
    for d in range(far - 1, 0, -1):
        order += [d, -d]
    order.append(0)
    place = {d: i for i, d in enumerate(order)}
    place[-far] = 0
    ring_wait = {}

    def token_mask(b, i):
        v = jnp.transpose(jnp.concatenate([vt[b], jnp.zeros((tok - 8, tok), F32)], axis=0))
        out = None
        r = (lane + i * tok).astype(F32)
        for e in sorted({(i * tok) // cap, (i * tok + tok - 1) // cap}):
            m = (r >= v[:, e:e + 1]) & (r < v[:, e + n_exp:e + n_exp + 1])
            out = m if out is None else out | m
        return out

    n_cols = x_in.shape[1]
    tile_n = 256

    def chunk_y(d):
        q, di = chip(d), place[d]
        for k in range(2):
            b = k * chips + q
            for i in range(rows // tok):
                m = token_mask(b, i)
                for s in range(3):
                    lhs[s * 2 * tok + k * tok:s * 2 * tok + (k + 1) * tok, i * tok:(i + 1) * tok] = (
                        jnp.where(m, grow[i, s:s + 1, :], 0.0).astype(BF16))

        def body(n, carry):
            cs = pl.ds(pl.multiple_of(n * tile_n, tile_n), tile_n)
            r = dot_nn(lhs[...], orow[:, cs])
            part[di, :, cs] = r[0:2 * tok] + r[2 * tok:4 * tok] + r[4 * tok:6 * tok]
            return carry

        lax.fori_loop(0, n_cols // tile_n, body, 0)
        twin_part(0, d)

    def chunk_x(d):
        q, di = chip(d), place[d]
        for cp in ring_wait.pop(di):
            cp.wait_send()
        for k in range(2):
            b = k * chips + q
            for i in range(rows // tok):
                m = token_mask(b, i)
                lhs[k * tok:(k + 1) * tok, i * tok:(i + 1) * tok] = jnp.where(m, 1.0, 0.0).astype(BF16)

        def body(n, carry):
            cs = pl.ds(pl.multiple_of(n * tile_n, tile_n), tile_n)
            part[di, :, cs] = dot_nn(lhs[0:2 * tok, :], orow[:, cs])
            return carry

        lax.fori_loop(0, n_cols // tile_n, body, 0)
        twin_part(1, d)
        dg = dot_nn(lhs[0:2 * tok, :], mg[...])
        for k in range(2):
            t = jnp.transpose(dg[k * tok:(k + 1) * tok, :])
            dgp[k, q] = t[0:8] + t[8:16] + t[16:24]

    def mine(d, h):
        return part.at[place[d], pl.ds(pl.multiple_of(c * tok + h * half, half), half)]

    def twin_part(a, d):
        di = place[d]
        src = part.at[di, pl.ds(pl.multiple_of((1 - c) * tok, tok), tok)]
        ring_wait.setdefault(di, []).append(send(src, sib.at[a, di], rsb_s.at[a, di], rsb_r.at[a, di], twin))

    seen = set()

    def twin_part_wait(a, d):
        di = place[d]
        if (a, di) not in seen:
            seen.add((a, di))
            landed(sib.at[a, di], rsb_s.at[a, di], rsb_r.at[a, di], twin)

    def items(r):
        near, other = (0, 1) if r == 0 else (1, 0)
        out = [(far, near)]
        for d in range(far - 1, 0, -1):
            out += [(d, other), (d, near)]
        return out

    def ring_send(a, i, r):
        d, h = items(r)[i]
        sd = d if r == 0 else -d
        di = place[sd]
        twin_part_wait(a, sd)
        ref = mine(sd, h)
        total = ref[...] + sib[a, di, h * half:(h + 1) * half, :]
        if (d + 1, h) in items(r):
            p = items(r).index((d + 1, h))
            landed(ring.at[a, r, p], rs_s.at[a, r, p], rs_r.at[a, r, p], side[r])
            total = total + ring[a, r, p]
        ref[...] = total
        ring_wait.setdefault(di, []).append(send(ref, ring.at[a, r, i], rs_s.at[a, r, i], rs_r.at[a, r, i], side[r]))

    def ring_send2(a, i):
        ring_send(a, i, 0)
        ring_send(a, i, 1)

    def finish(a, src, dst):
        twin_part_wait(a, 0)
        for h in range(2):
            total = mine(0, h)[...] + sib[a, place[0], h * half:(h + 1) * half, :]
            for r in range(2):
                p = items(r).index((1, h))
                landed(ring.at[a, r, p], rs_s.at[a, r, p], rs_r.at[a, r, p], side[r])
                total = total + ring[a, r, p]
            hs = slice(h * half, (h + 1) * half)
            dst[hs, :] = (src[hs, :].astype(F32) + total).astype(BF16)

    outs = []

    def backward(e):
        es = slice(e * cap, (e + 1) * cap)
        dyr = gy[es, :].astype(F32)
        dg = jnp.sum(dyr * orow[es, :].astype(F32), axis=1, keepdims=True)
        lane_e = lax.broadcasted_iota(jnp.int32, (cap, tok), 1)
        hi, mid, lo = split3(jnp.where(lane_e < top_k, bfeat[es, :] * dg, 0.0))
        mg[es, :] = (hi + pltpu.roll(mid, 8, 1) + pltpu.roll(lo, 16, 1)).astype(BF16)
        g = (bfeat[es, top_k:top_k + 1] * dyr).astype(BF16)
        gy[es, :] = g
        dh = dot_nt(g, w2[e]).astype(BF16)
        da = (dh.astype(F32) * slope[es, :]).astype(BF16)
        dact[es, :] = da
        orow[es, :] = dot_nt(da, w1[e]).astype(BF16)

    def weight_grads(e):
        es = slice(e * cap, (e + 1) * cap)
        ff = w1.shape[2]
        deep = xa.shape[1]
        g2 = ff // deep
        for s in range(g2):
            dya[g2 * e + s] = dot_tn(hid[es, s * deep:(s + 1) * deep], gy[es, :]).astype(BF16)
            cp = pltpu.make_async_copy(dya.at[g2 * e + s], dw2_hbm.at[e, pl.ds(s * deep, deep)], o_sem.at[0, e, s])
            cp.start()
            outs.append(cp)
        g1 = n_cols // deep
        lo = ff * (e % 2)
        for s in range(g1):
            q = g1 * (e // 2) + s
            xa[q, :, lo:lo + ff] = dot_tn(brow[es, s * deep:(s + 1) * deep], dact[es, :]).astype(BF16)
            cp = pltpu.make_async_copy(xa.at[q, :, pl.ds(lo, ff)], dw1_hbm.at[e, pl.ds(s * deep, deep)], o_sem.at[1, e, s])
            cp.start()
            outs.append(cp)

    chunk_y(far)
    poll2(1, 3, 0)
    chunk_y(3)
    poll2(1, 3, 1)
    chunk_y(-3)
    ring_send2(0, 0)
    ring_send2(0, 1)
    poll2(1, 4, 0)
    poll2(1, 4, 1)
    chunk_y(2)
    chunk_y(-2)
    ring_send2(0, 2)
    gather_step(1, 0)
    chunk_y(1)
    ring_send2(0, 3)
    chunk_y(-1)
    chunk_y(0)
    gather_step(1, -1)
    ring_send2(0, 4)
    for d in (1, -2, 2, -3, 3, 4):
        gather_step(1, d)
    ring_send2(0, 5)
    backward(0)
    backward(1)
    ring_send2(0, 6)
    backward(2)
    backward(3)
    for cp in pending:
        cp.wait_send()
    pending.clear()
    chunk_x(far)
    chunk_x(3)
    chunk_x(-3)
    ring_send2(1, 0)
    ring_send2(1, 1)
    chunk_x(2)
    chunk_x(-2)
    chunk_x(1)
    finish(0, x_in, y_out)
    chunk_x(-1)
    chunk_x(0)
    ring_send2(1, 2)
    dg_cp = send(dgp.at[1 - c], dgs, dgb_s.at[0], dgb_r.at[0], twin)
    weight_grads(0)
    ring_send2(1, 3)
    landed(dgs, dgb_s.at[0], dgb_r.at[0], twin)
    dg_cp.wait_send()
    dgp[c] = dgp[c] + dgs[...]
    dg_sends = [send(dgp.at[c, chip(d)], dgr.at[z], dg_s.at[d], dg_r.at[d], dev(chip(d), c)) for d in range(1, chips)]
    weight_grads(1)
    ring_send2(1, 4)
    weight_grads(2)
    ring_send2(1, 5)
    weight_grads(3)
    ring_send2(1, 6)
    dg_total = dgp[c, z]
    for d in range(1, chips):
        landed(dgr.at[chip(-d)], dg_s.at[d], dg_r.at[d], twin)
        dg_total = dg_total + dgr[chip(-d)]
    dg_out[...] = dg_total
    finish(1, dy_in, dx_out)
    for cp in dg_sends:
        cp.wait_send()
    for v in ring_wait.values():
        for cp in v:
            cp.wait_send()
    for cp in outs:
        cp.wait()


def solution(mesh):
    groups = mesh.shape['expert']
    tok_spec = P(('data', 'expert'), None)
    weight_spec = P('expert', None, None)
    grad_spec = P(('data', 'expert'), None, None)

    def device_pass(x_in, expert_idx, gate_weight, grad_y, w_in, w_out):
        tok, top_k = expert_idx.shape
        n_exp, dm, ff = w_in.shape
        n_pairs = tok * top_k
        cap = (CAP_NUM * n_pairs) // (CAP_DEN * n_exp)
        rows = n_exp * cap
        chips = groups // 2
        info = jnp.concatenate([expert_idx.T.astype(F32), gate_weight.T], axis=0)
        vmem = pl.BlockSpec(memory_space=pltpu.VMEM)
        hbm = pl.BlockSpec(memory_space=pl.ANY)
        dma = pltpu.SemaphoreType.DMA
        y, dx, dg, dw1, dw2 = pl.pallas_call(
            functools.partial(moe_kernel, chips, cap, n_exp),
            name='moe',
            out_shape=(jax.ShapeDtypeStruct((tok, dm), BF16), jax.ShapeDtypeStruct((tok, dm), BF16),
                       jax.ShapeDtypeStruct((top_k, tok), F32),
                       jax.ShapeDtypeStruct((n_exp, dm, ff), BF16), jax.ShapeDtypeStruct((n_exp, ff, dm), BF16)),
            in_specs=[vmem, vmem, vmem, hbm, hbm],
            out_specs=(vmem, vmem, vmem, hbm, hbm),
            scratch_shapes=[
                pltpu.VMEM((2, chips, 2 * top_k, tok), F32),
                pltpu.VMEM((chips, 2 * tok, dm), BF16),
                pltpu.VMEM((chips, 2 * tok, dm), BF16),
                pltpu.VMEM((2 * chips, 8, tok), F32),
                pltpu.VMEM((2 * chips, 8, tok), F32),
                pltpu.VMEM((chips, tok, 2 * tok), BF16),
                pltpu.VMEM((rows, tok), F32),
                pltpu.VMEM((rows // tok, 8, tok), F32),
                pltpu.VMEM((rows, dm), BF16),
                pltpu.VMEM((rows, dm), BF16),
                pltpu.VMEM((rows, ff), BF16),
                pltpu.VMEM((rows, ff), F32),
                pltpu.VMEM((rows, dm), BF16),
                pltpu.VMEM((rows, ff), BF16),
                pltpu.VMEM((6 * tok, rows), BF16),
                pltpu.VMEM((chips, 2 * tok, dm), F32),
                pltpu.VMEM((2, chips, tok, dm), F32),
                pltpu.VMEM((2, 2, chips - 1, tok // 2, dm), F32),
                pltpu.VMEM((rows, tok), BF16),
                pltpu.VMEM((2, chips, 8, tok), F32),
                pltpu.VMEM((chips, 8, tok), F32),
                pltpu.VMEM((chips, 8, tok), F32),
                pltpu.VMEM((n_exp, dm, ff), BF16),
                pltpu.VMEM((n_exp, ff, dm), BF16),
                dma((2, 2, chips - 1)), dma((2, 2, chips - 1)),
                dma((2, chips, 2)), dma((2, chips, 2)),
                dma((chips,)), dma((chips,)), dma((1,)), dma((1,)),
                dma((2, 2, chips - 1)), dma((2, 2, chips - 1)),
                dma((2, chips)), dma((2, chips)),
                dma((chips,)), dma((chips,)), dma((1,)), dma((1,)),
                dma((2, n_exp)), dma((2, n_exp, 4)),
            ],
            compiler_params=pltpu.CompilerParams(collective_id=0, has_side_effects=True,
                                                 vmem_limit_bytes=VMEM_BYTES),
        )(info, x_in, grad_y, w_in, w_out)
        return y, dx, dg.T, dw1, dw2

    return jax.shard_map(device_pass, mesh=mesh,
                         in_specs=(tok_spec, tok_spec, tok_spec, tok_spec, weight_spec, weight_spec),
                         out_specs=(tok_spec, tok_spec, tok_spec, grad_spec, grad_spec), check_vma=False)
```

```python
import functools

import jax
import jax.numpy as jnp
from jax import lax
from jax.experimental import pallas as pl
from jax.experimental.pallas import tpu as pltpu
from jax.sharding import PartitionSpec as P

CAP_NUM = 5
CAP_DEN = 4
BIG = 3.3e38
F32 = jnp.float32
BF16 = jnp.bfloat16
K0 = 0.7978845608028654
K1 = 0.044715
MESH = pl.DeviceIdType.MESH
VMEM_BYTES = 67_000_000


def split3(v):
    hi = jnp.clip(v, -BIG, BIG).astype(BF16).astype(F32)
    rest = v - hi
    mid = rest.astype(BF16).astype(F32)
    lo = (rest - mid).astype(BF16).astype(F32)
    return hi, mid, lo


def gelu_and_slope(a):
    t = jnp.tanh(K0 * (a + K1 * (a * a * a)))
    cdf = 0.5 * (1.0 + t)
    return a * cdf, cdf + a * (0.5 * (1.0 - t * t)) * (K0 * (1.0 + 3.0 * K1 * (a * a)))


def dot_nn(a, b):
    return lax.dot_general(a, b, (((1,), (0,)), ((), ())), preferred_element_type=F32)


def dot_nt(a, b):
    return lax.dot_general(a, b, (((1,), (1,)), ((), ())), preferred_element_type=F32)


def dot_tn(a, b):
    return lax.dot_general(a, b, (((0,), (0,)), ((), ())), preferred_element_type=F32)


def moe_kernel(chips, cap, n_exp,
               idx_in, gate_in, x_in, dy_in, w1_hbm, w2_hbm,
               y_out, dx_out, dg_out, brow_hbm, hid_hbm, gy_hbm, dact_hbm,
               idx_all, gate_all, xa, dya, vt, cnt, tab, bfeat, grow, brow, gy, hid, slope, orow, dact, pick,
               go, tail, part, spare, sib, ring, mgt, dgp, dgt, dgs, dgr, w1, w2,
               ag_s, ag_r, agb_s, agb_r, in_s, in_r, inb_s, inb_r, rs_s, rs_r, rsb_s, rsb_r,
               dg_s, dg_r, dgb_s, dgb_r, w_sem, o_sem):
    top_k, tok = idx_in.shape
    half = tok // 2
    rows = n_exp * cap
    me = lax.axis_index('expert')
    z = me // 2
    c = me % 2
    far = chips // 2

    def chip(d):
        return (z + d + chips) % chips

    def dev(q, k):
        return {'expert': q * 2 + k}

    right, left, twin = dev(chip(1), c), dev(chip(-1), c), {'expert': z * 2 + 1 - c}
    side = (right, left)
    pending = ([], [])
    outs = []

    def emit(k, src, dst):
        cp = pltpu.make_async_copy(src, dst, o_sem.at[k])
        cp.start()
        outs.append(cp)

    def rcopy(src, dst, ss, rs, to):
        return pltpu.make_async_remote_copy(src_ref=src, dst_ref=dst, send_sem=ss, recv_sem=rs,
                                            device_id=to, device_id_type=MESH)

    def send(src, dst, ss, rs, to):
        cp = rcopy(src, dst, ss, rs, to)
        cp.start()
        return cp

    def landed(dst, ss, rs, to):
        rcopy(dst, dst, ss, rs, to).wait_recv()

    loads = []
    for e in range(n_exp):
        for k, (src, dst) in enumerate(((w1_hbm, w1), (w2_hbm, w2))):
            cp = pltpu.make_async_copy(src.at[e], dst.at[e], w_sem.at[k, e])
            cp.start()
            loads.append(cp)

    barrier = pltpu.get_barrier_semaphore()
    for d in range(1, chips):
        pl.semaphore_signal(barrier, inc=1, device_id=dev(chip(d), c), device_id_type=MESH)
    pl.semaphore_signal(barrier, inc=1, device_id=twin, device_id_type=MESH)
    pl.semaphore_wait(barrier, chips)

    bufs = (xa, dya)
    own = (x_in, dy_in)

    def item(k, h):
        return 2 * (k - 1) + h if k < far else 2 * (far - 1)

    def slot(a, q, h, k=None):
        kk = c if k is None else k
        return bufs[a].at[q, pl.ds(pl.multiple_of(kk * tok + h * half, half), half)]

    def twin_send(a, d, h, src):
        di = d % chips
        pending[a].append(send(src, slot(a, chip(d), h), agb_s.at[a, di, h], agb_r.at[a, di, h], twin))

    def twin_wait(a, d):
        di = d % chips
        for h in range(2):
            landed(slot(a, chip(d), h, 1 - c), agb_s.at[a, di, h], agb_r.at[a, di, h], twin)

    def first_send(a, h):
        src = own[a].at[pl.ds(h * half, half)]
        for r in range(2):
            i = item(1, h)
            pending[a].append(send(src, slot(a, z, h), ag_s.at[a, r, i], ag_r.at[a, r, i], side[r]))

    def poll(a, k, h, r):
        q = chip(-k) if r == 0 else chip(k)
        i = item(k, h)
        here = slot(a, q, h)
        landed(here, ag_s.at[a, r, i], ag_r.at[a, r, i], side[r])
        if k + 1 < far or (k + 1 == far and h == r):
            j = item(k + 1, h)
            pending[a].append(send(here, slot(a, q, h), ag_s.at[a, r, j], ag_r.at[a, r, j], side[r]))
        twin_send(a, (-k if r == 0 else k), h, here)

    def poll2(a, k, h):
        if k == far:
            poll(a, k, h, h)
        else:
            poll(a, k, h, 0)
            poll(a, k, h, 1)

    small = ((idx_in, idx_all), (gate_in, gate_all))
    for d in range(1, chips):
        for s, (src, dst) in enumerate(small):
            pending[1].append(send(src, dst.at[c, z], in_s.at[s, d], in_r.at[s, d], dev(chip(d), c)))
    first_send(0, 0)
    first_send(0, 1)
    first_send(1, 0)
    for src, dst in small:
        dst[c, z] = src[...]
    xa[z, pl.ds(pl.multiple_of(c * tok, tok), tok)] = x_in[...]
    dya[z, pl.ds(pl.multiple_of(c * tok, tok), tok)] = dy_in[...]
    for a in range(2):
        for h in range(2):
            twin_send(a, 0, h, own[a].at[pl.ds(h * half, half)])
    for s, (src, dst) in enumerate(small):
        for d in range(1, chips):
            landed(dst.at[c, chip(-d)], in_s.at[s, d], in_r.at[s, d], twin)
        pending[1].append(send(dst.at[c], dst.at[c], inb_s.at[s], inb_r.at[s], twin))
    poll2(0, 1, 0)
    for s, (src, dst) in enumerate(small):
        landed(dst.at[1 - c], inb_s.at[s], inb_r.at[s], twin)

    first_e = (me * n_exp).astype(F32)
    sub8 = lax.broadcasted_iota(jnp.int32, (8, tok), 0)

    def count_block(b, carry):
        k, q = b // chips, b % chips
        loc = idx_all[k, q].astype(F32) - first_e
        for e in range(n_exp):
            s = jnp.sum(jnp.where(loc == e, 1.0, 0.0), axis=0, keepdims=True)
            cnt[b, e:e + 1, :] = s
            cnt[b, n_exp + e:n_exp + e + 1, :] = s
        return carry

    lax.fori_loop(0, 2 * chips, count_block, 0)
    cmat = cnt[...].reshape(2 * chips * 8, tok)
    ri = lax.broadcasted_iota(jnp.int32, (tok, tok), 0)
    ci = lax.broadcasted_iota(jnp.int32, (tok, tok), 1)
    upper = jnp.where(ri < ci, 1.0, 0.0).astype(BF16)
    rb, cb = ri // 8, ci // 8
    r_ord, c_ord = 2 * (rb % chips) + rb // chips, 2 * (cb % chips) + cb // chips
    prior = jnp.where((c_ord < r_ord) & (ri % 8 == ci % 8), 1.0, 0.0).astype(BF16)
    cbf = cmat.astype(BF16)
    start = dot_nn(cbf, upper) + jnp.sum(dot_nn(prior, cbf), axis=1, keepdims=True)
    cnt[...] = start.reshape(2 * chips, 8, tok)
    row8 = ri % 8
    edge = jnp.where(row8 < n_exp, start, start + cmat)
    edge = jnp.minimum(edge, float(cap)) + (row8 % n_exp).astype(F32) * cap
    vt[...] = edge.reshape(2 * chips, 8, tok)
    poll2(0, 1, 1)

    def table_block(b, carry):
        k, q = b // chips, b % chips
        idx = idx_all[k, q].astype(F32)
        loc = idx - first_e
        at = jnp.zeros((top_k, tok), F32)
        for e in range(n_exp):
            at = at + jnp.where(loc == e, cnt[b, e:e + 1, :], 0.0)
        for j in range(top_k - 1):
            at = at + jnp.where((idx[j:j + 1, :] == idx) & (sub8 > j), 1.0, 0.0)
        ok = (loc >= 0.0) & (loc < n_exp) & (at < cap)
        rr = loc * cap + at
        coarse = jnp.floor(rr * 0.125)
        hi, mid, lo = split3(gate_all[k, q])
        code = jnp.where(ok, coarse - rows // 16, 200.0)
        fine = jnp.where(ok, rr - 8.0 * coarse, 0.0)
        tile = jnp.concatenate([hi, mid, lo, code, fine, jnp.zeros((tok - 40, tok), F32)], axis=0)
        tab[q, :, pl.ds(pl.multiple_of(k * tok, tok), tok)] = tile.astype(BF16)
        return carry

    lax.fori_loop(0, 2 * chips, table_block, 0)

    def esl(e):
        return pl.ds(pl.multiple_of(e * cap, cap), cap)

    def pick_rows(q, e):
        r = (lax.broadcasted_iota(jnp.int32, (cap, tok), 0) + e * cap).astype(F32)
        out = []
        for k in range(2):
            b = k * chips + q
            lo = vt[b, pl.ds(e, 1), :]
            hi = vt[b, pl.ds(e + n_exp, 1), :]
            out.append(jnp.where((r >= lo) & (r < hi), 1.0, 0.0).astype(BF16))
        return jnp.concatenate(out, axis=1)

    def gather_step(a, d):
        twin_wait(a, d)
        q = chip(d)
        dst = brow if a == 0 else gy

        def body(e, carry):
            if a == 0:
                pick[q, esl(e), :] = pick_rows(q, e)
            p = pick[q, esl(e), :]
            g = dot_nn(p, bufs[a][q]).astype(BF16)
            if d == 0:
                dst[esl(e), :] = g
            else:
                dst[esl(e), :] = dst[esl(e), :] + g
            if a == 0:
                f = dot_nt(p, tab[q])
                bfeat[esl(e), :] = f if d == 0 else bfeat[esl(e), :] + f
            return carry

        lax.fori_loop(0, n_exp, body, 0)

    gather_step(0, 0)
    poll2(0, 2, 0)
    gather_step(0, -1)
    poll2(0, 2, 1)
    gather_step(0, 1)
    poll2(0, 3, 0)
    gather_step(0, -2)
    poll2(0, 3, 1)
    first_send(1, 1)
    poll2(1, 1, 0)
    gather_step(0, 2)
    poll2(0, 4, 0)
    poll2(0, 4, 1)
    gather_step(0, -3)
    gather_step(0, 3)
    poll2(1, 1, 1)
    gather_step(0, 4)

    for cp in loads:
        cp.wait()

    def forward(e):
        act, sl = gelu_and_slope(dot_nn(brow[esl(e), :], w1[e]))
        hb = act.astype(BF16)
        hid[esl(e), :] = hb
        slope[esl(e), :] = sl
        orow[esl(e), :] = dot_nn(hb, w2[e]).astype(BF16)

    def forward_pair(e0):
        def body(i, carry):
            forward(e0 + i)
            return carry
        lax.fori_loop(0, 2, body, 0)

    forward_pair(0)
    poll2(1, 2, 0)
    forward_pair(2)
    emit(0, brow, brow_hbm)
    emit(1, hid, hid_hbm)

    lane = lax.broadcasted_iota(jnp.int32, (tok, tok), 1)

    def gate_rows(i, carry):
        sl = pl.ds(pl.multiple_of(i * tok, tok), tok)
        f = bfeat[sl, :]
        r = ri + i * tok
        want_c = (r // 8 - rows // 16).astype(F32)
        want_f = (r % 8).astype(F32)
        hit = (pltpu.roll(f, tok - 24, 1) == want_c) & (pltpu.roll(f, tok - 32, 1) == want_f) & (lane < top_k)
        val = f + pltpu.roll(f, tok - 8, 1) + pltpu.roll(f, tok - 16, 1)
        g = jnp.sum(jnp.where(hit, val, 0.0), axis=1, keepdims=True)
        bfeat[sl, :] = jnp.where(lane == top_k, g, jnp.where(hit, 1.0, 0.0))
        hi, mid, lo = split3(g)
        cols = jnp.where(lane == 0, hi, jnp.where(lane == 1, mid, jnp.where(lane == 2, lo, 0.0)))
        grow[i] = jnp.transpose(cols)[0:8, :]
        return carry

    lax.fori_loop(0, rows // tok, gate_rows, 0)
    poll2(1, 2, 1)

    order = [far]
    for d in range(far - 1, 0, -1):
        order += [d, -d]
    order.append(0)
    place = {d: i for i, d in enumerate(order)}
    place[-far] = 0
    own_wait, twin_wait_s = {}, {}
    n_cols = x_in.shape[1]
    tile = xa.shape[1]
    wide = xa.shape[2]
    blocks = rows // tok
    main = wide // tok

    def mtile(m):
        return pl.ds(pl.multiple_of(m * tile, tile), tile)

    def scale_rows(j, carry):
        js = pl.ds(pl.multiple_of(j * tok, tok), tok)
        m = j // (tile // tok)
        ms = pl.ds(pl.multiple_of((j % (tile // tok)) * tok, tok), tok)
        for i in range(blocks):
            t = jnp.transpose(orow[i * tok:(i + 1) * tok, js]).astype(F32)
            hi, mid, lo = split3(t * jnp.sum(grow[i, 0:3, :], axis=0, keepdims=True))
            go[js, i * tok:(i + 1) * tok] = hi.astype(BF16)
            for s, v in enumerate((mid, lo)):
                if i < main:
                    xa[s * (n_cols // tile) + m, ms, i * tok:(i + 1) * tok] = v.astype(BF16)
                else:
                    tail[s, js, (i - main) * tok:(i - main + 1) * tok] = v.astype(BF16)
        return carry

    def flip_rows(j, carry):
        js = pl.ds(pl.multiple_of(j * tok, tok), tok)
        for i in range(blocks):
            go[js, i * tok:(i + 1) * tok] = jnp.transpose(orow[i * tok:(i + 1) * tok, js])
        return carry

    def chunk(a, d):
        q, di = chip(d), place[d]
        sp = di % spare.shape[0]
        for cp in own_wait.pop(di, []):
            cp.wait_send()
        if sp in twin_wait_s:
            twin_wait_s.pop(sp).wait_send()

        def body(m, carry):
            ms = mtile(m)
            r = dot_nn(go[ms, :], pick[q])
            if a == 0:
                for s in range(2):
                    r = r + dot_nn(xa[s * (n_cols // tile) + m], pick[q, 0:wide, :])
                    r = r + dot_nn(tail[s, ms, :], pick[q, wide:rows, :])
            r0, r1 = r[:, 0:tok], r[:, tok:2 * tok]
            part[di, ms, :] = jnp.where(c == 0, r0, r1)
            spare[sp, ms, :] = jnp.where(c == 0, r1, r0)
            return carry

        lax.fori_loop(0, n_cols // tile, body, 0)
        twin_wait_s[sp] = send(spare.at[sp], sib.at[a, di], rsb_s.at[a, di], rsb_r.at[a, di], twin)
        if a == 1:
            t = dot_nn(mgt[...], pick[q])
            t = t[0:8] + t[8:16] + t[16:24]
            dgp[q] = jnp.where(c == 0, t[:, 0:tok], t[:, tok:2 * tok])
            dgt[q] = jnp.where(c == 0, t[:, tok:2 * tok], t[:, 0:tok])

    hd = n_cols // 2

    def mine(d, h):
        return part.at[place[d], pl.ds(h * hd, hd)]

    seen = set()

    def twin_part_wait(a, d):
        di = place[d]
        if (a, di) not in seen:
            seen.add((a, di))
            landed(sib.at[a, di], rsb_s.at[a, di], rsb_r.at[a, di], twin)

    def items(r):
        near, other = (0, 1) if r == 0 else (1, 0)
        out = [(far, near)]
        for d in range(far - 1, 0, -1):
            out += [(d, other), (d, near)]
        return out

    def ring_send(a, i, r):
        d, h = items(r)[i]
        sd = d if r == 0 else -d
        di = place[sd]
        twin_part_wait(a, sd)
        ref = mine(sd, h)
        total = ref[...] + sib[a, di, h * hd:(h + 1) * hd, :]
        if (d + 1, h) in items(r):
            p = items(r).index((d + 1, h))
            landed(ring.at[a, r, p], rs_s.at[a, r, p], rs_r.at[a, r, p], side[r])
            total = total + ring[a, r, p]
        ref[...] = total
        own_wait.setdefault(di, []).append(send(ref, ring.at[a, r, i], rs_s.at[a, r, i], rs_r.at[a, r, i], side[r]))

    def ring_send2(a, i):
        ring_send(a, i, 0)
        ring_send(a, i, 1)

    def finish(a, src, dst):
        twin_part_wait(a, 0)
        for h in range(2):
            total = mine(0, h)[...] + sib[a, place[0], h * hd:(h + 1) * hd, :]
            for r in range(2):
                p = items(r).index((1, h))
                landed(ring.at[a, r, p], rs_s.at[a, r, p], rs_r.at[a, r, p], side[r])
                total = total + ring[a, r, p]
            for j in range(hd // tok):
                cs = slice(h * hd + j * tok, h * hd + (j + 1) * tok)
                dst[:, cs] = (src[:, cs].astype(F32) + jnp.transpose(total[j * tok:(j + 1) * tok, :])).astype(BF16)

    def backward_pair(e0):
        def body(i, carry):
            e = e0 + i
            es = esl(e)
            dyr = gy[es, :].astype(F32)
            f = bfeat[es, :]
            dg = jnp.sum(dyr * orow[es, :].astype(F32), axis=1, keepdims=True)
            lane_e = lax.broadcasted_iota(jnp.int32, (cap, tok), 1)
            hi, mid, lo = split3(jnp.where(lane_e < top_k, f * dg, 0.0))
            bfeat[es, :] = hi + pltpu.roll(mid, 8, 1) + pltpu.roll(lo, 16, 1)
            g = (f[:, top_k:top_k + 1] * dyr).astype(BF16)
            gy[es, :] = g
            dh = dot_nt(g, w2[e]).astype(BF16)
            da = (dh.astype(F32) * slope[es, :]).astype(BF16)
            dact[es, :] = da
            orow[es, :] = dot_nt(da, w1[e]).astype(BF16)
            return carry
        lax.fori_loop(0, 2, body, 0)

    def gate_cols(i, carry):
        sl = pl.ds(pl.multiple_of(i * tok, tok), tok)
        mgt[:, sl] = jnp.transpose(bfeat[sl, :])[0:mgt.shape[0], :].astype(BF16)
        return carry

    for cp in pending[0]:
        cp.wait_send()
    lax.fori_loop(0, n_cols // tok, scale_rows, 0)
    poll2(1, 3, 0)
    chunk(0, far)
    poll2(1, 3, 1)
    chunk(0, 3)
    ring_send2(0, 0)
    chunk(0, -3)
    ring_send2(0, 1)
    poll2(1, 4, 0)
    poll2(1, 4, 1)
    chunk(0, 2)
    chunk(0, -2)
    ring_send2(0, 2)
    chunk(0, 1)
    chunk(0, -1)
    ring_send2(0, 3)
    chunk(0, 0)
    gather_step(1, 0)
    gather_step(1, -1)
    ring_send2(0, 4)
    for d in (1, -2, 2, -3, 3, 4):
        gather_step(1, d)
    ring_send2(0, 5)
    backward_pair(0)
    ring_send2(0, 6)
    backward_pair(2)
    emit(2, gy, gy_hbm)
    emit(3, dact, dact_hbm)
    lax.fori_loop(0, blocks, gate_cols, 0)
    lax.fori_loop(0, n_cols // tok, flip_rows, 0)
    chunk(1, far)
    chunk(1, 3)
    ring_send2(1, 0)
    chunk(1, -3)
    ring_send2(1, 1)
    chunk(1, 2)
    chunk(1, -2)
    chunk(1, 1)
    chunk(1, -1)
    finish(0, x_in, y_out)
    ring_send2(1, 2)
    chunk(1, 0)
    dg_cp = send(dgt, dgs, dgb_s.at[0], dgb_r.at[0], twin)
    ring_send2(1, 3)
    landed(dgs, dgb_s.at[0], dgb_r.at[0], twin)
    dgp[...] = dgp[...] + dgs[...]
    dg_sends = [send(dgp.at[chip(d)], dgr.at[z], dg_s.at[d], dg_r.at[d], dev(chip(d), c)) for d in range(1, chips)]
    ring_send2(1, 4)
    ring_send2(1, 5)
    ring_send2(1, 6)
    dg_total = dgp[z]
    for d in range(1, chips):
        landed(dgr.at[chip(-d)], dg_s.at[d], dg_r.at[d], twin)
        dg_total = dg_total + dgr[chip(-d)]
    dg_out[...] = dg_total
    finish(1, dy_in, dx_out)
    dg_cp.wait_send()
    for group in (dg_sends, pending[1], list(twin_wait_s.values()), *own_wait.values()):
        for cp in group:
            cp.wait_send()
    for cp in outs:
        cp.wait()


def weight_kernel(y_ref, dx_ref, dg_ref, brow, hid, gy, dact, y_out, dx_out, dg_out, dw1, dw2):
    @pl.when(pl.program_id(0) == 0)
    def _():
        y_out[...] = y_ref[...]
        dx_out[...] = dx_ref[...]
        dg_out[...] = dg_ref[...]

    dw2[0] = dot_tn(hid[...], gy[...]).astype(BF16)
    dw1[0] = dot_tn(brow[...], dact[...]).astype(BF16)


def solution(mesh):
    groups = mesh.shape['expert']
    tok_spec = P(('data', 'expert'), None)
    weight_spec = P('expert', None, None)
    grad_spec = P(('data', 'expert'), None, None)

    def device_pass(x_in, expert_idx, gate_weight, grad_y, w_in, w_out):
        tok, top_k = expert_idx.shape
        n_exp, dm, ff = w_in.shape
        n_pairs = tok * top_k
        cap = (CAP_NUM * n_pairs) // (CAP_DEN * n_exp)
        rows = n_exp * cap
        chips = groups // 2
        vmem = pl.BlockSpec(memory_space=pltpu.VMEM)
        hbm = pl.BlockSpec(memory_space=pl.ANY)
        dma = pltpu.SemaphoreType.DMA
        shape = jax.ShapeDtypeStruct
        small = (shape((tok, dm), BF16), shape((tok, dm), BF16), shape((top_k, tok), F32))
        mids = pl.pallas_call(
            functools.partial(moe_kernel, chips, cap, n_exp),
            name='moe',
            out_shape=small + (shape((rows, dm), BF16), shape((rows, ff), BF16), shape((rows, dm), BF16), shape((rows, ff), BF16)),
            in_specs=[vmem, vmem, vmem, vmem, hbm, hbm],
            out_specs=(vmem, vmem, vmem, hbm, hbm, hbm, hbm),
            scratch_shapes=[
                pltpu.VMEM((2, chips, top_k, tok), jnp.int32),
                pltpu.VMEM((2, chips, top_k, tok), F32),
                pltpu.VMEM((chips, 2 * tok, dm), BF16),
                pltpu.VMEM((chips, 2 * tok, dm), BF16),
                pltpu.VMEM((2 * chips, 8, tok), F32),
                pltpu.VMEM((2 * chips, 8, tok), F32),
                pltpu.VMEM((chips, tok, 2 * tok), BF16),
                pltpu.VMEM((rows, tok), F32),
                pltpu.VMEM((rows // tok, 8, tok), F32),
                pltpu.VMEM((rows, dm), BF16),
                pltpu.VMEM((rows, dm), BF16),
                pltpu.VMEM((rows, ff), BF16),
                pltpu.VMEM((rows, ff), F32),
                pltpu.VMEM((rows, dm), BF16),
                pltpu.VMEM((rows, ff), BF16),
                pltpu.VMEM((chips, rows, 2 * tok), BF16),
                pltpu.VMEM((dm, rows), BF16),
                pltpu.VMEM((2, dm, rows - dm), BF16),
                pltpu.VMEM((chips, dm, tok), F32),
                pltpu.VMEM((4, dm, tok), F32),
                pltpu.VMEM((2, chips, dm, tok), F32),
                pltpu.VMEM((2, 2, chips - 1, dm // 2, tok), F32),
                pltpu.VMEM((32, rows), BF16),
                pltpu.VMEM((chips, 8, tok), F32),
                pltpu.VMEM((chips, 8, tok), F32),
                pltpu.VMEM((chips, 8, tok), F32),
                pltpu.VMEM((chips, 8, tok), F32),
                pltpu.VMEM((n_exp, dm, ff), BF16),
                pltpu.VMEM((n_exp, ff, dm), BF16),
                dma((2, 2, chips - 1)), dma((2, 2, chips - 1)),
                dma((2, chips, 2)), dma((2, chips, 2)),
                dma((2, chips)), dma((2, chips)), dma((2,)), dma((2,)),
                dma((2, 2, chips - 1)), dma((2, 2, chips - 1)),
                dma((2, chips)), dma((2, chips)),
                dma((chips,)), dma((chips,)), dma((1,)), dma((1,)),
                dma((2, n_exp)), dma((4,)),
            ],
            compiler_params=pltpu.CompilerParams(collective_id=0, has_side_effects=True,
                                                 vmem_limit_bytes=VMEM_BYTES),
        )(expert_idx.T, gate_weight.T, x_in, grad_y, w_in, w_out)
        y, dx, dg, dw1, dw2 = pl.pallas_call(
            weight_kernel,
            name='weights',
            grid=(n_exp,),
            out_shape=small + (shape((n_exp, dm, ff), BF16), shape((n_exp, ff, dm), BF16)),
            in_specs=[pl.BlockSpec((tok, dm), lambda e: (0, 0)), pl.BlockSpec((tok, dm), lambda e: (0, 0)),
                      pl.BlockSpec((top_k, tok), lambda e: (0, 0)),
                      pl.BlockSpec((cap, dm), lambda e: (e, 0)), pl.BlockSpec((cap, ff), lambda e: (e, 0)),
                      pl.BlockSpec((cap, dm), lambda e: (e, 0)), pl.BlockSpec((cap, ff), lambda e: (e, 0))],
            out_specs=(pl.BlockSpec((tok, dm), lambda e: (0, 0)), pl.BlockSpec((tok, dm), lambda e: (0, 0)),
                       pl.BlockSpec((top_k, tok), lambda e: (0, 0)),
                       pl.BlockSpec((1, dm, ff), lambda e: (e, 0, 0)), pl.BlockSpec((1, ff, dm), lambda e: (e, 0, 0))),
        )(*mids)
        return y, dx, dg.T, dw1, dw2

    return jax.shard_map(device_pass, mesh=mesh,
                         in_specs=(tok_spec, tok_spec, tok_spec, tok_spec, weight_spec, weight_spec),
                         out_specs=(tok_spec, tok_spec, tok_spec, grad_spec, grad_spec), check_vma=False)
```

```python
import functools

import jax
import jax.numpy as jnp
from jax import lax
from jax.experimental import pallas as pl
from jax.experimental.pallas import tpu as pltpu
from jax.sharding import PartitionSpec as P

CAP_NUM = 5
CAP_DEN = 4
BIG = 3.3e38
F32 = jnp.float32
BF16 = jnp.bfloat16
K0 = 0.7978845608028654
K1 = 0.044715
MESH = pl.DeviceIdType.MESH
VMEM_BYTES = 67_000_000


def split3(v):
    hi = jnp.clip(v, -BIG, BIG).astype(BF16).astype(F32)
    rest = v - hi
    mid = rest.astype(BF16).astype(F32)
    lo = (rest - mid).astype(BF16).astype(F32)
    return hi, mid, lo


def gelu_and_slope(a):
    t = jnp.tanh(K0 * (a + K1 * (a * a * a)))
    cdf = 0.5 * (1.0 + t)
    return a * cdf, cdf + a * (0.5 * (1.0 - t * t)) * (K0 * (1.0 + 3.0 * K1 * (a * a)))


def dot_nn(a, b):
    return lax.dot_general(a, b, (((1,), (0,)), ((), ())), preferred_element_type=F32)


def dot_nt(a, b):
    return lax.dot_general(a, b, (((1,), (1,)), ((), ())), preferred_element_type=F32)


def dot_tn(a, b):
    return lax.dot_general(a, b, (((0,), (0,)), ((), ())), preferred_element_type=F32)


def moe_kernel(chips, cap, n_exp,
               idx_hbm, gate_hbm, x_hbm, dy_hbm, w1_hbm, w2_hbm,
               y_hbm, dx_hbm, dg_hbm, dw1_hbm, dw2_hbm,
               xs, ys, idx_all, gate_all, xa, dya, vt, cnt, tab, ft, hitm, grow, gcol, brow, gy, hid, slope, orow, dact,
               pick, go, tail, part, spare, sib, ring, mgt, dgp, dgt, dgs, dgr, w1, w2,
               ag_s, ag_r, agb_s, agb_r, in_s, in_r, inb_s, inb_r, rs_s, rs_r, rsb_s, rsb_r,
               dg_s, dg_r, dgb_s, dgb_r, l_sem, w_sem, o_sem, dw_sem):
    top_k, tok = idx_all.shape[2:]
    half = tok // 2
    rows = n_exp * cap
    me = lax.axis_index('expert')
    z = me // 2
    c = me % 2
    far = chips // 2

    def chip(d):
        return (z + d + chips) % chips

    def dev(q, k):
        return {'expert': q * 2 + k}

    right, left, twin = dev(chip(1), c), dev(chip(-1), c), {'expert': z * 2 + 1 - c}
    side = (right, left)
    pending = ([], [])
    outs = []

    def emit(k, src, dst):
        cp = pltpu.make_async_copy(src, dst, o_sem.at[k])
        cp.start()
        outs.append(cp)

    def rcopy(src, dst, ss, rs, to):
        return pltpu.make_async_remote_copy(src_ref=src, dst_ref=dst, send_sem=ss, recv_sem=rs,
                                            device_id=to, device_id_type=MESH)

    def send(src, dst, ss, rs, to):
        cp = rcopy(src, dst, ss, rs, to)
        cp.start()
        return cp

    def landed(dst, ss, rs, to):
        rcopy(dst, dst, ss, rs, to).wait_recv()

    own_rows = pl.ds(pl.multiple_of(c * tok, tok), tok)
    inputs = []
    for k, (src, dst) in enumerate(((idx_hbm, idx_all.at[c, z]), (gate_hbm, gate_all.at[c, z]), (x_hbm, xs), (dy_hbm, ys),
                                    (x_hbm, xa.at[z, own_rows]), (dy_hbm, dya.at[z, own_rows]))):
        cp = pltpu.make_async_copy(src, dst, l_sem.at[k])
        cp.start()
        inputs.append(cp)

    barrier = pltpu.get_barrier_semaphore()
    for d in range(1, chips):
        pl.semaphore_signal(barrier, inc=1, device_id=dev(chip(d), c), device_id_type=MESH)
    pl.semaphore_signal(barrier, inc=1, device_id=twin, device_id_type=MESH)

    loads = []
    for e in range(n_exp):
        for k, (src, dst) in enumerate(((w1_hbm, w1), (w2_hbm, w2))):
            cp = pltpu.make_async_copy(src.at[e], dst.at[e], w_sem.at[k, e])
            cp.start()
            loads.append(cp)
    for cp in inputs:
        cp.wait()
    pl.semaphore_wait(barrier, chips)

    bufs = (xa, dya)
    own = (xs, ys)

    def item(k, h):
        return 2 * (k - 1) + h if k < far else 2 * (far - 1)

    def slot(a, q, h, k=None):
        kk = c if k is None else k
        return bufs[a].at[q, pl.ds(pl.multiple_of(kk * tok + h * half, half), half)]

    def twin_send(a, d, h, src):
        di = d % chips
        pending[a].append(send(src, slot(a, chip(d), h), agb_s.at[a, di, h], agb_r.at[a, di, h], twin))

    def twin_wait(a, d):
        di = d % chips
        for h in range(2):
            landed(slot(a, chip(d), h, 1 - c), agb_s.at[a, di, h], agb_r.at[a, di, h], twin)

    def first_send(a, h):
        src = own[a].at[pl.ds(h * half, half)]
        for r in range(2):
            i = item(1, h)
            pending[a].append(send(src, slot(a, z, h), ag_s.at[a, r, i], ag_r.at[a, r, i], side[r]))

    def poll(a, k, h, r):
        q = chip(-k) if r == 0 else chip(k)
        i = item(k, h)
        here = slot(a, q, h)
        landed(here, ag_s.at[a, r, i], ag_r.at[a, r, i], side[r])
        if k + 1 < far or (k + 1 == far and h == r):
            j = item(k + 1, h)
            pending[a].append(send(here, slot(a, q, h), ag_s.at[a, r, j], ag_r.at[a, r, j], side[r]))
        twin_send(a, (-k if r == 0 else k), h, here)

    def poll2(a, k, h):
        if k == far:
            poll(a, k, h, h)
        else:
            poll(a, k, h, 0)
            poll(a, k, h, 1)

    small = (idx_all, gate_all)
    for d in range(1, chips):
        for s, dst in enumerate(small):
            pending[1].append(send(dst.at[c, z], dst.at[c, z], in_s.at[s, d], in_r.at[s, d], dev(chip(d), c)))
    first_send(0, 0)
    first_send(0, 1)
    first_send(1, 0)
    for a in range(2):
        for h in range(2):
            twin_send(a, 0, h, own[a].at[pl.ds(h * half, half)])
    for s, dst in enumerate(small):
        for d in range(1, chips):
            landed(dst.at[c, chip(-d)], in_s.at[s, d], in_r.at[s, d], twin)
        pending[1].append(send(dst.at[c], dst.at[c], inb_s.at[s], inb_r.at[s], twin))
    poll2(0, 1, 0)
    for s, dst in enumerate(small):
        landed(dst.at[1 - c], inb_s.at[s], inb_r.at[s], twin)

    first_e = (me * n_exp).astype(F32)
    sub8 = lax.broadcasted_iota(jnp.int32, (8, tok), 0)

    def count_block(b, carry):
        k, q = b // chips, b % chips
        loc = idx_all[k, q].astype(F32) - first_e
        for e in range(n_exp):
            s = jnp.sum(jnp.where(loc == e, 1.0, 0.0), axis=0, keepdims=True)
            cnt[b, e:e + 1, :] = s
            cnt[b, n_exp + e:n_exp + e + 1, :] = s
        return carry

    lax.fori_loop(0, 2 * chips, count_block, 0)
    cmat = cnt[...].reshape(2 * chips * 8, tok)
    ri = lax.broadcasted_iota(jnp.int32, (tok, tok), 0)
    ci = lax.broadcasted_iota(jnp.int32, (tok, tok), 1)
    upper = jnp.where(ri < ci, 1.0, 0.0).astype(BF16)
    rb, cb = ri // 8, ci // 8
    r_ord, c_ord = 2 * (rb % chips) + rb // chips, 2 * (cb % chips) + cb // chips
    prior = jnp.where((c_ord < r_ord) & (ri % 8 == ci % 8), 1.0, 0.0).astype(BF16)
    cbf = cmat.astype(BF16)
    start = dot_nn(cbf, upper) + jnp.sum(dot_nn(prior, cbf), axis=1, keepdims=True)
    cnt[...] = start.reshape(2 * chips, 8, tok)
    row8 = ri % 8
    edge = jnp.where(row8 < n_exp, start, start + cmat)
    edge = jnp.minimum(edge, float(cap)) + (row8 % n_exp).astype(F32) * cap
    vt[...] = edge.reshape(2 * chips, 8, tok)
    poll2(0, 1, 1)

    def table_block(b, carry):
        k, q = b // chips, b % chips
        idx = idx_all[k, q].astype(F32)
        loc = idx - first_e
        at = jnp.zeros((top_k, tok), F32)
        for e in range(n_exp):
            at = at + jnp.where(loc == e, cnt[b, e:e + 1, :], 0.0)
        for j in range(top_k - 1):
            at = at + jnp.where((idx[j:j + 1, :] == idx) & (sub8 > j), 1.0, 0.0)
        ok = (loc >= 0.0) & (loc < n_exp) & (at < cap)
        rr = loc * cap + at
        coarse = jnp.floor(rr * 0.125)
        hi, mid, lo = split3(gate_all[k, q])
        code = jnp.where(ok, coarse - rows // 16, 200.0)
        fine = jnp.where(ok, rr - 8.0 * coarse, 0.0)
        tile = jnp.concatenate([hi, mid, lo, code, fine, jnp.zeros((8, tok), F32)], axis=0)
        tab[q, :, pl.ds(pl.multiple_of(k * tok, tok), tok)] = tile.astype(BF16)
        return carry

    lax.fori_loop(0, 2 * chips, table_block, 0)

    def esl(e):
        return pl.ds(pl.multiple_of(e * cap, cap), cap)

    ft[...] = jnp.zeros_like(ft)

    def pick_block(q, carry):
        for e in range(n_exp):
            r = (lax.broadcasted_iota(jnp.int32, (cap, tok), 0) + e * cap).astype(F32)
            out = []
            for k in range(2):
                b = k * chips + q
                out.append(jnp.where((r >= vt[b, e:e + 1, :]) & (r < vt[b, n_exp + e:n_exp + e + 1, :]), 1.0, 0.0).astype(BF16))
            pick[q, e * cap:(e + 1) * cap, :] = jnp.concatenate(out, axis=1)
        ft[...] = ft[...] + dot_nt(tab[q], pick[q])
        return carry

    lax.fori_loop(0, chips // 2, pick_block, 0)
    poll2(0, 2, 0)
    lax.fori_loop(chips // 2, chips, pick_block, 0)
    poll2(0, 2, 1)
    first_send(1, 1)

    r8 = lax.broadcasted_iota(jnp.int32, (top_k, rows), 1)
    hit = (ft[24:32, :] == ((r8 >> 3) - rows // 16).astype(F32)) & (ft[32:40, :] == (r8 & 7).astype(F32))
    val = ft[0:8, :] + ft[8:16, :] + ft[16:24, :]
    hitm[...] = jnp.where(hit, 1.0, 0.0)
    grow[...] = jnp.broadcast_to(jnp.sum(jnp.where(hit, val, 0.0), axis=0, keepdims=True), (8, rows))

    def gate_col(i, carry):
        sl = pl.ds(pl.multiple_of(i * tok, tok), tok)
        gcol[sl, :] = jnp.transpose(jnp.broadcast_to(grow[0:1, sl], (tok, tok)))
        return carry

    lax.fori_loop(0, rows // tok, gate_col, 0)

    def gather(a, ds, first=False):
        for d in ds:
            twin_wait(a, d)
        dst = brow if a == 0 else gy

        def body(e, carry):
            r = None
            for d in ds:
                q = chip(d)
                t = dot_nn(pick[q, esl(e), :], bufs[a][q])
                r = t if r is None else r + t
            r = r.astype(BF16)
            dst[esl(e), :] = r if first else dst[esl(e), :] + r
            return carry

        lax.fori_loop(0, n_exp, body, 0)

    gather(0, (0, 1, -1), True)
    poll2(0, 3, 0)
    gather(0, (2, -2))
    poll2(0, 3, 1)
    poll2(1, 1, 0)
    poll2(0, 4, 0)
    poll2(0, 4, 1)
    poll2(1, 1, 1)
    gather(0, (3, -3, 4))

    for cp in loads:
        cp.wait()

    def forward_pair(e0):
        def body(i, carry):
            e = e0 + i
            act, sl = gelu_and_slope(dot_nn(brow[esl(e), :], w1[e]))
            hb = act.astype(BF16)
            hid[esl(e), :] = hb
            slope[esl(e), :] = sl
            orow[esl(e), :] = dot_nn(hb, w2[e]).astype(BF16)
            return carry
        lax.fori_loop(0, 2, body, 0)

    forward_pair(0)
    poll2(1, 2, 0)
    forward_pair(2)
    poll2(1, 2, 1)

    order = [far]
    for d in range(far - 1, 0, -1):
        order += [d, -d]
    order.append(0)
    place = {d: i for i, d in enumerate(order)}
    place[-far] = 0
    own_wait, twin_wait_s = {}, {}
    n_cols = xs.shape[1]
    tile = xa.shape[1]
    wide = xa.shape[2]
    blocks = rows // tok
    main = wide // tok

    def mtile(m):
        return pl.ds(pl.multiple_of(m * tile, tile), tile)

    def scale_rows(j, carry):
        js = pl.ds(pl.multiple_of(j * tok, tok), tok)
        m = j // (tile // tok)
        ms = pl.ds(pl.multiple_of((j % (tile // tok)) * tok, tok), tok)
        for i in range(blocks):
            t = jnp.transpose(orow[i * tok:(i + 1) * tok, js]).astype(F32)
            hi, mid, lo = split3(t * grow[0:1, i * tok:(i + 1) * tok])
            go[js, i * tok:(i + 1) * tok] = hi.astype(BF16)
            for s, v in enumerate((mid, lo)):
                if i < main:
                    xa[s * (n_cols // tile) + m, ms, i * tok:(i + 1) * tok] = v.astype(BF16)
                else:
                    tail[s, js, (i - main) * tok:(i - main + 1) * tok] = v.astype(BF16)
        return carry

    def flip_rows(j, carry):
        js = pl.ds(pl.multiple_of(j * tok, tok), tok)
        for i in range(blocks):
            go[js, i * tok:(i + 1) * tok] = jnp.transpose(orow[i * tok:(i + 1) * tok, js])
        return carry

    def chunk(a, d):
        q, di = chip(d), place[d]
        sp = di % spare.shape[0]
        for cp in own_wait.pop(di, []):
            cp.wait_send()
        if sp in twin_wait_s:
            twin_wait_s.pop(sp).wait_send()

        def body(m, carry):
            ms = mtile(m)
            r = dot_nn(go[ms, :], pick[q])
            if a == 0:
                for s in range(2):
                    r = r + dot_nn(xa[s * (n_cols // tile) + m], pick[q, 0:wide, :])
                    r = r + dot_nn(tail[s, ms, :], pick[q, wide:rows, :])
            r0, r1 = r[:, 0:tok], r[:, tok:2 * tok]
            part[di, ms, :] = jnp.where(c == 0, r0, r1)
            spare[sp, ms, :] = jnp.where(c == 0, r1, r0)
            return carry

        lax.fori_loop(0, n_cols // tile, body, 0)
        twin_wait_s[sp] = send(spare.at[sp], sib.at[a, di], rsb_s.at[a, di], rsb_r.at[a, di], twin)
        if a == 1:
            t = dot_nn(mgt[...], pick[q])
            t = t[0:8] + t[8:16] + t[16:24]
            dgp[q] = jnp.where(c == 0, t[:, 0:tok], t[:, tok:2 * tok])
            dgt[q] = jnp.where(c == 0, t[:, tok:2 * tok], t[:, 0:tok])

    hd = n_cols // 2

    def mine(d, h):
        return part.at[place[d], pl.ds(h * hd, hd)]

    seen = set()

    def twin_part_wait(a, d):
        di = place[d]
        if (a, di) not in seen:
            seen.add((a, di))
            landed(sib.at[a, di], rsb_s.at[a, di], rsb_r.at[a, di], twin)

    def items(r):
        near, other = (0, 1) if r == 0 else (1, 0)
        out = [(far, near)]
        for d in range(far - 1, 0, -1):
            out += [(d, other), (d, near)]
        return out

    def ring_send(a, i, r):
        d, h = items(r)[i]
        sd = d if r == 0 else -d
        di = place[sd]
        twin_part_wait(a, sd)
        ref = mine(sd, h)
        total = ref[...] + sib[a, di, h * hd:(h + 1) * hd, :]
        if (d + 1, h) in items(r):
            p = items(r).index((d + 1, h))
            landed(ring.at[a, r, p], rs_s.at[a, r, p], rs_r.at[a, r, p], side[r])
            total = total + ring[a, r, p]
        ref[...] = total
        own_wait.setdefault(di, []).append(send(ref, ring.at[a, r, i], rs_s.at[a, r, i], rs_r.at[a, r, i], side[r]))

    def ring_send2(a, i):
        ring_send(a, i, 0)
        ring_send(a, i, 1)

    def finish(a, src, dst):
        twin_part_wait(a, 0)
        for h in range(2):
            total = mine(0, h)[...] + sib[a, place[0], h * hd:(h + 1) * hd, :]
            for r in range(2):
                p = items(r).index((1, h))
                landed(ring.at[a, r, p], rs_s.at[a, r, p], rs_r.at[a, r, p], side[r])
                total = total + ring[a, r, p]
            for j in range(hd // tok):
                cs = slice(h * hd + j * tok, h * hd + (j + 1) * tok)
                dst[:, cs] = (src[:, cs].astype(F32) + jnp.transpose(total[j * tok:(j + 1) * tok, :])).astype(BF16)

    def backward_pair(e0):
        def body(i, carry):
            e = e0 + i
            es = esl(e)
            dyr = gy[es, :].astype(F32)
            gc = gcol[es, :]
            dg = jnp.sum(dyr * orow[es, :].astype(F32), axis=1, keepdims=True)
            gcol[es, :] = jnp.broadcast_to(dg, (cap, tok))
            g = (jnp.concatenate([gc] * (n_cols // tok), axis=1) * dyr).astype(BF16)
            gy[es, :] = g
            dh = dot_nt(g, w2[e]).astype(BF16)
            da = (dh.astype(F32) * slope[es, :]).astype(BF16)
            dact[es, :] = da
            orow[es, :] = dot_nt(da, w1[e]).astype(BF16)
            return carry
        lax.fori_loop(0, 2, body, 0)

    def gate_cols(i, carry):
        sl = pl.ds(pl.multiple_of(i * tok, tok), tok)
        d = jnp.transpose(gcol[sl, :])[0:8, :]
        hi, mid, lo = split3(jnp.where(hitm[:, sl] > 0.0, d, 0.0))
        mgt[:, sl] = jnp.concatenate([hi, mid, lo, jnp.zeros_like(hi)], axis=0).astype(BF16)
        return carry

    ff = w1.shape[2]
    g1, g2 = n_cols // tile, ff // tile

    def weight_copies(e):
        lo = pl.multiple_of(ff * (e % 2), ff)
        out = []
        for s in range(g2):
            out.append(pltpu.make_async_copy(dya.at[g2 * e + s], dw2_hbm.at[e, pl.ds(s * tile, tile)], dw_sem.at[0, e, s]))
        for s in range(g1):
            out.append(pltpu.make_async_copy(xa.at[g1 * (e // 2) + s, :, pl.ds(lo, ff)],
                                             dw1_hbm.at[e, pl.ds(s * tile, tile)], dw_sem.at[1, e, s]))
        return out

    def weight_pair(e0):
        def body(i, carry):
            e = e0 + i
            es = esl(e)
            lo = pl.multiple_of(ff * (e % 2), ff)
            for s in range(g2):
                dya[g2 * e + s] = dot_tn(hid[es, s * tile:(s + 1) * tile], gy[es, :]).astype(BF16)
            for s in range(g1):
                xa[g1 * (e // 2) + s, :, pl.ds(lo, ff)] = dot_tn(brow[es, s * tile:(s + 1) * tile], dact[es, :]).astype(BF16)
            for cp in weight_copies(e):
                cp.start()
            return carry
        lax.fori_loop(0, 2, body, 0)

    for cp in pending[0]:
        cp.wait_send()
    lax.fori_loop(0, n_cols // tok // 2, scale_rows, 0)
    poll2(1, 3, 0)
    lax.fori_loop(n_cols // tok // 2, n_cols // tok, scale_rows, 0)
    poll2(1, 3, 1)
    chunk(0, far)
    chunk(0, 3)
    ring_send2(0, 0)
    chunk(0, -3)
    ring_send(0, 1, 0)
    poll2(1, 4, 0)
    poll2(1, 4, 1)
    chunk(0, 2)
    ring_send(0, 1, 1)
    chunk(0, -2)
    ring_send(0, 2, 0)
    chunk(0, 1)
    ring_send(0, 2, 1)
    ring_send2(0, 3)
    chunk(0, -1)
    gather(1, (0, 1, -1, 2), True)
    ring_send2(0, 4)
    chunk(0, 0)
    gather(1, (-2, 3, -3, 4))
    ring_send2(0, 5)
    backward_pair(0)
    backward_pair(2)
    lax.fori_loop(0, blocks, gate_cols, 0)
    lax.fori_loop(0, n_cols // tok, flip_rows, 0)
    ring_send2(0, 6)
    chunk(1, far)
    chunk(1, 3)
    ring_send2(1, 0)
    chunk(1, -3)
    chunk(1, 2)
    ring_send2(1, 1)
    finish(0, xs, xs)
    emit(0, xs, y_hbm)
    chunk(1, -2)
    chunk(1, 1)
    ring_send2(1, 2)
    chunk(1, -1)
    chunk(1, 0)
    dg_cp = send(dgt, dgs, dgb_s.at[0], dgb_r.at[0], twin)
    ring_send2(1, 3)
    for cp in pending[1]:
        cp.wait_send()
    landed(dgs, dgb_s.at[0], dgb_r.at[0], twin)
    dgp[...] = dgp[...] + dgs[...]
    dg_sends = [send(dgp.at[chip(d)], dgr.at[z], dg_s.at[d], dg_r.at[d], dev(chip(d), c)) for d in range(1, chips)]
    weight_pair(0)
    ring_send2(1, 4)
    weight_pair(2)
    ring_send2(1, 5)
    dg_total = dgp[z]
    for d in range(1, chips):
        landed(dgr.at[chip(-d)], dg_s.at[d], dg_r.at[d], twin)
        dg_total = dg_total + dgr[chip(-d)]
    dgr[z] = dg_total
    emit(2, dgr.at[z], dg_hbm)
    ring_send2(1, 6)
    dg_cp.wait_send()
    for cp in dg_sends:
        cp.wait_send()
    for e in range(n_exp):
        for cp in weight_copies(e):
            cp.wait()
    finish(1, ys, ys)
    emit(1, ys, dx_hbm)
    for group in (list(twin_wait_s.values()), *own_wait.values()):
        for cp in group:
            cp.wait_send()
    for cp in outs:
        cp.wait()


def copy_kernel(n, *refs):
    ins, outs, bufs, sem = refs[:n], refs[n:2 * n], refs[2 * n:3 * n], refs[3 * n]
    jobs = []
    for k in range(n - 1, -1, -1):
        if ins[k].ndim == 3:
            jobs += [(k, e, ins[k].at[e], outs[k].at[e], bufs[k].at[e]) for e in range(ins[k].shape[0])]
        else:
            jobs.append((k, 0, ins[k], outs[k], bufs[k]))
    loads = [pltpu.make_async_copy(i, b, sem.at[0, k, e]) for k, e, i, o, b in jobs]
    stores = [pltpu.make_async_copy(b, o, sem.at[1, k, e]) for k, e, i, o, b in jobs]
    for cp in loads:
        cp.start()
    for ld, st in zip(loads, stores):
        ld.wait()
        st.start()
    for cp in stores:
        cp.wait()


def solution(mesh):
    groups = mesh.shape['expert']
    tok_spec = P(('data', 'expert'), None)
    weight_spec = P('expert', None, None)
    grad_spec = P(('data', 'expert'), None, None)

    def device_pass(x_in, expert_idx, gate_weight, grad_y, w_in, w_out):
        tok, top_k = expert_idx.shape
        n_exp, dm, ff = w_in.shape
        n_pairs = tok * top_k
        cap = (CAP_NUM * n_pairs) // (CAP_DEN * n_exp)
        rows = n_exp * cap
        chips = groups // 2
        hbm = pl.BlockSpec(memory_space=pl.ANY)
        dma = pltpu.SemaphoreType.DMA
        shape = jax.ShapeDtypeStruct
        outs = (shape((tok, dm), BF16), shape((tok, dm), BF16), shape((top_k, tok), F32),
                shape((n_exp, dm, ff), BF16), shape((n_exp, ff, dm), BF16))
        mids = pl.pallas_call(
            functools.partial(moe_kernel, chips, cap, n_exp),
            name='moe',
            out_shape=outs,
            in_specs=[hbm] * 6,
            out_specs=(hbm,) * 5,
            scratch_shapes=[
                pltpu.VMEM((tok, dm), BF16),
                pltpu.VMEM((tok, dm), BF16),
                pltpu.VMEM((2, chips, top_k, tok), jnp.int32),
                pltpu.VMEM((2, chips, top_k, tok), F32),
                pltpu.VMEM((chips, 2 * tok, dm), BF16),
                pltpu.VMEM((chips, 2 * tok, dm), BF16),
                pltpu.VMEM((2 * chips, 8, tok), F32),
                pltpu.VMEM((2 * chips, 8, tok), F32),
                pltpu.VMEM((chips, 48, 2 * tok), BF16),
                pltpu.VMEM((48, rows), F32),
                pltpu.VMEM((8, rows), F32),
                pltpu.VMEM((8, rows), F32),
                pltpu.VMEM((rows, tok), F32),
                pltpu.VMEM((rows, dm), BF16),
                pltpu.VMEM((rows, dm), BF16),
                pltpu.VMEM((rows, ff), BF16),
                pltpu.VMEM((rows, ff), F32),
                pltpu.VMEM((rows, dm), BF16),
                pltpu.VMEM((rows, ff), BF16),
                pltpu.VMEM((chips, rows, 2 * tok), BF16),
                pltpu.VMEM((dm, rows), BF16),
                pltpu.VMEM((2, dm, rows - dm), BF16),
                pltpu.VMEM((chips, dm, tok), F32),
                pltpu.VMEM((4, dm, tok), F32),
                pltpu.VMEM((2, chips, dm, tok), F32),
                pltpu.VMEM((2, 2, chips - 1, dm // 2, tok), F32),
                pltpu.VMEM((32, rows), BF16),
                pltpu.VMEM((chips, 8, tok), F32),
                pltpu.VMEM((chips, 8, tok), F32),
                pltpu.VMEM((chips, 8, tok), F32),
                pltpu.VMEM((chips, 8, tok), F32),
                pltpu.VMEM((n_exp, dm, ff), BF16),
                pltpu.VMEM((n_exp, ff, dm), BF16),
                dma((2, 2, chips - 1)), dma((2, 2, chips - 1)),
                dma((2, chips, 2)), dma((2, chips, 2)),
                dma((2, chips)), dma((2, chips)), dma((2,)), dma((2,)),
                dma((2, 2, chips - 1)), dma((2, 2, chips - 1)),
                dma((2, chips)), dma((2, chips)),
                dma((chips,)), dma((chips,)), dma((1,)), dma((1,)),
                dma((6,)), dma((2, n_exp)), dma((3,)), dma((2, n_exp, 4)),
            ],
            compiler_params=pltpu.CompilerParams(collective_id=0, has_side_effects=True,
                                                 vmem_limit_bytes=VMEM_BYTES),
        )(expert_idx.T, gate_weight.T, x_in, grad_y, w_in, w_out)
        y, dx, dg, dw1, dw2 = pl.pallas_call(
            functools.partial(copy_kernel, len(outs)),
            name='outputs',
            out_shape=outs,
            in_specs=[hbm] * len(outs),
            out_specs=(hbm,) * len(outs),
            scratch_shapes=[pltpu.VMEM(o.shape, o.dtype) for o in outs] + [dma((2, len(outs), n_exp))],
        )(*mids)
        return y, dx, dg.T, dw1, dw2

    return jax.shard_map(device_pass, mesh=mesh,
                         in_specs=(tok_spec, tok_spec, tok_spec, tok_spec, weight_spec, weight_spec),
                         out_specs=(tok_spec, tok_spec, tok_spec, grad_spec, grad_spec), check_vma=False)
```

```python
import functools

import jax
import jax.numpy as jnp
from jax import lax
from jax.experimental import pallas as pl
from jax.experimental.pallas import tpu as pltpu
from jax.sharding import PartitionSpec as P

CAP_NUM = 5
CAP_DEN = 4
BIG = 3.3e38
F32 = jnp.float32
BF16 = jnp.bfloat16
K0 = 0.7978845608028654
K1 = 0.044715
MESH = pl.DeviceIdType.MESH
VMEM_BYTES = 67_000_000


def split3(v):
    hi = jnp.clip(v, -BIG, BIG).astype(BF16).astype(F32)
    rest = v - hi
    mid = rest.astype(BF16).astype(F32)
    lo = (rest - mid).astype(BF16).astype(F32)
    return hi, mid, lo


def gelu_and_slope(a):
    t = jnp.tanh(K0 * (a + K1 * (a * a * a)))
    cdf = 0.5 * (1.0 + t)
    return a * cdf, cdf + a * (0.5 * (1.0 - t * t)) * (K0 * (1.0 + 3.0 * K1 * (a * a)))


def dot_nn(a, b):
    return lax.dot_general(a, b, (((1,), (0,)), ((), ())), preferred_element_type=F32)


def dot_nt(a, b):
    return lax.dot_general(a, b, (((1,), (1,)), ((), ())), preferred_element_type=F32)


def dot_tn(a, b):
    return lax.dot_general(a, b, (((0,), (0,)), ((), ())), preferred_element_type=F32)


def moe_kernel(chips, cap, n_exp,
               idx_hbm, gate_hbm, x_hbm, dy_hbm, w1_hbm, w2_hbm,
               y_hbm, dx_hbm, dg_hbm, dw1_hbm, dw2_hbm,
               xs, ys, idx_all, gate_all, xa, dya, vt, cnt, tab, ft, hitm, grow, gcol, gpart, brow, gy, hid, slope, orow, dact,
               pick, go, part, spare, sib, ring, mgt, dgp, dgt, dgs, dgr, w1, w2,
               ag_s, ag_r, agb_s, agb_r, in_s, in_r, inb_s, inb_r, rs_s, rs_r, rsb_s, rsb_r,
               dg_s, dg_r, dgb_s, dgb_r, l_sem, w_sem, o_sem, dw_sem):
    top_k, tok = idx_all.shape[2:]
    half = tok // 2
    rows = n_exp * cap
    me = lax.axis_index('expert')
    z = me // 2
    c = me % 2
    far = chips // 2

    def chip(d):
        return (z + d + chips) % chips

    def dev(q, k):
        return {'expert': q * 2 + k}

    right, left, twin = dev(chip(1), c), dev(chip(-1), c), {'expert': z * 2 + 1 - c}
    side = (right, left)
    pending = ([], [])
    outs = []

    def emit(k, src, dst):
        cp = pltpu.make_async_copy(src, dst, o_sem.at[k])
        cp.start()
        outs.append(cp)

    def rcopy(src, dst, ss, rs, to):
        return pltpu.make_async_remote_copy(src_ref=src, dst_ref=dst, send_sem=ss, recv_sem=rs,
                                            device_id=to, device_id_type=MESH)

    def send(src, dst, ss, rs, to):
        cp = rcopy(src, dst, ss, rs, to)
        cp.start()
        return cp

    def landed(dst, ss, rs, to):
        rcopy(dst, dst, ss, rs, to).wait_recv()

    own_rows = pl.ds(pl.multiple_of(c * tok, tok), tok)
    inputs = []
    for k, (src, dst) in enumerate(((idx_hbm, idx_all.at[c, z]), (gate_hbm, gate_all.at[c, z]), (x_hbm, xs), (dy_hbm, ys),
                                    (x_hbm, xa.at[z, own_rows]), (dy_hbm, dya.at[z, own_rows]))):
        cp = pltpu.make_async_copy(src, dst, l_sem.at[k])
        cp.start()
        inputs.append(cp)

    barrier = pltpu.get_barrier_semaphore()
    for d in sorted(range(1, chips), key=lambda d: -min(d, chips - d)):
        pl.semaphore_signal(barrier, inc=1, device_id=dev(chip(d), c), device_id_type=MESH)
    pl.semaphore_signal(barrier, inc=1, device_id=twin, device_id_type=MESH)

    loads = []
    for e in range(n_exp):
        for k, (src, dst) in enumerate(((w1_hbm, w1), (w2_hbm, w2))):
            cp = pltpu.make_async_copy(src.at[e], dst.at[e], w_sem.at[k, e])
            cp.start()
            loads.append(cp)
    for cp in inputs:
        cp.wait()
    pl.semaphore_wait(barrier, chips)

    bufs = (xa, dya)
    own = (xs, ys)

    def item(k, h):
        return 2 * (k - 1) + h if k < far else 2 * (far - 1)

    def slot(a, q, h, k=None):
        kk = c if k is None else k
        return bufs[a].at[q, pl.ds(pl.multiple_of(kk * tok + h * half, half), half)]

    def twin_send(a, d, h, src):
        di = d % chips
        pending[a].append(send(src, slot(a, chip(d), h), agb_s.at[a, di, h], agb_r.at[a, di, h], twin))

    def twin_wait(a, d):
        di = d % chips
        for h in range(2):
            landed(slot(a, chip(d), h, 1 - c), agb_s.at[a, di, h], agb_r.at[a, di, h], twin)

    def first_send(a, h):
        src = own[a].at[pl.ds(h * half, half)]
        for r in range(2):
            i = item(1, h)
            pending[a].append(send(src, slot(a, z, h), ag_s.at[a, r, i], ag_r.at[a, r, i], side[r]))

    def poll(a, k, h, r):
        q = chip(-k) if r == 0 else chip(k)
        i = item(k, h)
        here = slot(a, q, h)
        landed(here, ag_s.at[a, r, i], ag_r.at[a, r, i], side[r])
        if k + 1 < far or (k + 1 == far and h == r):
            j = item(k + 1, h)
            pending[a].append(send(here, slot(a, q, h), ag_s.at[a, r, j], ag_r.at[a, r, j], side[r]))
        twin_send(a, (-k if r == 0 else k), h, here)

    def poll2(a, k, h):
        if k == far:
            poll(a, k, h, h)
        else:
            poll(a, k, h, 0)
            poll(a, k, h, 1)

    small = (idx_all, gate_all)
    for d in range(1, chips):
        for s, dst in enumerate(small):
            pending[1].append(send(dst.at[c, z], dst.at[c, z], in_s.at[s, d], in_r.at[s, d], dev(chip(d), c)))
    first_send(0, 0)
    first_send(0, 1)
    first_send(1, 0)
    for a in range(2):
        for h in range(2):
            twin_send(a, 0, h, own[a].at[pl.ds(h * half, half)])
    for s, dst in enumerate(small):
        for d in range(1, chips):
            landed(dst.at[c, chip(-d)], in_s.at[s, d], in_r.at[s, d], twin)
        pending[1].append(send(dst.at[c], dst.at[c], inb_s.at[s], inb_r.at[s], twin))
    poll2(0, 1, 0)
    for s, dst in enumerate(small):
        landed(dst.at[1 - c], inb_s.at[s], inb_r.at[s], twin)

    first_e = (me * n_exp).astype(F32)
    sub8 = lax.broadcasted_iota(jnp.int32, (8, tok), 0)

    def count_block(b, carry):
        k, q = b // chips, b % chips
        loc = idx_all[k, q].astype(F32) - first_e
        for e in range(n_exp):
            s = jnp.sum(jnp.where(loc == e, 1.0, 0.0), axis=0, keepdims=True)
            cnt[b, e:e + 1, :] = s
            cnt[b, n_exp + e:n_exp + e + 1, :] = s
        return carry

    lax.fori_loop(0, 2 * chips, count_block, 0)
    cmat = cnt[...].reshape(2 * chips * 8, tok)
    ri = lax.broadcasted_iota(jnp.int32, (tok, tok), 0)
    ci = lax.broadcasted_iota(jnp.int32, (tok, tok), 1)
    upper = jnp.where(ri < ci, 1.0, 0.0).astype(BF16)
    rb, cb = ri // 8, ci // 8
    r_ord, c_ord = 2 * (rb % chips) + rb // chips, 2 * (cb % chips) + cb // chips
    prior = jnp.where((c_ord < r_ord) & (ri % 8 == ci % 8), 1.0, 0.0).astype(BF16)
    cbf = cmat.astype(BF16)
    start = dot_nn(cbf, upper) + jnp.sum(dot_nn(prior, cbf), axis=1, keepdims=True)
    cnt[...] = start.reshape(2 * chips, 8, tok)
    row8 = ri % 8
    edge = jnp.where(row8 < n_exp, start, start + cmat)
    edge = jnp.minimum(edge, float(cap)) + (row8 % n_exp).astype(F32) * cap
    vt[...] = edge.reshape(2 * chips, 8, tok)
    poll2(0, 1, 1)

    def table_block(b, carry):
        k, q = b // chips, b % chips
        idx = idx_all[k, q].astype(F32)
        loc = idx - first_e
        at = jnp.zeros((top_k, tok), F32)
        for e in range(n_exp):
            at = at + jnp.where(loc == e, cnt[b, e:e + 1, :], 0.0)
        for j in range(top_k - 1):
            at = at + jnp.where((idx[j:j + 1, :] == idx) & (sub8 > j), 1.0, 0.0)
        ok = (loc >= 0.0) & (loc < n_exp) & (at < cap)
        rr = loc * cap + at
        coarse = jnp.floor(rr * 0.125)
        hi, mid, lo = split3(gate_all[k, q])
        code = jnp.where(ok, coarse - rows // 16, 200.0)
        fine = jnp.where(ok, rr - 8.0 * coarse, 0.0)
        tile = jnp.concatenate([hi, mid, lo, code, fine, jnp.zeros((8, tok), F32)], axis=0)
        tab[q, :, pl.ds(pl.multiple_of(k * tok, tok), tok)] = tile.astype(BF16)
        return carry

    lax.fori_loop(0, 2 * chips, table_block, 0)

    def esl(e):
        return pl.ds(pl.multiple_of(e * cap, cap), cap)

    ft[...] = jnp.zeros_like(ft)

    def pick_block(q, carry):
        for e in range(n_exp):
            r = (lax.broadcasted_iota(jnp.int32, (cap, tok), 0) + e * cap).astype(F32)
            out = []
            for k in range(2):
                b = k * chips + q
                out.append(jnp.where((r >= vt[b, e:e + 1, :]) & (r < vt[b, n_exp + e:n_exp + e + 1, :]), 1.0, 0.0).astype(BF16))
            pick[q, e * cap:(e + 1) * cap, :] = jnp.concatenate(out, axis=1)
        ft[...] = ft[...] + dot_nt(tab[q], pick[q])
        return carry

    lax.fori_loop(0, chips // 2, pick_block, 0)
    poll2(0, 2, 0)
    lax.fori_loop(chips // 2, chips, pick_block, 0)
    poll2(0, 2, 1)
    first_send(1, 1)

    r8 = lax.broadcasted_iota(jnp.int32, (top_k, rows), 1)
    hit = (ft[24:32, :] == ((r8 >> 3) - rows // 16).astype(F32)) & (ft[32:40, :] == (r8 & 7).astype(F32))
    val = ft[0:8, :] + ft[8:16, :] + ft[16:24, :]
    hitm[...] = jnp.where(hit, 1.0, 0.0)
    grow[...] = jnp.broadcast_to(jnp.sum(jnp.where(hit, val, 0.0), axis=0, keepdims=True), (8, rows))

    def gate_col(i, carry):
        sl = pl.ds(pl.multiple_of(i * tok, tok), tok)
        v = jnp.transpose(jnp.broadcast_to(grow[0:1, sl], (tok, tok)))
        gcol[sl, :] = v
        for s, w in enumerate(split3(v)):
            gpart[s, sl, :] = w.astype(BF16)
        return carry

    lax.fori_loop(0, rows // tok, gate_col, 0)

    def gather(a, ds, first=False):
        for d in ds:
            twin_wait(a, d)
        dst = brow if a == 0 else gy

        def body(e, carry):
            r = None
            for d in ds:
                q = chip(d)
                t = dot_nn(pick[q, esl(e), :], bufs[a][q])
                r = t if r is None else r + t
            r = r.astype(BF16)
            dst[esl(e), :] = r if first else dst[esl(e), :] + r
            return carry

        lax.fori_loop(0, n_exp, body, 0)

    gather(0, (0, 1, -1), True)
    poll2(0, 3, 0)
    gather(0, (2, -2))
    poll2(0, 3, 1)
    poll2(1, 1, 0)
    poll2(0, 4, 0)
    poll2(0, 4, 1)
    poll2(1, 1, 1)
    gather(0, (3, -3, 4))

    for cp in loads:
        cp.wait()

    def forward_pair(e0):
        def body(i, carry):
            e = e0 + i
            act, sl = gelu_and_slope(dot_nn(brow[esl(e), :], w1[e]))
            hb = act.astype(BF16)
            hid[esl(e), :] = hb
            slope[esl(e), :] = sl
            orow[esl(e), :] = dot_nn(hb, w2[e]).astype(BF16)
            return carry
        lax.fori_loop(0, 2, body, 0)

    forward_pair(0)
    poll2(1, 2, 0)
    forward_pair(2)
    poll2(1, 2, 1)

    order = [far]
    for d in range(far - 1, 0, -1):
        order += [d, -d]
    order.append(0)
    place = {d: i for i, d in enumerate(order)}
    place[-far] = 0
    own_wait, twin_wait_s = {}, {}
    n_cols = xs.shape[1]
    tile = xa.shape[1]
    step = 2 * tile
    blocks = rows // tok

    def mtile(m):
        return pl.ds(pl.multiple_of(m * step, step), step)

    def flip_rows(j, carry):
        js = pl.ds(pl.multiple_of(j * tok, tok), tok)
        for i in range(blocks):
            go[js, i * tok:(i + 1) * tok] = jnp.transpose(orow[i * tok:(i + 1) * tok, js])
        return carry

    def chunk(a, d):
        q, di = chip(d), place[d]
        sp = di % spare.shape[0]
        for cp in own_wait.pop(di, []):
            cp.wait_send()
        if sp in twin_wait_s:
            twin_wait_s.pop(sp).wait_send()

        per = tile // tok
        if a == 0:
            def scale(i, carry):
                sl = pl.ds(pl.multiple_of(i * tok, tok), tok)
                sub = pl.ds(pl.multiple_of((i % per) * tok, tok), tok)
                for s in range(3):
                    g = gpart[s, sl, :]
                    xa[i // per, sub, s * 2 * tok:(s + 1) * 2 * tok] = pick[q, sl, :] * jnp.concatenate([g, g], axis=1)
                return carry
            lax.fori_loop(0, blocks, scale, 0)

        def body(m, carry):
            ms = mtile(m)
            if a == 0:
                r = None
                for s in range(3):
                    w = xa[0:rows // tile, :, s * 2 * tok:(s + 1) * 2 * tok].reshape(rows, 2 * tok)
                    t = dot_nn(go[ms, :], w)
                    r = t if r is None else r + t
            else:
                r = dot_nn(go[ms, :], pick[q])
            r0, r1 = r[:, 0:tok], r[:, tok:2 * tok]
            part[di, ms, :] = jnp.where(c == 0, r0, r1)
            spare[sp, ms, :] = jnp.where(c == 0, r1, r0)
            return carry

        lax.fori_loop(0, n_cols // step, body, 0)
        twin_wait_s[sp] = send(spare.at[sp], sib.at[a, di], rsb_s.at[a, di], rsb_r.at[a, di], twin)
        if a == 1:
            t = dot_nn(mgt[...], pick[q])
            t = t[0:8] + t[8:16] + t[16:24]
            dgp[q] = jnp.where(c == 0, t[:, 0:tok], t[:, tok:2 * tok])
            dgt[q] = jnp.where(c == 0, t[:, tok:2 * tok], t[:, 0:tok])

    hd = n_cols // 2

    def mine(d, h):
        return part.at[place[d], pl.ds(h * hd, hd)]

    seen = set()

    def twin_part_wait(a, d):
        di = place[d]
        if (a, di) not in seen:
            seen.add((a, di))
            landed(sib.at[a, di], rsb_s.at[a, di], rsb_r.at[a, di], twin)

    def items(r):
        near, other = (0, 1) if r == 0 else (1, 0)
        out = [(far, near)]
        for d in range(far - 1, 0, -1):
            out += [(d, other), (d, near)]
        return out

    def ring_send(a, i, r):
        d, h = items(r)[i]
        sd = d if r == 0 else -d
        di = place[sd]
        twin_part_wait(a, sd)
        ref = mine(sd, h)
        total = ref[...] + sib[a, di, h * hd:(h + 1) * hd, :]
        if (d + 1, h) in items(r):
            p = items(r).index((d + 1, h))
            landed(ring.at[a, r, p], rs_s.at[a, r, p], rs_r.at[a, r, p], side[r])
            total = total + ring[a, r, p]
        ref[...] = total
        own_wait.setdefault(di, []).append(send(ref, ring.at[a, r, i], rs_s.at[a, r, i], rs_r.at[a, r, i], side[r]))

    def ring_send2(a, i):
        ring_send(a, i, 0)
        ring_send(a, i, 1)

    def finish(a, src, dst):
        twin_part_wait(a, 0)
        for h in range(2):
            total = mine(0, h)[...] + sib[a, place[0], h * hd:(h + 1) * hd, :]
            for r in range(2):
                p = items(r).index((1, h))
                landed(ring.at[a, r, p], rs_s.at[a, r, p], rs_r.at[a, r, p], side[r])
                total = total + ring[a, r, p]
            for j in range(hd // tok):
                cs = slice(h * hd + j * tok, h * hd + (j + 1) * tok)
                dst[:, cs] = (src[:, cs].astype(F32) + jnp.transpose(total[j * tok:(j + 1) * tok, :])).astype(BF16)

    def backward_pair(e0):
        def body(i, carry):
            e = e0 + i
            es = esl(e)
            dyr = gy[es, :].astype(F32)
            gc = gcol[es, :]
            dg = jnp.sum(dyr * orow[es, :].astype(F32), axis=1, keepdims=True)
            gcol[es, :] = jnp.broadcast_to(dg, (cap, tok))
            g = (jnp.concatenate([gc] * (n_cols // tok), axis=1) * dyr).astype(BF16)
            gy[es, :] = g
            dh = dot_nt(g, w2[e]).astype(BF16)
            da = (dh.astype(F32) * slope[es, :]).astype(BF16)
            dact[es, :] = da
            orow[es, :] = dot_nt(da, w1[e]).astype(BF16)
            return carry
        lax.fori_loop(0, 2, body, 0)

    def gate_cols(i, carry):
        sl = pl.ds(pl.multiple_of(i * tok, tok), tok)
        d = jnp.transpose(gcol[sl, :])[0:8, :]
        hi, mid, lo = split3(jnp.where(hitm[:, sl] > 0.0, d, 0.0))
        mgt[:, sl] = jnp.concatenate([hi, mid, lo, jnp.zeros_like(hi)], axis=0).astype(BF16)
        return carry

    ff = w1.shape[2]
    g1, g2 = n_cols // tile, ff // tile

    def weight_copies(e):
        lo = pl.multiple_of(ff * (e % 2), ff)
        out = []
        for s in range(g2):
            out.append(pltpu.make_async_copy(dya.at[g2 * e + s], dw2_hbm.at[e, pl.ds(s * tile, tile)], dw_sem.at[0, e, s]))
        for s in range(g1):
            out.append(pltpu.make_async_copy(xa.at[g1 * (e // 2) + s, :, pl.ds(lo, ff)],
                                             dw1_hbm.at[e, pl.ds(s * tile, tile)], dw_sem.at[1, e, s]))
        return out

    def weight_pair(e0):
        def body(i, carry):
            e = e0 + i
            es = esl(e)
            lo = pl.multiple_of(ff * (e % 2), ff)
            for s in range(g2):
                dya[g2 * e + s] = dot_tn(hid[es, s * tile:(s + 1) * tile], gy[es, :]).astype(BF16)
            for s in range(g1):
                xa[g1 * (e // 2) + s, :, pl.ds(lo, ff)] = dot_tn(brow[es, s * tile:(s + 1) * tile], dact[es, :]).astype(BF16)
            for cp in weight_copies(e):
                cp.start()
            return carry
        lax.fori_loop(0, 2, body, 0)

    lax.fori_loop(0, n_cols // tok, flip_rows, 0)
    poll2(1, 3, 0)
    for cp in pending[0]:
        cp.wait_send()
    chunk(0, far)
    poll2(1, 3, 1)
    chunk(0, 3)
    ring_send2(0, 0)
    chunk(0, -3)
    ring_send(0, 1, 0)
    poll2(1, 4, 0)
    poll2(1, 4, 1)
    chunk(0, 2)
    ring_send(0, 1, 1)
    chunk(0, -2)
    ring_send(0, 2, 0)
    chunk(0, 1)
    ring_send(0, 2, 1)
    ring_send2(0, 3)
    chunk(0, -1)
    gather(1, (0, 1, -1, 2), True)
    ring_send2(0, 4)
    chunk(0, 0)
    gather(1, (-2, 3, -3, 4))
    ring_send2(0, 5)
    backward_pair(0)
    backward_pair(2)
    lax.fori_loop(0, blocks, gate_cols, 0)
    lax.fori_loop(0, n_cols // tok, flip_rows, 0)
    ring_send2(0, 6)
    chunk(1, far)
    chunk(1, 3)
    ring_send2(1, 0)
    chunk(1, -3)
    chunk(1, 2)
    ring_send2(1, 1)
    finish(0, xs, xs)
    emit(0, xs, y_hbm)
    chunk(1, -2)
    chunk(1, 1)
    ring_send2(1, 2)
    chunk(1, -1)
    chunk(1, 0)
    dg_cp = send(dgt, dgs, dgb_s.at[0], dgb_r.at[0], twin)
    ring_send2(1, 3)
    for cp in pending[1]:
        cp.wait_send()
    landed(dgs, dgb_s.at[0], dgb_r.at[0], twin)
    dgp[...] = dgp[...] + dgs[...]
    dg_sends = [send(dgp.at[chip(d)], dgr.at[z], dg_s.at[d], dg_r.at[d], dev(chip(d), c)) for d in range(1, chips)]
    weight_pair(0)
    ring_send2(1, 4)
    weight_pair(2)
    ring_send2(1, 5)
    dg_total = dgp[z]
    for d in range(1, chips):
        landed(dgr.at[chip(-d)], dg_s.at[d], dg_r.at[d], twin)
        dg_total = dg_total + dgr[chip(-d)]
    dgr[z] = dg_total
    emit(2, dgr.at[z], dg_hbm)
    ring_send2(1, 6)
    dg_cp.wait_send()
    for cp in dg_sends:
        cp.wait_send()
    for e in range(n_exp):
        for cp in weight_copies(e):
            cp.wait()
    finish(1, ys, ys)
    emit(1, ys, dx_hbm)
    for group in (list(twin_wait_s.values()), *own_wait.values()):
        for cp in group:
            cp.wait_send()
    for cp in outs:
        cp.wait()


def copy_kernel(n, *refs):
    ins, outs, bufs, sem = refs[:n], refs[n:2 * n], refs[2 * n:3 * n], refs[3 * n]
    jobs = []
    for k in range(n - 1, -1, -1):
        if ins[k].ndim == 3:
            jobs += [(k, e, ins[k].at[e], outs[k].at[e], bufs[k].at[e]) for e in range(ins[k].shape[0])]
        else:
            jobs.append((k, 0, ins[k], outs[k], bufs[k]))
    loads = [pltpu.make_async_copy(i, b, sem.at[0, k, e]) for k, e, i, o, b in jobs]
    stores = [pltpu.make_async_copy(b, o, sem.at[1, k, e]) for k, e, i, o, b in jobs]
    for cp in loads:
        cp.start()
    for ld, st in zip(loads, stores):
        ld.wait()
        st.start()
    for cp in stores:
        cp.wait()


def solution(mesh):
    groups = mesh.shape['expert']
    tok_spec = P(('data', 'expert'), None)
    weight_spec = P('expert', None, None)
    grad_spec = P(('data', 'expert'), None, None)

    def device_pass(x_in, expert_idx, gate_weight, grad_y, w_in, w_out):
        tok, top_k = expert_idx.shape
        n_exp, dm, ff = w_in.shape
        n_pairs = tok * top_k
        cap = (CAP_NUM * n_pairs) // (CAP_DEN * n_exp)
        rows = n_exp * cap
        chips = groups // 2
        hbm = pl.BlockSpec(memory_space=pl.ANY)
        dma = pltpu.SemaphoreType.DMA
        shape = jax.ShapeDtypeStruct
        outs = (shape((tok, dm), BF16), shape((tok, dm), BF16), shape((top_k, tok), F32),
                shape((n_exp, dm, ff), BF16), shape((n_exp, ff, dm), BF16))
        mids = pl.pallas_call(
            functools.partial(moe_kernel, chips, cap, n_exp),
            name='moe',
            out_shape=outs,
            in_specs=[hbm] * 6,
            out_specs=(hbm,) * 5,
            scratch_shapes=[
                pltpu.VMEM((tok, dm), BF16),
                pltpu.VMEM((tok, dm), BF16),
                pltpu.VMEM((2, chips, top_k, tok), jnp.int32),
                pltpu.VMEM((2, chips, top_k, tok), F32),
                pltpu.VMEM((chips, 2 * tok, dm), BF16),
                pltpu.VMEM((chips, 2 * tok, dm), BF16),
                pltpu.VMEM((2 * chips, 8, tok), F32),
                pltpu.VMEM((2 * chips, 8, tok), F32),
                pltpu.VMEM((chips, 48, 2 * tok), BF16),
                pltpu.VMEM((48, rows), F32),
                pltpu.VMEM((8, rows), F32),
                pltpu.VMEM((8, rows), F32),
                pltpu.VMEM((rows, tok), F32),
                pltpu.VMEM((3, rows, tok), BF16),
                pltpu.VMEM((rows, dm), BF16),
                pltpu.VMEM((rows, dm), BF16),
                pltpu.VMEM((rows, ff), BF16),
                pltpu.VMEM((rows, ff), F32),
                pltpu.VMEM((rows, dm), BF16),
                pltpu.VMEM((rows, ff), BF16),
                pltpu.VMEM((chips, rows, 2 * tok), BF16),
                pltpu.VMEM((dm, rows), BF16),
                pltpu.VMEM((chips, dm, tok), F32),
                pltpu.VMEM((4, dm, tok), F32),
                pltpu.VMEM((2, chips, dm, tok), F32),
                pltpu.VMEM((2, 2, chips - 1, dm // 2, tok), F32),
                pltpu.VMEM((32, rows), BF16),
                pltpu.VMEM((chips, 8, tok), F32),
                pltpu.VMEM((chips, 8, tok), F32),
                pltpu.VMEM((chips, 8, tok), F32),
                pltpu.VMEM((chips, 8, tok), F32),
                pltpu.VMEM((n_exp, dm, ff), BF16),
                pltpu.VMEM((n_exp, ff, dm), BF16),
                dma((2, 2, chips - 1)), dma((2, 2, chips - 1)),
                dma((2, chips, 2)), dma((2, chips, 2)),
                dma((2, chips)), dma((2, chips)), dma((2,)), dma((2,)),
                dma((2, 2, chips - 1)), dma((2, 2, chips - 1)),
                dma((2, chips)), dma((2, chips)),
                dma((chips,)), dma((chips,)), dma((1,)), dma((1,)),
                dma((6,)), dma((2, n_exp)), dma((3,)), dma((2, n_exp, 4)),
            ],
            compiler_params=pltpu.CompilerParams(collective_id=0, has_side_effects=True,
                                                 vmem_limit_bytes=VMEM_BYTES),
        )(expert_idx.T, gate_weight.T, x_in, grad_y, w_in, w_out)
        y, dx, dg, dw1, dw2 = pl.pallas_call(
            functools.partial(copy_kernel, len(outs)),
            name='outputs',
            out_shape=outs,
            in_specs=[hbm] * len(outs),
            out_specs=(hbm,) * len(outs),
            scratch_shapes=[pltpu.VMEM(o.shape, o.dtype) for o in outs] + [dma((2, len(outs), n_exp))],
        )(*mids)
        return y, dx, dg.T, dw1, dw2

    return jax.shard_map(device_pass, mesh=mesh,
                         in_specs=(tok_spec, tok_spec, tok_spec, tok_spec, weight_spec, weight_spec),
                         out_specs=(tok_spec, tok_spec, tok_spec, grad_spec, grad_spec), check_vma=False)
```

```python
import functools

import jax
import jax.numpy as jnp
from jax import lax
from jax.experimental import pallas as pl
from jax.experimental.pallas import tpu as pltpu
from jax.sharding import PartitionSpec as P

CAP_NUM = 5
CAP_DEN = 4
BIG = 3.3e38
F32 = jnp.float32
BF16 = jnp.bfloat16
K0 = 0.7978845608028654
K1 = 0.044715
MESH = pl.DeviceIdType.MESH
VMEM_BYTES = 57_900_000


def split3(v):
    hi = jnp.clip(v, -BIG, BIG).astype(BF16).astype(F32)
    rest = v - hi
    mid = rest.astype(BF16).astype(F32)
    lo = (rest - mid).astype(BF16).astype(F32)
    return hi, mid, lo


def gelu_and_slope(a):
    t = jnp.tanh(K0 * (a + K1 * (a * a * a)))
    cdf = 0.5 * (1.0 + t)
    return a * cdf, cdf + a * (0.5 * (1.0 - t * t)) * (K0 * (1.0 + 3.0 * K1 * (a * a)))


def dot_nn(a, b):
    return lax.dot_general(a, b, (((1,), (0,)), ((), ())), preferred_element_type=F32)


def dot_nt(a, b):
    return lax.dot_general(a, b, (((1,), (1,)), ((), ())), preferred_element_type=F32)


def dot_tn(a, b):
    return lax.dot_general(a, b, (((0,), (0,)), ((), ())), preferred_element_type=F32)


def moe_kernel(chips, cap, n_exp,
               idx_hbm, gate_hbm, x_hbm, dy_hbm, w1_hbm, w2_hbm,
               xs, ys, dgs, xa, dya,
               idx_all, gate_all, vt, cnt, tab, ft, hitm, grow, gcol, gpart, brow, gy, hid, slope, orow, dact,
               pick, go, part, spare, sib, ring, mgt, dgp, dgt, dgr, w1, w2,
               ag_s, ag_r, agb_s, agb_r, in_s, in_r, inb_s, inb_r, rs_s, rs_r, rsb_s, rsb_r,
               dg_s, dg_r, dgb_s, dgb_r, l_sem, w_sem):
    top_k, tok = idx_all.shape[2:]
    half = tok // 2
    rows = n_exp * cap
    me = lax.axis_index('expert')
    z = me // 2
    c = me % 2
    far = chips // 2

    def chip(d):
        return (z + d + chips) % chips

    def dev(q, k):
        return {'expert': q * 2 + k}

    right, left, twin = dev(chip(1), c), dev(chip(-1), c), {'expert': z * 2 + 1 - c}
    side = (right, left)
    pending = ([], [])
    def rcopy(src, dst, ss, rs, to):
        return pltpu.make_async_remote_copy(src_ref=src, dst_ref=dst, send_sem=ss, recv_sem=rs,
                                            device_id=to, device_id_type=MESH)

    def send(src, dst, ss, rs, to):
        cp = rcopy(src, dst, ss, rs, to)
        cp.start()
        return cp

    def landed(dst, ss, rs, to):
        rcopy(dst, dst, ss, rs, to).wait_recv()

    own_rows = pl.ds(pl.multiple_of(c * tok, tok), tok)
    inputs = []
    for k, (src, dst) in enumerate(((idx_hbm, idx_all.at[c, z]), (gate_hbm, gate_all.at[c, z]), (x_hbm, xs), (dy_hbm, ys),
                                    (x_hbm, xa.at[z, own_rows]), (dy_hbm, dya.at[z, own_rows]))):
        cp = pltpu.make_async_copy(src, dst, l_sem.at[k])
        cp.start()
        inputs.append(cp)

    barrier = pltpu.get_barrier_semaphore()
    for d in sorted(range(1, chips), key=lambda d: -min(d, chips - d)):
        pl.semaphore_signal(barrier, inc=1, device_id=dev(chip(d), c), device_id_type=MESH)
    pl.semaphore_signal(barrier, inc=1, device_id=twin, device_id_type=MESH)

    loads = []
    for e in range(n_exp):
        for k, (src, dst) in enumerate(((w1_hbm, w1), (w2_hbm, w2))):
            cp = pltpu.make_async_copy(src.at[e], dst.at[e], w_sem.at[k, e])
            cp.start()
            loads.append(cp)
    for cp in inputs:
        cp.wait()
    pl.semaphore_wait(barrier, chips)

    bufs = (xa, dya)
    own = (xs, ys)

    def item(k, h):
        return 2 * (k - 1) + h if k < far else 2 * (far - 1)

    def slot(a, q, h, k=None):
        kk = c if k is None else k
        return bufs[a].at[q, pl.ds(pl.multiple_of(kk * tok + h * half, half), half)]

    def twin_send(a, d, h, src):
        di = d % chips
        pending[a].append(send(src, slot(a, chip(d), h), agb_s.at[a, di, h], agb_r.at[a, di, h], twin))

    def twin_wait(a, d):
        di = d % chips
        for h in range(2):
            landed(slot(a, chip(d), h, 1 - c), agb_s.at[a, di, h], agb_r.at[a, di, h], twin)

    def first_send(a, h):
        src = own[a].at[pl.ds(h * half, half)]
        for r in range(2):
            i = item(1, h)
            pending[a].append(send(src, slot(a, z, h), ag_s.at[a, r, i], ag_r.at[a, r, i], side[r]))

    def poll(a, k, h, r):
        q = chip(-k) if r == 0 else chip(k)
        i = item(k, h)
        here = slot(a, q, h)
        landed(here, ag_s.at[a, r, i], ag_r.at[a, r, i], side[r])
        if k + 1 < far or (k + 1 == far and h == r):
            j = item(k + 1, h)
            pending[a].append(send(here, slot(a, q, h), ag_s.at[a, r, j], ag_r.at[a, r, j], side[r]))
        twin_send(a, (-k if r == 0 else k), h, here)

    def poll2(a, k, h):
        if k == far:
            poll(a, k, h, h)
        else:
            poll(a, k, h, 0)
            poll(a, k, h, 1)

    small = (idx_all, gate_all)
    for d in range(1, chips):
        for s, dst in enumerate(small):
            pending[1].append(send(dst.at[c, z], dst.at[c, z], in_s.at[s, d], in_r.at[s, d], dev(chip(d), c)))
    first_send(0, 0)
    first_send(0, 1)
    first_send(1, 0)
    for a in range(2):
        for h in range(2):
            twin_send(a, 0, h, own[a].at[pl.ds(h * half, half)])
    for s, dst in enumerate(small):
        for d in range(1, chips):
            landed(dst.at[c, chip(-d)], in_s.at[s, d], in_r.at[s, d], twin)
        pending[1].append(send(dst.at[c], dst.at[c], inb_s.at[s], inb_r.at[s], twin))
    poll2(0, 1, 0)
    for s, dst in enumerate(small):
        landed(dst.at[1 - c], inb_s.at[s], inb_r.at[s], twin)

    first_e = (me * n_exp).astype(F32)
    sub8 = lax.broadcasted_iota(jnp.int32, (8, tok), 0)

    def count_block(b, carry):
        k, q = b // chips, b % chips
        loc = idx_all[k, q].astype(F32) - first_e
        for e in range(n_exp):
            s = jnp.sum(jnp.where(loc == e, 1.0, 0.0), axis=0, keepdims=True)
            cnt[b, e:e + 1, :] = s
            cnt[b, n_exp + e:n_exp + e + 1, :] = s
        return carry

    lax.fori_loop(0, 2 * chips, count_block, 0)
    cmat = cnt[...].reshape(2 * chips * 8, tok)
    ri = lax.broadcasted_iota(jnp.int32, (tok, tok), 0)
    ci = lax.broadcasted_iota(jnp.int32, (tok, tok), 1)
    upper = jnp.where(ri < ci, 1.0, 0.0).astype(BF16)
    rb, cb = ri // 8, ci // 8
    r_ord, c_ord = 2 * (rb % chips) + rb // chips, 2 * (cb % chips) + cb // chips
    prior = jnp.where((c_ord < r_ord) & (ri % 8 == ci % 8), 1.0, 0.0).astype(BF16)
    cbf = cmat.astype(BF16)
    start = dot_nn(cbf, upper) + jnp.sum(dot_nn(prior, cbf), axis=1, keepdims=True)
    cnt[...] = start.reshape(2 * chips, 8, tok)
    row8 = ri % 8
    edge = jnp.where(row8 < n_exp, start, start + cmat)
    edge = jnp.minimum(edge, float(cap)) + (row8 % n_exp).astype(F32) * cap
    vt[...] = edge.reshape(2 * chips, 8, tok)
    poll2(0, 1, 1)

    def table_block(b, carry):
        k, q = b // chips, b % chips
        idx = idx_all[k, q].astype(F32)
        loc = idx - first_e
        at = jnp.zeros((top_k, tok), F32)
        for e in range(n_exp):
            at = at + jnp.where(loc == e, cnt[b, e:e + 1, :], 0.0)
        for j in range(top_k - 1):
            at = at + jnp.where((idx[j:j + 1, :] == idx) & (sub8 > j), 1.0, 0.0)
        ok = (loc >= 0.0) & (loc < n_exp) & (at < cap)
        rr = loc * cap + at
        coarse = jnp.floor(rr * 0.125)
        hi, mid, lo = split3(gate_all[k, q])
        code = jnp.where(ok, coarse - rows // 16, 200.0)
        fine = jnp.where(ok, rr - 8.0 * coarse, 0.0)
        tile = jnp.concatenate([hi, mid, lo, code, fine, jnp.zeros((8, tok), F32)], axis=0)
        tab[q, :, pl.ds(pl.multiple_of(k * tok, tok), tok)] = tile.astype(BF16)
        return carry

    lax.fori_loop(0, 2 * chips, table_block, 0)

    def esl(e):
        return pl.ds(pl.multiple_of(e * cap, cap), cap)

    ft[...] = jnp.zeros_like(ft)

    def pick_block(q, carry):
        for e in range(n_exp):
            r = (lax.broadcasted_iota(jnp.int32, (cap, tok), 0) + e * cap).astype(F32)
            out = []
            for k in range(2):
                b = k * chips + q
                out.append(jnp.where((r >= vt[b, e:e + 1, :]) & (r < vt[b, n_exp + e:n_exp + e + 1, :]), 1.0, 0.0).astype(BF16))
            pick[q, e * cap:(e + 1) * cap, :] = jnp.concatenate(out, axis=1)
        ft[...] = ft[...] + dot_nt(tab[q], pick[q])
        return carry

    lax.fori_loop(0, chips // 2, pick_block, 0)
    poll2(0, 2, 0)
    lax.fori_loop(chips // 2, chips, pick_block, 0)
    poll2(0, 2, 1)
    first_send(1, 1)

    r8 = lax.broadcasted_iota(jnp.int32, (top_k, rows), 1)
    hit = (ft[24:32, :] == ((r8 >> 3) - rows // 16).astype(F32)) & (ft[32:40, :] == (r8 & 7).astype(F32))
    val = ft[0:8, :] + ft[8:16, :] + ft[16:24, :]
    hitm[...] = jnp.where(hit, 1.0, 0.0)
    grow[...] = jnp.broadcast_to(jnp.sum(jnp.where(hit, val, 0.0), axis=0, keepdims=True), (8, rows))

    def gate_col(i, carry):
        sl = pl.ds(pl.multiple_of(i * tok, tok), tok)
        v = jnp.transpose(jnp.broadcast_to(grow[0:1, sl], (tok, tok)))
        gcol[sl, :] = v
        for s, w in enumerate(split3(v)):
            gpart[s, sl, :] = w.astype(BF16)
        return carry

    lax.fori_loop(0, rows // tok, gate_col, 0)

    def gather(a, ds, first=False):
        for d in ds:
            twin_wait(a, d)
        dst = brow if a == 0 else gy

        def body(e, carry):
            r = None
            for d in ds:
                q = chip(d)
                t = dot_nn(pick[q, esl(e), :], bufs[a][q])
                r = t if r is None else r + t
            r = r.astype(BF16)
            dst[esl(e), :] = r if first else dst[esl(e), :] + r
            return carry

        lax.fori_loop(0, n_exp, body, 0)

    gather(0, (0, 1, -1), True)
    poll2(0, 3, 0)
    gather(0, (2, -2))
    poll2(0, 3, 1)
    poll2(1, 1, 0)
    poll2(0, 4, 0)
    poll2(0, 4, 1)
    poll2(1, 1, 1)
    gather(0, (3, -3, 4))

    for cp in loads:
        cp.wait()

    def forward_pair(e0):
        def body(i, carry):
            e = e0 + i
            act, sl = gelu_and_slope(dot_nn(brow[esl(e), :], w1[e]))
            hb = act.astype(BF16)
            hid[esl(e), :] = hb
            slope[esl(e), :] = sl
            orow[esl(e), :] = dot_nn(hb, w2[e]).astype(BF16)
            return carry
        lax.fori_loop(0, 2, body, 0)

    forward_pair(0)
    poll2(1, 2, 0)
    forward_pair(2)
    poll2(1, 2, 1)

    order = [far]
    for d in range(far - 1, 0, -1):
        order += [d, -d]
    order.append(0)
    place = {d: i for i, d in enumerate(order)}
    place[-far] = 0
    own_wait, twin_wait_s = {}, {}
    n_cols = xs.shape[1]
    tile = xa.shape[1]
    step = 2 * tile
    blocks = rows // tok

    def mtile(m):
        return pl.ds(pl.multiple_of(m * step, step), step)

    def flip_rows(j, carry):
        js = pl.ds(pl.multiple_of(j * tok, tok), tok)
        for i in range(blocks):
            go[js, i * tok:(i + 1) * tok] = jnp.transpose(orow[i * tok:(i + 1) * tok, js])
        return carry

    def chunk(a, d):
        q, di = chip(d), place[d]
        sp = di % spare.shape[0]
        for cp in own_wait.pop(di, []):
            cp.wait_send()
        if sp in twin_wait_s:
            twin_wait_s.pop(sp).wait_send()

        per = tile // tok
        if a == 0:
            def scale(i, carry):
                sl = pl.ds(pl.multiple_of(i * tok, tok), tok)
                sub = pl.ds(pl.multiple_of((i % per) * tok, tok), tok)
                for s in range(3):
                    g = gpart[s, sl, :]
                    xa[i // per, sub, s * 2 * tok:(s + 1) * 2 * tok] = pick[q, sl, :] * jnp.concatenate([g, g], axis=1)
                return carry
            lax.fori_loop(0, blocks, scale, 0)

        def body(m, carry):
            ms = mtile(m)
            if a == 0:
                r = None
                for s in range(3):
                    w = xa[0:rows // tile, :, s * 2 * tok:(s + 1) * 2 * tok].reshape(rows, 2 * tok)
                    t = dot_nn(go[ms, :], w)
                    r = t if r is None else r + t
            else:
                r = dot_nn(go[ms, :], pick[q])
            r0, r1 = r[:, 0:tok], r[:, tok:2 * tok]
            part[di, ms, :] = jnp.where(c == 0, r0, r1)
            spare[sp, ms, :] = jnp.where(c == 0, r1, r0)
            return carry

        lax.fori_loop(0, n_cols // step, body, 0)
        twin_wait_s[sp] = send(spare.at[sp], sib.at[a, di], rsb_s.at[a, di], rsb_r.at[a, di], twin)
        if a == 1:
            t = dot_nn(mgt[...], pick[q])
            t = t[0:8] + t[8:16] + t[16:24]
            dgp[q] = jnp.where(c == 0, t[:, 0:tok], t[:, tok:2 * tok])
            dgt[q] = jnp.where(c == 0, t[:, tok:2 * tok], t[:, 0:tok])

    hd = n_cols // 2

    def mine(d, h):
        return part.at[place[d], pl.ds(h * hd, hd)]

    seen = set()

    def twin_part_wait(a, d):
        di = place[d]
        if (a, di) not in seen:
            seen.add((a, di))
            landed(sib.at[a, di], rsb_s.at[a, di], rsb_r.at[a, di], twin)

    def items(r):
        near, other = (0, 1) if r == 0 else (1, 0)
        out = [(far, near)]
        for d in range(far - 1, 0, -1):
            out += [(d, other), (d, near)]
        return out

    def ring_send(a, i, r):
        d, h = items(r)[i]
        sd = d if r == 0 else -d
        di = place[sd]
        twin_part_wait(a, sd)
        ref = mine(sd, h)
        total = ref[...] + sib[a, di, h * hd:(h + 1) * hd, :]
        if (d + 1, h) in items(r):
            p = items(r).index((d + 1, h))
            landed(ring.at[a, r, p], rs_s.at[a, r, p], rs_r.at[a, r, p], side[r])
            total = total + ring[a, r, p]
        ref[...] = total
        own_wait.setdefault(di, []).append(send(ref, ring.at[a, r, i], rs_s.at[a, r, i], rs_r.at[a, r, i], side[r]))

    def ring_send2(a, i):
        ring_send(a, i, 0)
        ring_send(a, i, 1)

    def finish(a, src, dst):
        twin_part_wait(a, 0)
        for h in range(2):
            total = mine(0, h)[...] + sib[a, place[0], h * hd:(h + 1) * hd, :]
            for r in range(2):
                p = items(r).index((1, h))
                landed(ring.at[a, r, p], rs_s.at[a, r, p], rs_r.at[a, r, p], side[r])
                total = total + ring[a, r, p]
            for j in range(hd // tok):
                cs = slice(h * hd + j * tok, h * hd + (j + 1) * tok)
                dst[:, cs] = (src[:, cs].astype(F32) + jnp.transpose(total[j * tok:(j + 1) * tok, :])).astype(BF16)

    def backward_pair(e0):
        def body(i, carry):
            e = e0 + i
            es = esl(e)
            dyr = gy[es, :].astype(F32)
            gc = gcol[es, :]
            dg = jnp.sum(dyr * orow[es, :].astype(F32), axis=1, keepdims=True)
            gcol[es, :] = jnp.broadcast_to(dg, (cap, tok))
            g = (jnp.concatenate([gc] * (n_cols // tok), axis=1) * dyr).astype(BF16)
            gy[es, :] = g
            dh = dot_nt(g, w2[e]).astype(BF16)
            da = (dh.astype(F32) * slope[es, :]).astype(BF16)
            dact[es, :] = da
            orow[es, :] = dot_nt(da, w1[e]).astype(BF16)
            return carry
        lax.fori_loop(0, 2, body, 0)

    def gate_cols(i, carry):
        sl = pl.ds(pl.multiple_of(i * tok, tok), tok)
        d = jnp.transpose(gcol[sl, :])[0:8, :]
        hi, mid, lo = split3(jnp.where(hitm[:, sl] > 0.0, d, 0.0))
        mgt[:, sl] = jnp.concatenate([hi, mid, lo, jnp.zeros_like(hi)], axis=0).astype(BF16)
        return carry

    ff = w1.shape[2]
    g1, g2 = n_cols // tile, ff // tile

    def weight_pair(e0):
        def body(i, carry):
            e = e0 + i
            es = esl(e)
            lo = pl.multiple_of(ff * (e % 2), ff)
            for s in range(g2):
                dya[g2 * e + s] = dot_tn(hid[es, s * tile:(s + 1) * tile], gy[es, :]).astype(BF16)
            for s in range(g1):
                xa[g1 * (e // 2) + s, :, pl.ds(lo, ff)] = dot_tn(brow[es, s * tile:(s + 1) * tile], dact[es, :]).astype(BF16)
            return carry
        lax.fori_loop(0, 2, body, 0)

    lax.fori_loop(0, n_cols // tok, flip_rows, 0)
    poll2(1, 3, 0)
    for cp in pending[0]:
        cp.wait_send()
    chunk(0, far)
    poll2(1, 3, 1)
    chunk(0, 3)
    ring_send2(0, 0)
    chunk(0, -3)
    ring_send(0, 1, 0)
    poll2(1, 4, 0)
    poll2(1, 4, 1)
    chunk(0, 2)
    ring_send(0, 1, 1)
    chunk(0, -2)
    ring_send(0, 2, 0)
    chunk(0, 1)
    ring_send(0, 2, 1)
    ring_send2(0, 3)
    chunk(0, -1)
    gather(1, (0, 1, -1, 2), True)
    ring_send2(0, 4)
    chunk(0, 0)
    gather(1, (-2, 3, -3, 4))
    ring_send2(0, 5)
    backward_pair(0)
    backward_pair(2)
    lax.fori_loop(0, blocks, gate_cols, 0)
    lax.fori_loop(0, n_cols // tok, flip_rows, 0)
    ring_send2(0, 6)
    chunk(1, far)
    chunk(1, 3)
    ring_send2(1, 0)
    chunk(1, -3)
    chunk(1, 2)
    ring_send2(1, 1)
    finish(0, xs, xs)
    chunk(1, -2)
    chunk(1, 1)
    ring_send2(1, 2)
    chunk(1, -1)
    chunk(1, 0)
    dg_cp = send(dgt, dgs, dgb_s.at[0], dgb_r.at[0], twin)
    ring_send2(1, 3)
    for cp in pending[1]:
        cp.wait_send()
    landed(dgs, dgb_s.at[0], dgb_r.at[0], twin)
    dgp[...] = dgp[...] + dgs[...]
    dg_sends = [send(dgp.at[chip(d)], dgr.at[z], dg_s.at[d], dg_r.at[d], dev(chip(d), c)) for d in range(1, chips)]
    weight_pair(0)
    ring_send2(1, 4)
    weight_pair(2)
    ring_send2(1, 5)
    dg_total = dgp[z]
    for d in range(1, chips):
        landed(dgr.at[chip(-d)], dg_s.at[d], dg_r.at[d], twin)
        dg_total = dg_total + dgr[chip(-d)]
    dgs[0] = dg_total
    ring_send2(1, 6)
    dg_cp.wait_send()
    for cp in dg_sends:
        cp.wait_send()
    finish(1, ys, ys)
    for group in (list(twin_wait_s.values()), *own_wait.values()):
        for cp in group:
            cp.wait_send()


def copy_kernel(xs, ys, dgs, xa, dya, y, dx, dg, dw1, dw2, sem):
    n_exp, n_cols, ff = dw1.shape
    tile = xa.shape[1]
    g1, g2 = n_cols // tile, ff // tile
    jobs = [(xs, y), (ys, dx), (dgs.at[0], dg)]
    for e in range(n_exp):
        lo = ff * (e % 2)
        jobs += [(dya.at[g2 * e + s], dw2.at[e, pl.ds(s * tile, tile)]) for s in range(g2)]
        jobs += [(xa.at[g1 * (e // 2) + s, :, pl.ds(lo, ff)], dw1.at[e, pl.ds(s * tile, tile)]) for s in range(g1)]
    copies = [pltpu.make_async_copy(a, b, sem.at[k]) for k, (a, b) in enumerate(jobs)]
    for cp in copies:
        cp.start()
    for cp in copies:
        cp.wait()


def solution(mesh):
    groups = mesh.shape['expert']
    tok_spec = P(('data', 'expert'), None)
    weight_spec = P('expert', None, None)
    grad_spec = P(('data', 'expert'), None, None)

    def device_pass(x_in, expert_idx, gate_weight, grad_y, w_in, w_out):
        tok, top_k = expert_idx.shape
        n_exp, dm, ff = w_in.shape
        n_pairs = tok * top_k
        cap = (CAP_NUM * n_pairs) // (CAP_DEN * n_exp)
        rows = n_exp * cap
        chips = groups // 2
        hbm = pl.BlockSpec(memory_space=pl.ANY)
        dma = pltpu.SemaphoreType.DMA
        shape = jax.ShapeDtypeStruct
        outs = (shape((tok, dm), BF16), shape((tok, dm), BF16), shape((top_k, tok), F32),
                shape((n_exp, dm, ff), BF16), shape((n_exp, ff, dm), BF16))
        vmem = pl.BlockSpec(memory_space=pltpu.VMEM)
        mids = (pltpu.VMEM((tok, dm), BF16), pltpu.VMEM((tok, dm), BF16), pltpu.VMEM((chips, top_k, tok), F32),
                pltpu.VMEM((chips, 2 * tok, dm), BF16), pltpu.VMEM((chips, 2 * tok, dm), BF16))
        held = pl.pallas_call(
            functools.partial(moe_kernel, chips, cap, n_exp),
            name='moe',
            out_shape=mids,
            in_specs=[hbm] * 6,
            out_specs=(vmem,) * 5,
            scratch_shapes=[
                pltpu.VMEM((2, chips, top_k, tok), jnp.int32),
                pltpu.VMEM((2, chips, top_k, tok), F32),
                pltpu.VMEM((2 * chips, 8, tok), F32),
                pltpu.VMEM((2 * chips, 8, tok), F32),
                pltpu.VMEM((chips, 48, 2 * tok), BF16),
                pltpu.VMEM((48, rows), F32),
                pltpu.VMEM((8, rows), F32),
                pltpu.VMEM((8, rows), F32),
                pltpu.VMEM((rows, tok), F32),
                pltpu.VMEM((3, rows, tok), BF16),
                pltpu.VMEM((rows, dm), BF16),
                pltpu.VMEM((rows, dm), BF16),
                pltpu.VMEM((rows, ff), BF16),
                pltpu.VMEM((rows, ff), F32),
                pltpu.VMEM((rows, dm), BF16),
                pltpu.VMEM((rows, ff), BF16),
                pltpu.VMEM((chips, rows, 2 * tok), BF16),
                pltpu.VMEM((dm, rows), BF16),
                pltpu.VMEM((chips, dm, tok), F32),
                pltpu.VMEM((4, dm, tok), F32),
                pltpu.VMEM((2, chips, dm, tok), F32),
                pltpu.VMEM((2, 2, chips - 1, dm // 2, tok), F32),
                pltpu.VMEM((32, rows), BF16),
                pltpu.VMEM((chips, 8, tok), F32),
                pltpu.VMEM((chips, 8, tok), F32),
                pltpu.VMEM((chips, 8, tok), F32),
                pltpu.VMEM((n_exp, dm, ff), BF16),
                pltpu.VMEM((n_exp, ff, dm), BF16),
                dma((2, 2, chips - 1)), dma((2, 2, chips - 1)),
                dma((2, chips, 2)), dma((2, chips, 2)),
                dma((2, chips)), dma((2, chips)), dma((2,)), dma((2,)),
                dma((2, 2, chips - 1)), dma((2, 2, chips - 1)),
                dma((2, chips)), dma((2, chips)),
                dma((chips,)), dma((chips,)), dma((1,)), dma((1,)),
                dma((6,)), dma((2, n_exp)),
            ],
            compiler_params=pltpu.CompilerParams(collective_id=0, has_side_effects=True,
                                                 vmem_limit_bytes=VMEM_BYTES),
        )(expert_idx.T, gate_weight.T, x_in, grad_y, w_in, w_out)
        y, dx, dg, dw1, dw2 = pl.pallas_call(
            copy_kernel,
            name='outputs',
            out_shape=outs,
            in_specs=[vmem] * len(mids),
            out_specs=(hbm,) * len(outs),
            scratch_shapes=[dma((3 + n_exp * (dm + ff) // (2 * tok),))],
            compiler_params=pltpu.CompilerParams(vmem_limit_bytes=1 << 20),
        )(*[pltpu.with_memory_space_constraint(v, pltpu.VMEM) for v in held])
        return y, dx, dg.T, dw1, dw2

    return jax.shard_map(device_pass, mesh=mesh,
                         in_specs=(tok_spec, tok_spec, tok_spec, tok_spec, weight_spec, weight_spec),
                         out_specs=(tok_spec, tok_spec, tok_spec, grad_spec, grad_spec), check_vma=False)
```

```python
import functools

import jax
import jax.numpy as jnp
from jax import lax
from jax.experimental import pallas as pl
from jax.experimental.pallas import tpu as pltpu
from jax.sharding import PartitionSpec as P

CAP_NUM = 5
CAP_DEN = 4
BIG = 3.3e38
F32 = jnp.float32
BF16 = jnp.bfloat16
K0 = 0.7978845608028654
K1 = 0.044715
MESH = pl.DeviceIdType.MESH
VMEM_BYTES = 57_900_000


def split3(v):
    hi = jnp.clip(v, -BIG, BIG).astype(BF16).astype(F32)
    rest = v - hi
    mid = rest.astype(BF16).astype(F32)
    lo = (rest - mid).astype(BF16).astype(F32)
    return hi, mid, lo


def gelu_and_slope(a):
    t = jnp.tanh(K0 * (a + K1 * (a * a * a)))
    cdf = 0.5 * (1.0 + t)
    return a * cdf, cdf + a * (0.5 * (1.0 - t * t)) * (K0 * (1.0 + 3.0 * K1 * (a * a)))


def dot_nn(a, b):
    return lax.dot_general(a, b, (((1,), (0,)), ((), ())), preferred_element_type=F32)


def dot_nt(a, b):
    return lax.dot_general(a, b, (((1,), (1,)), ((), ())), preferred_element_type=F32)


def dot_tn(a, b):
    return lax.dot_general(a, b, (((0,), (0,)), ((), ())), preferred_element_type=F32)


def moe_kernel(chips, cap, n_exp,
               idx_hbm, gate_hbm, x_hbm, dy_hbm, w1_hbm, w2_hbm,
               xs, ys, dgs, xa, dya,
               idx_all, gate_all, vt, cnt, tab, ft, hitm, grow, gcol, gpart, brow, gy, hid, slope, orow, dact,
               pick, go, part, spare, sib, ring, mgt, dgp, dgt, dgr, w1, w2,
               ag_s, ag_r, agb_s, agb_r, in_s, in_r, inb_s, inb_r, rs_s, rs_r, rsb_s, rsb_r,
               dg_s, dg_r, dgb_s, dgb_r, l_sem, w_sem):
    top_k, tok = idx_all.shape[2:]
    half = tok // 2
    rows = n_exp * cap
    me = lax.axis_index('expert')
    z = me // 2
    c = me % 2
    far = chips // 2

    def chip(d):
        return (z + d + chips) % chips

    def dev(q, k):
        return {'expert': q * 2 + k}

    right, left, twin = dev(chip(1), c), dev(chip(-1), c), {'expert': z * 2 + 1 - c}
    side = (right, left)
    pending = ([], [])
    def rcopy(src, dst, ss, rs, to):
        return pltpu.make_async_remote_copy(src_ref=src, dst_ref=dst, send_sem=ss, recv_sem=rs,
                                            device_id=to, device_id_type=MESH)

    def send(src, dst, ss, rs, to):
        cp = rcopy(src, dst, ss, rs, to)
        cp.start()
        return cp

    def landed(dst, ss, rs, to):
        rcopy(dst, dst, ss, rs, to).wait_recv()

    own_rows = pl.ds(pl.multiple_of(c * tok, tok), tok)
    inputs = []
    for k, (src, dst) in enumerate(((idx_hbm, idx_all.at[c, z]), (gate_hbm, gate_all.at[c, z]), (x_hbm, xs), (dy_hbm, ys),
                                    (x_hbm, xa.at[z, own_rows]), (dy_hbm, dya.at[z, own_rows]))):
        cp = pltpu.make_async_copy(src, dst, l_sem.at[k])
        cp.start()
        inputs.append(cp)

    barrier = pltpu.get_barrier_semaphore()
    for d in sorted(range(1, chips), key=lambda d: -min(d, chips - d)):
        pl.semaphore_signal(barrier, inc=1, device_id=dev(chip(d), c), device_id_type=MESH)
    pl.semaphore_signal(barrier, inc=1, device_id=twin, device_id_type=MESH)

    loads = []
    for e in range(n_exp):
        for k, (src, dst) in enumerate(((w1_hbm, w1), (w2_hbm, w2))):
            cp = pltpu.make_async_copy(src.at[e], dst.at[e], w_sem.at[k, e])
            cp.start()
            loads.append(cp)
    for cp in inputs:
        cp.wait()
    pl.semaphore_wait(barrier, chips)

    bufs = (xa, dya)
    own = (xs, ys)

    def item(k, h):
        return 2 * (k - 1) + h if k < far else 2 * (far - 1)

    def slot(a, q, h, k=None):
        kk = c if k is None else k
        return bufs[a].at[q, pl.ds(pl.multiple_of(kk * tok + h * half, half), half)]

    def twin_send(a, d, h, src):
        di = d % chips
        pending[a].append(send(src, slot(a, chip(d), h), agb_s.at[a, di, h], agb_r.at[a, di, h], twin))

    def twin_wait(a, d):
        di = d % chips
        for h in range(2):
            landed(slot(a, chip(d), h, 1 - c), agb_s.at[a, di, h], agb_r.at[a, di, h], twin)

    def first_send(a, h):
        src = own[a].at[pl.ds(h * half, half)]
        for r in range(2):
            i = item(1, h)
            pending[a].append(send(src, slot(a, z, h), ag_s.at[a, r, i], ag_r.at[a, r, i], side[r]))

    def poll(a, k, h, r):
        q = chip(-k) if r == 0 else chip(k)
        i = item(k, h)
        here = slot(a, q, h)
        landed(here, ag_s.at[a, r, i], ag_r.at[a, r, i], side[r])
        if k + 1 < far or (k + 1 == far and h == r):
            j = item(k + 1, h)
            pending[a].append(send(here, slot(a, q, h), ag_s.at[a, r, j], ag_r.at[a, r, j], side[r]))
        twin_send(a, (-k if r == 0 else k), h, here)

    def poll2(a, k, h):
        if k == far:
            poll(a, k, h, h)
        else:
            poll(a, k, h, 0)
            poll(a, k, h, 1)

    small = (idx_all, gate_all)
    for d in range(1, chips):
        for s, dst in enumerate(small):
            pending[1].append(send(dst.at[c, z], dst.at[c, z], in_s.at[s, d], in_r.at[s, d], dev(chip(d), c)))
    first_send(0, 0)
    first_send(0, 1)
    first_send(1, 0)
    for a in range(2):
        for h in range(2):
            twin_send(a, 0, h, own[a].at[pl.ds(h * half, half)])
    for s, dst in enumerate(small):
        for d in range(1, chips):
            landed(dst.at[c, chip(-d)], in_s.at[s, d], in_r.at[s, d], twin)
        pending[1].append(send(dst.at[c], dst.at[c], inb_s.at[s], inb_r.at[s], twin))
    poll2(0, 1, 0)
    for s, dst in enumerate(small):
        landed(dst.at[1 - c], inb_s.at[s], inb_r.at[s], twin)

    first_e = (me * n_exp).astype(F32)
    sub8 = lax.broadcasted_iota(jnp.int32, (8, tok), 0)

    def count_block(b, carry):
        k, q = b // chips, b % chips
        loc = idx_all[k, q].astype(F32) - first_e
        for e in range(n_exp):
            s = jnp.sum(jnp.where(loc == e, 1.0, 0.0), axis=0, keepdims=True)
            cnt[b, e:e + 1, :] = s
            cnt[b, n_exp + e:n_exp + e + 1, :] = s
        return carry

    lax.fori_loop(0, 2 * chips, count_block, 0)
    cmat = cnt[...].reshape(2 * chips * 8, tok)
    ri = lax.broadcasted_iota(jnp.int32, (tok, tok), 0)
    ci = lax.broadcasted_iota(jnp.int32, (tok, tok), 1)
    upper = jnp.where(ri < ci, 1.0, 0.0).astype(BF16)
    rb, cb = ri // 8, ci // 8
    r_ord, c_ord = 2 * (rb % chips) + rb // chips, 2 * (cb % chips) + cb // chips
    prior = jnp.where((c_ord < r_ord) & (ri % 8 == ci % 8), 1.0, 0.0).astype(BF16)
    cbf = cmat.astype(BF16)
    start = dot_nn(cbf, upper) + jnp.sum(dot_nn(prior, cbf), axis=1, keepdims=True)
    cnt[...] = start.reshape(2 * chips, 8, tok)
    row8 = ri % 8
    edge = jnp.where(row8 < n_exp, start, start + cmat)
    edge = jnp.minimum(edge, float(cap)) + (row8 % n_exp).astype(F32) * cap
    vt[...] = edge.reshape(2 * chips, 8, tok)
    poll2(0, 1, 1)

    def table_block(b, carry):
        k, q = b // chips, b % chips
        idx = idx_all[k, q].astype(F32)
        loc = idx - first_e
        at = jnp.zeros((top_k, tok), F32)
        for e in range(n_exp):
            at = at + jnp.where(loc == e, cnt[b, e:e + 1, :], 0.0)
        for j in range(top_k - 1):
            at = at + jnp.where((idx[j:j + 1, :] == idx) & (sub8 > j), 1.0, 0.0)
        ok = (loc >= 0.0) & (loc < n_exp) & (at < cap)
        rr = loc * cap + at
        coarse = jnp.floor(rr * 0.125)
        hi, mid, lo = split3(gate_all[k, q])
        code = jnp.where(ok, coarse - rows // 16, 200.0)
        fine = jnp.where(ok, rr - 8.0 * coarse, 0.0)
        tile = jnp.concatenate([hi, mid, lo, code, fine, jnp.zeros((8, tok), F32)], axis=0)
        tab[q, :, pl.ds(pl.multiple_of(k * tok, tok), tok)] = tile.astype(BF16)
        return carry

    lax.fori_loop(0, 2 * chips, table_block, 0)

    def esl(e):
        return pl.ds(pl.multiple_of(e * cap, cap), cap)

    ft[...] = jnp.zeros_like(ft)

    def pick_block(q, carry):
        for e in range(n_exp):
            r = (lax.broadcasted_iota(jnp.int32, (cap, tok), 0) + e * cap).astype(F32)
            out = []
            for k in range(2):
                b = k * chips + q
                out.append(jnp.where((r >= vt[b, e:e + 1, :]) & (r < vt[b, n_exp + e:n_exp + e + 1, :]), 1.0, 0.0).astype(BF16))
            pick[q, e * cap:(e + 1) * cap, :] = jnp.concatenate(out, axis=1)
        ft[...] = ft[...] + dot_nt(tab[q], pick[q])
        return carry

    lax.fori_loop(0, chips // 2, pick_block, 0)
    poll2(0, 2, 0)
    lax.fori_loop(chips // 2, chips, pick_block, 0)
    poll2(0, 2, 1)
    first_send(1, 1)

    r8 = lax.broadcasted_iota(jnp.int32, (top_k, rows), 1)
    hit = (ft[24:32, :] == ((r8 >> 3) - rows // 16).astype(F32)) & (ft[32:40, :] == (r8 & 7).astype(F32))
    val = ft[0:8, :] + ft[8:16, :] + ft[16:24, :]
    hitm[...] = jnp.where(hit, 1.0, 0.0)
    grow[...] = jnp.broadcast_to(jnp.sum(jnp.where(hit, val, 0.0), axis=0, keepdims=True), (8, rows))

    def gate_col(i, carry):
        sl = pl.ds(pl.multiple_of(i * tok, tok), tok)
        v = jnp.transpose(jnp.broadcast_to(grow[0:1, sl], (tok, tok)))
        gcol[sl, :] = v
        for s, w in enumerate(split3(v)):
            gpart[s, sl, :] = w.astype(BF16)
        return carry

    lax.fori_loop(0, rows // tok, gate_col, 0)

    def gather(a, ds, first=False):
        for d in ds:
            twin_wait(a, d)
        dst = brow if a == 0 else gy

        def body(e, carry):
            r = None
            for d in ds:
                q = chip(d)
                t = dot_nn(pick[q, esl(e), :], bufs[a][q])
                r = t if r is None else r + t
            r = r.astype(BF16)
            dst[esl(e), :] = r if first else dst[esl(e), :] + r
            return carry

        lax.fori_loop(0, n_exp, body, 0)

    gather(0, (0, 1, -1), True)
    poll2(0, 3, 0)
    gather(0, (2, -2))
    poll2(0, 3, 1)
    poll2(1, 1, 0)
    gather(0, (3, -3))
    poll2(0, 4, 0)
    poll2(0, 4, 1)
    poll2(1, 1, 1)
    poll2(1, 2, 0)
    gather(0, (4,))

    for cp in loads:
        cp.wait()

    def forward_pair(e0):
        def body(i, carry):
            e = e0 + i
            act, sl = gelu_and_slope(dot_nn(brow[esl(e), :], w1[e]))
            hb = act.astype(BF16)
            hid[esl(e), :] = hb
            slope[esl(e), :] = sl
            orow[esl(e), :] = dot_nn(hb, w2[e]).astype(BF16)
            return carry
        lax.fori_loop(0, 2, body, 0)

    forward_pair(0)
    poll2(1, 2, 1)
    forward_pair(2)

    order = [far]
    for d in range(far - 1, 0, -1):
        order += [d, -d]
    order.append(0)
    place = {d: i for i, d in enumerate(order)}
    place[-far] = 0
    own_wait, twin_wait_s = {}, {}
    n_cols = xs.shape[1]
    tile = xa.shape[1]
    step = 2 * tile
    blocks = rows // tok

    def mtile(m):
        return pl.ds(pl.multiple_of(m * step, step), step)

    def flip_rows(j, carry):
        js = pl.ds(pl.multiple_of(j * tok, tok), tok)
        for i in range(blocks):
            go[js, i * tok:(i + 1) * tok] = jnp.transpose(orow[i * tok:(i + 1) * tok, js])
        return carry

    def chunk(a, d):
        q, di = chip(d), place[d]
        sp = di % spare.shape[0]
        for cp in own_wait.pop(di, []):
            cp.wait_send()
        if sp in twin_wait_s:
            twin_wait_s.pop(sp).wait_send()

        per = tile // tok
        if a == 0:
            def scale(i, carry):
                sl = pl.ds(pl.multiple_of(i * tok, tok), tok)
                sub = pl.ds(pl.multiple_of((i % per) * tok, tok), tok)
                for s in range(3):
                    g = gpart[s, sl, :]
                    xa[i // per, sub, s * 2 * tok:(s + 1) * 2 * tok] = pick[q, sl, :] * jnp.concatenate([g, g], axis=1)
                return carry
            lax.fori_loop(0, blocks, scale, 0)

        def body(m, carry):
            ms = mtile(m)
            if a == 0:
                r = None
                for s in range(3):
                    w = xa[0:rows // tile, :, s * 2 * tok:(s + 1) * 2 * tok].reshape(rows, 2 * tok)
                    t = dot_nn(go[ms, :], w)
                    r = t if r is None else r + t
            else:
                r = dot_nn(go[ms, :], pick[q])
            r0, r1 = r[:, 0:tok], r[:, tok:2 * tok]
            part[di, ms, :] = jnp.where(c == 0, r0, r1)
            spare[sp, ms, :] = jnp.where(c == 0, r1, r0)
            return carry

        lax.fori_loop(0, n_cols // step, body, 0)
        twin_wait_s[sp] = send(spare.at[sp], sib.at[a, di], rsb_s.at[a, di], rsb_r.at[a, di], twin)
        if a == 1:
            t = dot_nn(mgt[...], pick[q])
            t = t[0:8] + t[8:16] + t[16:24]
            dgp[q] = jnp.where(c == 0, t[:, 0:tok], t[:, tok:2 * tok])
            dgt[q] = jnp.where(c == 0, t[:, tok:2 * tok], t[:, 0:tok])

    hd = n_cols // 2

    def mine(d, h):
        return part.at[place[d], pl.ds(h * hd, hd)]

    seen = set()

    def twin_part_wait(a, d):
        di = place[d]
        if (a, di) not in seen:
            seen.add((a, di))
            landed(sib.at[a, di], rsb_s.at[a, di], rsb_r.at[a, di], twin)

    def items(r):
        near, other = (0, 1) if r == 0 else (1, 0)
        out = [(far, near)]
        for d in range(far - 1, 0, -1):
            out += [(d, other), (d, near)]
        return out

    def ring_send(a, i, r):
        d, h = items(r)[i]
        sd = d if r == 0 else -d
        di = place[sd]
        twin_part_wait(a, sd)
        ref = mine(sd, h)
        total = ref[...] + sib[a, di, h * hd:(h + 1) * hd, :]
        if (d + 1, h) in items(r):
            p = items(r).index((d + 1, h))
            landed(ring.at[a, r, p], rs_s.at[a, r, p], rs_r.at[a, r, p], side[r])
            total = total + ring[a, r, p]
        ref[...] = total
        own_wait.setdefault(di, []).append(send(ref, ring.at[a, r, i], rs_s.at[a, r, i], rs_r.at[a, r, i], side[r]))

    def ring_send2(a, i):
        ring_send(a, i, 0)
        ring_send(a, i, 1)

    def finish(a, src, dst):
        twin_part_wait(a, 0)
        for h in range(2):
            total = mine(0, h)[...] + sib[a, place[0], h * hd:(h + 1) * hd, :]
            for r in range(2):
                p = items(r).index((1, h))
                landed(ring.at[a, r, p], rs_s.at[a, r, p], rs_r.at[a, r, p], side[r])
                total = total + ring[a, r, p]
            for j in range(hd // tok):
                cs = slice(h * hd + j * tok, h * hd + (j + 1) * tok)
                dst[:, cs] = (src[:, cs].astype(F32) + jnp.transpose(total[j * tok:(j + 1) * tok, :])).astype(BF16)

    def backward_pair(e0):
        def body(i, carry):
            e = e0 + i
            es = esl(e)
            dyr = gy[es, :].astype(F32)
            gc = gcol[es, :]
            dg = jnp.sum(dyr * orow[es, :].astype(F32), axis=1, keepdims=True)
            gcol[es, :] = jnp.broadcast_to(dg, (cap, tok))
            g = (jnp.concatenate([gc] * (n_cols // tok), axis=1) * dyr).astype(BF16)
            gy[es, :] = g
            dh = dot_nt(g, w2[e]).astype(BF16)
            da = (dh.astype(F32) * slope[es, :]).astype(BF16)
            dact[es, :] = da
            orow[es, :] = dot_nt(da, w1[e]).astype(BF16)
            return carry
        lax.fori_loop(0, 2, body, 0)

    def gate_cols(i, carry):
        sl = pl.ds(pl.multiple_of(i * tok, tok), tok)
        d = jnp.transpose(gcol[sl, :])[0:8, :]
        hi, mid, lo = split3(jnp.where(hitm[:, sl] > 0.0, d, 0.0))
        mgt[:, sl] = jnp.concatenate([hi, mid, lo, jnp.zeros_like(hi)], axis=0).astype(BF16)
        return carry

    ff = w1.shape[2]
    g1, g2 = n_cols // tile, ff // tile

    def weight_pair(e0):
        def body(i, carry):
            e = e0 + i
            es = esl(e)
            lo = pl.multiple_of(ff * (e % 2), ff)
            for s in range(g2):
                dya[g2 * e + s] = dot_tn(hid[es, s * tile:(s + 1) * tile], gy[es, :]).astype(BF16)
            for s in range(g1):
                xa[g1 * (e // 2) + s, :, pl.ds(lo, ff)] = dot_tn(brow[es, s * tile:(s + 1) * tile], dact[es, :]).astype(BF16)
            return carry
        lax.fori_loop(0, 2, body, 0)

    lax.fori_loop(0, n_cols // tok, flip_rows, 0)
    poll2(1, 3, 0)
    for cp in pending[0]:
        cp.wait_send()
    chunk(0, far)
    poll2(1, 3, 1)
    chunk(0, 3)
    ring_send2(0, 0)
    chunk(0, -3)
    ring_send(0, 1, 0)
    poll2(1, 4, 0)
    poll2(1, 4, 1)
    chunk(0, 2)
    ring_send(0, 1, 1)
    chunk(0, -2)
    ring_send(0, 2, 0)
    chunk(0, 1)
    ring_send(0, 2, 1)
    ring_send2(0, 3)
    chunk(0, -1)
    gather(1, (0, 1, -1, 2), True)
    ring_send2(0, 4)
    chunk(0, 0)
    gather(1, (-2, 3, -3, 4))
    ring_send2(0, 5)
    backward_pair(0)
    backward_pair(2)
    lax.fori_loop(0, blocks, gate_cols, 0)
    lax.fori_loop(0, n_cols // tok, flip_rows, 0)
    ring_send2(0, 6)
    chunk(1, far)
    chunk(1, 3)
    ring_send2(1, 0)
    chunk(1, -3)
    chunk(1, 2)
    ring_send2(1, 1)
    finish(0, xs, xs)
    chunk(1, -2)
    chunk(1, 1)
    ring_send2(1, 2)
    chunk(1, -1)
    chunk(1, 0)
    dg_cp = send(dgt, dgs, dgb_s.at[0], dgb_r.at[0], twin)
    ring_send2(1, 3)
    for cp in pending[1]:
        cp.wait_send()
    landed(dgs, dgb_s.at[0], dgb_r.at[0], twin)
    dgp[...] = dgp[...] + dgs[...]
    dg_sends = [send(dgp.at[chip(d)], dgr.at[z], dg_s.at[d], dg_r.at[d], dev(chip(d), c)) for d in range(1, chips)]
    weight_pair(0)
    ring_send2(1, 4)
    weight_pair(2)
    ring_send2(1, 5)
    dg_total = dgp[z]
    for d in range(1, chips):
        landed(dgr.at[chip(-d)], dg_s.at[d], dg_r.at[d], twin)
        dg_total = dg_total + dgr[chip(-d)]
    dgs[0] = dg_total
    ring_send2(1, 6)
    dg_cp.wait_send()
    for cp in dg_sends:
        cp.wait_send()
    finish(1, ys, ys)
    for group in (list(twin_wait_s.values()), *own_wait.values()):
        for cp in group:
            cp.wait_send()


def copy_kernel(xs, ys, dgs, xa, dya, y, dx, dg, dw1, dw2, sem):
    n_exp, n_cols, ff = dw1.shape
    tile = xa.shape[1]
    g1, g2 = n_cols // tile, ff // tile
    jobs = [(xs, y), (ys, dx), (dgs.at[0], dg)]
    for e in range(n_exp):
        lo = ff * (e % 2)
        jobs += [(dya.at[g2 * e + s], dw2.at[e, pl.ds(s * tile, tile)]) for s in range(g2)]
        jobs += [(xa.at[g1 * (e // 2) + s, :, pl.ds(lo, ff)], dw1.at[e, pl.ds(s * tile, tile)]) for s in range(g1)]
    copies = [pltpu.make_async_copy(a, b, sem.at[k]) for k, (a, b) in enumerate(jobs)]
    for cp in copies:
        cp.start()
    for cp in copies:
        cp.wait()


def solution(mesh):
    groups = mesh.shape['expert']
    tok_spec = P(('data', 'expert'), None)
    weight_spec = P('expert', None, None)
    grad_spec = P(('data', 'expert'), None, None)

    def device_pass(x_in, expert_idx, gate_weight, grad_y, w_in, w_out):
        tok, top_k = expert_idx.shape
        n_exp, dm, ff = w_in.shape
        n_pairs = tok * top_k
        cap = (CAP_NUM * n_pairs) // (CAP_DEN * n_exp)
        rows = n_exp * cap
        chips = groups // 2
        hbm = pl.BlockSpec(memory_space=pl.ANY)
        dma = pltpu.SemaphoreType.DMA
        shape = jax.ShapeDtypeStruct
        outs = (shape((tok, dm), BF16), shape((tok, dm), BF16), shape((top_k, tok), F32),
                shape((n_exp, dm, ff), BF16), shape((n_exp, ff, dm), BF16))
        vmem = pl.BlockSpec(memory_space=pltpu.VMEM)
        mids = (pltpu.VMEM((tok, dm), BF16), pltpu.VMEM((tok, dm), BF16), pltpu.VMEM((chips, top_k, tok), F32),
                pltpu.VMEM((chips, 2 * tok, dm), BF16), pltpu.VMEM((chips, 2 * tok, dm), BF16))
        held = pl.pallas_call(
            functools.partial(moe_kernel, chips, cap, n_exp),
            name='moe',
            out_shape=mids,
            in_specs=[hbm] * 6,
            out_specs=(vmem,) * 5,
            scratch_shapes=[
                pltpu.VMEM((2, chips, top_k, tok), jnp.int32),
                pltpu.VMEM((2, chips, top_k, tok), F32),
                pltpu.VMEM((2 * chips, 8, tok), F32),
                pltpu.VMEM((2 * chips, 8, tok), F32),
                pltpu.VMEM((chips, 48, 2 * tok), BF16),
                pltpu.VMEM((48, rows), F32),
                pltpu.VMEM((8, rows), F32),
                pltpu.VMEM((8, rows), F32),
                pltpu.VMEM((rows, tok), F32),
                pltpu.VMEM((3, rows, tok), BF16),
                pltpu.VMEM((rows, dm), BF16),
                pltpu.VMEM((rows, dm), BF16),
                pltpu.VMEM((rows, ff), BF16),
                pltpu.VMEM((rows, ff), F32),
                pltpu.VMEM((rows, dm), BF16),
                pltpu.VMEM((rows, ff), BF16),
                pltpu.VMEM((chips, rows, 2 * tok), BF16),
                pltpu.VMEM((dm, rows), BF16),
                pltpu.VMEM((chips, dm, tok), F32),
                pltpu.VMEM((4, dm, tok), F32),
                pltpu.VMEM((2, chips, dm, tok), F32),
                pltpu.VMEM((2, 2, chips - 1, dm // 2, tok), F32),
                pltpu.VMEM((32, rows), BF16),
                pltpu.VMEM((chips, 8, tok), F32),
                pltpu.VMEM((chips, 8, tok), F32),
                pltpu.VMEM((chips, 8, tok), F32),
                pltpu.VMEM((n_exp, dm, ff), BF16),
                pltpu.VMEM((n_exp, ff, dm), BF16),
                dma((2, 2, chips - 1)), dma((2, 2, chips - 1)),
                dma((2, chips, 2)), dma((2, chips, 2)),
                dma((2, chips)), dma((2, chips)), dma((2,)), dma((2,)),
                dma((2, 2, chips - 1)), dma((2, 2, chips - 1)),
                dma((2, chips)), dma((2, chips)),
                dma((chips,)), dma((chips,)), dma((1,)), dma((1,)),
                dma((6,)), dma((2, n_exp)),
            ],
            compiler_params=pltpu.CompilerParams(collective_id=0, has_side_effects=True,
                                                 vmem_limit_bytes=VMEM_BYTES),
        )(expert_idx.T, gate_weight.T, x_in, grad_y, w_in, w_out)
        y, dx, dg, dw1, dw2 = pl.pallas_call(
            copy_kernel,
            name='outputs',
            out_shape=outs,
            in_specs=[vmem] * len(mids),
            out_specs=(hbm,) * len(outs),
            scratch_shapes=[dma((3 + n_exp * (dm + ff) // (2 * tok),))],
            compiler_params=pltpu.CompilerParams(vmem_limit_bytes=1 << 20),
        )(*[pltpu.with_memory_space_constraint(v, pltpu.VMEM) for v in held])
        return y, dx, dg.T, dw1, dw2

    return jax.shard_map(device_pass, mesh=mesh,
                         in_specs=(tok_spec, tok_spec, tok_spec, tok_spec, weight_spec, weight_spec),
                         out_specs=(tok_spec, tok_spec, tok_spec, grad_spec, grad_spec), check_vma=False)
```

```python
import functools

import jax
import jax.numpy as jnp
from jax import lax
from jax.experimental import pallas as pl
from jax.experimental.pallas import tpu as pltpu
from jax.sharding import PartitionSpec as P

CAP_NUM = 5
CAP_DEN = 4
BIG = 3.3e38
F32 = jnp.float32
BF16 = jnp.bfloat16
K0 = 0.7978845608028654
K1 = 0.044715
MESH = pl.DeviceIdType.MESH
VMEM_BYTES = 57_900_000


def split3(v):
    hi = jnp.clip(v, -BIG, BIG).astype(BF16).astype(F32)
    rest = v - hi
    mid = rest.astype(BF16).astype(F32)
    lo = (rest - mid).astype(BF16).astype(F32)
    return hi, mid, lo


def gelu_and_slope(a):
    t = jnp.tanh(K0 * (a + K1 * (a * a * a)))
    cdf = 0.5 * (1.0 + t)
    return a * cdf, cdf + a * (0.5 * (1.0 - t * t)) * (K0 * (1.0 + 3.0 * K1 * (a * a)))


def dot_nn(a, b):
    return lax.dot_general(a, b, (((1,), (0,)), ((), ())), preferred_element_type=F32)


def dot_nt(a, b):
    return lax.dot_general(a, b, (((1,), (1,)), ((), ())), preferred_element_type=F32)


def dot_tn(a, b):
    return lax.dot_general(a, b, (((0,), (0,)), ((), ())), preferred_element_type=F32)


def moe_kernel(chips, cap, n_exp,
               idx_hbm, gate_hbm, x_hbm, dy_hbm, w1_hbm, w2_hbm,
               xs, ys, dgs, xa, dya,
               idx_all, gate_all, vt, cnt, tab, ft, hitm, grow, gcol, gpart, brow, gy, hid, slope, orow, dact,
               pick, go, part, spare, sib, ring, mgt, dgp, dgt, dgr, w1, w2,
               ag_s, ag_r, agb_s, agb_r, in_s, in_r, inb_s, inb_r, rs_s, rs_r, rsb_s, rsb_r,
               dg_s, dg_r, dgb_s, dgb_r, l_sem, w_sem):
    top_k, tok = idx_all.shape[2:]
    half = tok // 2
    rows = n_exp * cap
    me = lax.axis_index('expert')
    z = me // 2
    c = me % 2
    far = chips // 2

    def chip(d):
        return (z + d + chips) % chips

    def dev(q, k):
        return {'expert': q * 2 + k}

    right, left, twin = dev(chip(1), c), dev(chip(-1), c), {'expert': z * 2 + 1 - c}
    side = (right, left)
    pending = ([], [])
    def rcopy(src, dst, ss, rs, to):
        return pltpu.make_async_remote_copy(src_ref=src, dst_ref=dst, send_sem=ss, recv_sem=rs,
                                            device_id=to, device_id_type=MESH)

    def send(src, dst, ss, rs, to):
        cp = rcopy(src, dst, ss, rs, to)
        cp.start()
        return cp

    def landed(dst, ss, rs, to):
        rcopy(dst, dst, ss, rs, to).wait_recv()

    own_rows = pl.ds(pl.multiple_of(c * tok, tok), tok)
    inputs = []
    for k, (src, dst) in enumerate(((idx_hbm, idx_all.at[c, z]), (gate_hbm, gate_all.at[c, z]), (x_hbm, xs), (dy_hbm, ys),
                                    (x_hbm, xa.at[z, own_rows]), (dy_hbm, dya.at[z, own_rows]))):
        cp = pltpu.make_async_copy(src, dst, l_sem.at[k])
        cp.start()
        inputs.append(cp)

    barrier = pltpu.get_barrier_semaphore()
    for d in sorted(range(1, chips), key=lambda d: -min(d, chips - d)):
        pl.semaphore_signal(barrier, inc=1, device_id=dev(chip(d), c), device_id_type=MESH)
    pl.semaphore_signal(barrier, inc=1, device_id=twin, device_id_type=MESH)

    loads = []
    for e in range(n_exp):
        for k, (src, dst) in enumerate(((w1_hbm, w1), (w2_hbm, w2))):
            cp = pltpu.make_async_copy(src.at[e], dst.at[e], w_sem.at[k, e])
            cp.start()
            loads.append(cp)
    for cp in inputs:
        cp.wait()
    pl.semaphore_wait(barrier, chips)

    bufs = (xa, dya)
    own = (xs, ys)

    def item(k, h):
        return 2 * (k - 1) + h if k < far else 2 * (far - 1)

    def slot(a, q, h, k=None):
        kk = c if k is None else k
        return bufs[a].at[q, pl.ds(pl.multiple_of(kk * tok + h * half, half), half)]

    def twin_send(a, d, h, src):
        di = d % chips
        pending[a].append(send(src, slot(a, chip(d), h), agb_s.at[a, di, h], agb_r.at[a, di, h], twin))

    def twin_wait(a, d):
        di = d % chips
        for h in range(2):
            landed(slot(a, chip(d), h, 1 - c), agb_s.at[a, di, h], agb_r.at[a, di, h], twin)

    def first_send(a, h):
        for r, h in enumerate((h, 1 - h)):
            src = own[a].at[pl.ds(h * half, half)]
            i = item(1, h)
            pending[a].append(send(src, slot(a, z, h), ag_s.at[a, r, i], ag_r.at[a, r, i], side[r]))

    def poll(a, k, h, r):
        q = chip(-k) if r == 0 else chip(k)
        i = item(k, h)
        here = slot(a, q, h)
        landed(here, ag_s.at[a, r, i], ag_r.at[a, r, i], side[r])
        if k + 1 < far or (k + 1 == far and h == r):
            j = item(k + 1, h)
            pending[a].append(send(here, slot(a, q, h), ag_s.at[a, r, j], ag_r.at[a, r, j], side[r]))
        twin_send(a, (-k if r == 0 else k), h, here)

    def poll2(a, k, h):
        if k == far:
            poll(a, k, h, h)
        else:
            poll(a, k, h, 0)
            poll(a, k, 1 - h, 1)

    small = (idx_all, gate_all)
    for d in range(1, chips):
        for s, dst in enumerate(small):
            pending[1].append(send(dst.at[c, z], dst.at[c, z], in_s.at[s, d], in_r.at[s, d], dev(chip(d), c)))
    first_send(0, 0)
    first_send(0, 1)
    first_send(1, 0)
    for a in range(2):
        for h in range(2):
            twin_send(a, 0, h, own[a].at[pl.ds(h * half, half)])
    for s, dst in enumerate(small):
        for d in range(1, chips):
            landed(dst.at[c, chip(-d)], in_s.at[s, d], in_r.at[s, d], twin)
        pending[1].append(send(dst.at[c], dst.at[c], inb_s.at[s], inb_r.at[s], twin))
    poll2(0, 1, 0)
    for s, dst in enumerate(small):
        landed(dst.at[1 - c], inb_s.at[s], inb_r.at[s], twin)

    first_e = (me * n_exp).astype(F32)
    sub8 = lax.broadcasted_iota(jnp.int32, (8, tok), 0)

    def count_block(b, carry):
        k, q = b // chips, b % chips
        loc = idx_all[k, q].astype(F32) - first_e
        for e in range(n_exp):
            s = jnp.sum(jnp.where(loc == e, 1.0, 0.0), axis=0, keepdims=True)
            cnt[b, e:e + 1, :] = s
            cnt[b, n_exp + e:n_exp + e + 1, :] = s
        return carry

    lax.fori_loop(0, 2 * chips, count_block, 0)
    cmat = cnt[...].reshape(2 * chips * 8, tok)
    ri = lax.broadcasted_iota(jnp.int32, (tok, tok), 0)
    ci = lax.broadcasted_iota(jnp.int32, (tok, tok), 1)
    upper = jnp.where(ri < ci, 1.0, 0.0).astype(BF16)
    rb, cb = ri // 8, ci // 8
    r_ord, c_ord = 2 * (rb % chips) + rb // chips, 2 * (cb % chips) + cb // chips
    prior = jnp.where((c_ord < r_ord) & (ri % 8 == ci % 8), 1.0, 0.0).astype(BF16)
    cbf = cmat.astype(BF16)
    start = dot_nn(cbf, upper) + jnp.sum(dot_nn(prior, cbf), axis=1, keepdims=True)
    cnt[...] = start.reshape(2 * chips, 8, tok)
    row8 = ri % 8
    edge = jnp.where(row8 < n_exp, start, start + cmat)
    edge = jnp.minimum(edge, float(cap)) + (row8 % n_exp).astype(F32) * cap
    vt[...] = edge.reshape(2 * chips, 8, tok)
    poll2(0, 1, 1)

    def table_block(b, carry):
        k, q = b // chips, b % chips
        idx = idx_all[k, q].astype(F32)
        loc = idx - first_e
        at = jnp.zeros((top_k, tok), F32)
        for e in range(n_exp):
            at = at + jnp.where(loc == e, cnt[b, e:e + 1, :], 0.0)
        for j in range(top_k - 1):
            at = at + jnp.where((idx[j:j + 1, :] == idx) & (sub8 > j), 1.0, 0.0)
        ok = (loc >= 0.0) & (loc < n_exp) & (at < cap)
        rr = loc * cap + at
        coarse = jnp.floor(rr * 0.125)
        hi, mid, lo = split3(gate_all[k, q])
        code = jnp.where(ok, coarse - rows // 16, 200.0)
        fine = jnp.where(ok, rr - 8.0 * coarse, 0.0)
        tile = jnp.concatenate([hi, mid, lo, code, fine, jnp.zeros((8, tok), F32)], axis=0)
        tab[q, :, pl.ds(pl.multiple_of(k * tok, tok), tok)] = tile.astype(BF16)
        return carry

    lax.fori_loop(0, 2 * chips, table_block, 0)

    def esl(e):
        return pl.ds(pl.multiple_of(e * cap, cap), cap)

    ft[...] = jnp.zeros_like(ft)

    def pick_block(q, carry):
        for e in range(n_exp):
            r = (lax.broadcasted_iota(jnp.int32, (cap, tok), 0) + e * cap).astype(F32)
            out = []
            for k in range(2):
                b = k * chips + q
                out.append(jnp.where((r >= vt[b, e:e + 1, :]) & (r < vt[b, n_exp + e:n_exp + e + 1, :]), 1.0, 0.0).astype(BF16))
            pick[q, e * cap:(e + 1) * cap, :] = jnp.concatenate(out, axis=1)
        ft[...] = ft[...] + dot_nt(tab[q], pick[q])
        return carry

    lax.fori_loop(0, chips // 2, pick_block, 0)
    poll2(0, 2, 0)
    lax.fori_loop(chips // 2, chips, pick_block, 0)
    poll2(0, 2, 1)
    first_send(1, 1)

    r8 = lax.broadcasted_iota(jnp.int32, (top_k, rows), 1)
    hit = (ft[24:32, :] == ((r8 >> 3) - rows // 16).astype(F32)) & (ft[32:40, :] == (r8 & 7).astype(F32))
    val = ft[0:8, :] + ft[8:16, :] + ft[16:24, :]
    hitm[...] = jnp.where(hit, 1.0, 0.0)
    grow[...] = jnp.broadcast_to(jnp.sum(jnp.where(hit, val, 0.0), axis=0, keepdims=True), (8, rows))

    def gate_col(i, carry):
        sl = pl.ds(pl.multiple_of(i * tok, tok), tok)
        v = jnp.transpose(jnp.broadcast_to(grow[0:1, sl], (tok, tok)))
        gcol[sl, :] = v
        for s, w in enumerate(split3(v)):
            gpart[s, sl, :] = w.astype(BF16)
        return carry

    lax.fori_loop(0, rows // tok, gate_col, 0)

    def gather(a, ds, first=False):
        for d in ds:
            twin_wait(a, d)
        dst = brow if a == 0 else gy

        def body(e, carry):
            r = None
            for d in ds:
                q = chip(d)
                t = dot_nn(pick[q, esl(e), :], bufs[a][q])
                r = t if r is None else r + t
            r = r.astype(BF16)
            dst[esl(e), :] = r if first else dst[esl(e), :] + r
            return carry

        lax.fori_loop(0, n_exp, body, 0)

    gather(0, (0, 1, -1), True)
    poll2(0, 3, 0)
    gather(0, (2, -2))
    poll2(0, 3, 1)
    poll2(1, 1, 0)
    gather(0, (3, -3))
    poll2(0, 4, 0)
    poll2(0, 4, 1)
    poll2(1, 1, 1)
    poll2(1, 2, 0)
    gather(0, (4,))

    for cp in loads:
        cp.wait()

    def forward_pair(e0):
        def body(i, carry):
            e = e0 + i
            act, sl = gelu_and_slope(dot_nn(brow[esl(e), :], w1[e]))
            hb = act.astype(BF16)
            hid[esl(e), :] = hb
            slope[esl(e), :] = sl
            orow[esl(e), :] = dot_nn(hb, w2[e]).astype(BF16)
            return carry
        lax.fori_loop(0, 2, body, 0)

    forward_pair(0)
    poll2(1, 2, 1)
    forward_pair(2)

    order = [far]
    for d in range(far - 1, 0, -1):
        order += [d, -d]
    order.append(0)
    place = {d: i for i, d in enumerate(order)}
    place[-far] = 0
    own_wait, twin_wait_s = {}, {}
    n_cols = xs.shape[1]
    tile = xa.shape[1]
    step = 2 * tile
    blocks = rows // tok

    def mtile(m):
        return pl.ds(pl.multiple_of(m * step, step), step)

    def flip_rows(j, carry):
        js = pl.ds(pl.multiple_of(j * tok, tok), tok)
        for i in range(blocks):
            go[js, i * tok:(i + 1) * tok] = jnp.transpose(orow[i * tok:(i + 1) * tok, js])
        return carry

    def twin_copy(a, di, sp, m):
        ms = mtile(m)
        return rcopy(spare.at[sp, ms], sib.at[a, di, ms], rsb_s.at[a, di, m], rsb_r.at[a, di, m], twin)

    def chunk(a, d):
        q, di = chip(d), place[d]
        sp = di % spare.shape[0]
        for cp in own_wait.pop(di, []):
            cp.wait_send()
        if sp in twin_wait_s:
            for cp in twin_wait_s.pop(sp):
                cp.wait_send()

        per = tile // tok
        if a == 0:
            def scale(i, carry):
                sl = pl.ds(pl.multiple_of(i * tok, tok), tok)
                sub = pl.ds(pl.multiple_of((i % per) * tok, tok), tok)
                for s in range(3):
                    g = gpart[s, sl, :]
                    xa[i // per, sub, s * 2 * tok:(s + 1) * 2 * tok] = pick[q, sl, :] * jnp.concatenate([g, g], axis=1)
                return carry
            lax.fori_loop(0, blocks, scale, 0)

        def body(m, carry):
            ms = mtile(m)
            if a == 0:
                r = None
                for s in range(3):
                    w = xa[0:rows // tile, :, s * 2 * tok:(s + 1) * 2 * tok].reshape(rows, 2 * tok)
                    t = dot_nn(go[ms, :], w)
                    r = t if r is None else r + t
            else:
                r = dot_nn(go[ms, :], pick[q])
            r0, r1 = r[:, 0:tok], r[:, tok:2 * tok]
            part[di, ms, :] = jnp.where(c == 0, r0, r1)
            spare[sp, ms, :] = jnp.where(c == 0, r1, r0)
            twin_copy(a, di, sp, m).start()
            return carry

        lax.fori_loop(0, n_cols // step, body, 0)
        twin_wait_s[sp] = [twin_copy(a, di, sp, m) for m in range(n_cols // step)]
        if a == 1:
            t = dot_nn(mgt[...], pick[q])
            t = t[0:8] + t[8:16] + t[16:24]
            dgp[q] = jnp.where(c == 0, t[:, 0:tok], t[:, tok:2 * tok])
            dgt[q] = jnp.where(c == 0, t[:, tok:2 * tok], t[:, 0:tok])

    hd = n_cols // 2

    def mine(d, h):
        return part.at[place[d], pl.ds(h * hd, hd)]

    seen = set()

    def twin_part_wait(a, d, h):
        di = place[d]
        if (a, di, h) not in seen:
            seen.add((a, di, h))
            landed(sib.at[a, di, pl.ds(h * hd, hd)], rsb_s.at[a, di, h], rsb_r.at[a, di, h], twin)

    def items(r):
        near, other = (0, 1) if r == 0 else (1, 0)
        out = [(far, near)]
        for d in range(far - 1, 0, -1):
            out += [(d, other), (d, near)]
        return out

    def ring_send(a, i, r):
        d, h = items(r)[i]
        sd = d if r == 0 else -d
        di = place[sd]
        twin_part_wait(a, sd, h)
        ref = mine(sd, h)
        total = ref[...] + sib[a, di, h * hd:(h + 1) * hd, :]
        if (d + 1, h) in items(r):
            p = items(r).index((d + 1, h))
            landed(ring.at[a, r, p], rs_s.at[a, r, p], rs_r.at[a, r, p], side[r])
            total = total + ring[a, r, p]
        ref[...] = total
        own_wait.setdefault(di, []).append(send(ref, ring.at[a, r, i], rs_s.at[a, r, i], rs_r.at[a, r, i], side[r]))

    def ring_send2(a, i):
        ring_send(a, i, 0)
        ring_send(a, i, 1)

    def finish(a, src, dst):
        for h in range(2):
            twin_part_wait(a, 0, h)
            total = mine(0, h)[...] + sib[a, place[0], h * hd:(h + 1) * hd, :]
            for r in range(2):
                p = items(r).index((1, h))
                landed(ring.at[a, r, p], rs_s.at[a, r, p], rs_r.at[a, r, p], side[r])
                total = total + ring[a, r, p]
            for j in range(hd // tok):
                cs = slice(h * hd + j * tok, h * hd + (j + 1) * tok)
                dst[:, cs] = (src[:, cs].astype(F32) + jnp.transpose(total[j * tok:(j + 1) * tok, :])).astype(BF16)

    def backward_pair(e0):
        def body(i, carry):
            e = e0 + i
            es = esl(e)
            dyr = gy[es, :].astype(F32)
            gc = gcol[es, :]
            dg = jnp.sum(dyr * orow[es, :].astype(F32), axis=1, keepdims=True)
            gcol[es, :] = jnp.broadcast_to(dg, (cap, tok))
            g = (jnp.concatenate([gc] * (n_cols // tok), axis=1) * dyr).astype(BF16)
            gy[es, :] = g
            dh = dot_nt(g, w2[e]).astype(BF16)
            da = (dh.astype(F32) * slope[es, :]).astype(BF16)
            dact[es, :] = da
            orow[es, :] = dot_nt(da, w1[e]).astype(BF16)
            return carry
        lax.fori_loop(0, 2, body, 0)

    def gate_cols(i, carry):
        sl = pl.ds(pl.multiple_of(i * tok, tok), tok)
        d = jnp.transpose(gcol[sl, :])[0:8, :]
        hi, mid, lo = split3(jnp.where(hitm[:, sl] > 0.0, d, 0.0))
        mgt[:, sl] = jnp.concatenate([hi, mid, lo, jnp.zeros_like(hi)], axis=0).astype(BF16)
        return carry

    ff = w1.shape[2]
    g1, g2 = n_cols // tile, ff // tile

    def weight_pair(e0):
        def body(i, carry):
            e = e0 + i
            es = esl(e)
            lo = pl.multiple_of(ff * (e % 2), ff)
            for s in range(g2):
                dya[g2 * e + s] = dot_tn(hid[es, s * tile:(s + 1) * tile], gy[es, :]).astype(BF16)
            for s in range(g1):
                xa[g1 * (e // 2) + s, :, pl.ds(lo, ff)] = dot_tn(brow[es, s * tile:(s + 1) * tile], dact[es, :]).astype(BF16)
            return carry
        lax.fori_loop(0, 2, body, 0)

    lax.fori_loop(0, n_cols // tok, flip_rows, 0)
    poll2(1, 3, 0)
    for cp in pending[0]:
        cp.wait_send()
    chunk(0, far)
    poll2(1, 3, 1)
    chunk(0, 3)
    ring_send2(0, 0)
    chunk(0, -3)
    ring_send(0, 1, 0)
    poll2(1, 4, 0)
    poll2(1, 4, 1)
    chunk(0, 2)
    ring_send(0, 1, 1)
    chunk(0, -2)
    ring_send(0, 2, 0)
    chunk(0, 1)
    ring_send(0, 2, 1)
    ring_send2(0, 3)
    chunk(0, -1)
    gather(1, (0, 1, -1, 2), True)
    ring_send2(0, 4)
    chunk(0, 0)
    gather(1, (-2, 3, -3, 4))
    ring_send2(0, 5)
    backward_pair(0)
    backward_pair(2)
    lax.fori_loop(0, blocks, gate_cols, 0)
    lax.fori_loop(0, n_cols // tok, flip_rows, 0)
    ring_send2(0, 6)
    chunk(1, far)
    chunk(1, 3)
    ring_send2(1, 0)
    chunk(1, -3)
    chunk(1, 2)
    ring_send2(1, 1)
    finish(0, xs, xs)
    chunk(1, -2)
    chunk(1, 1)
    ring_send2(1, 2)
    chunk(1, -1)
    chunk(1, 0)
    dg_cp = send(dgt, dgs, dgb_s.at[0], dgb_r.at[0], twin)
    ring_send2(1, 3)
    for cp in pending[1]:
        cp.wait_send()
    landed(dgs, dgb_s.at[0], dgb_r.at[0], twin)
    dgp[...] = dgp[...] + dgs[...]
    dg_sends = [send(dgp.at[chip(d)], dgr.at[z], dg_s.at[d], dg_r.at[d], dev(chip(d), c)) for d in range(1, chips)]
    weight_pair(0)
    ring_send2(1, 4)
    weight_pair(2)
    ring_send2(1, 5)
    dg_total = dgp[z]
    for d in range(1, chips):
        landed(dgr.at[chip(-d)], dg_s.at[d], dg_r.at[d], twin)
        dg_total = dg_total + dgr[chip(-d)]
    dgs[0] = dg_total
    ring_send2(1, 6)
    dg_cp.wait_send()
    for cp in dg_sends:
        cp.wait_send()
    finish(1, ys, ys)
    for group in (*twin_wait_s.values(), *own_wait.values()):
        for cp in group:
            cp.wait_send()


def copy_kernel(xs, ys, dgs, xa, dya, y, dx, dg, dw1, dw2, sem):
    n_exp, n_cols, ff = dw1.shape
    tile = xa.shape[1]
    g1, g2 = n_cols // tile, ff // tile
    jobs = [(xs, y), (ys, dx), (dgs.at[0], dg)]
    for e in range(n_exp):
        lo = ff * (e % 2)
        jobs += [(dya.at[g2 * e + s], dw2.at[e, pl.ds(s * tile, tile)]) for s in range(g2)]
        jobs += [(xa.at[g1 * (e // 2) + s, :, pl.ds(lo, ff)], dw1.at[e, pl.ds(s * tile, tile)]) for s in range(g1)]
    copies = [pltpu.make_async_copy(a, b, sem.at[k]) for k, (a, b) in enumerate(jobs)]
    for cp in copies:
        cp.start()
    for cp in copies:
        cp.wait()


def solution(mesh):
    groups = mesh.shape['expert']
    tok_spec = P(('data', 'expert'), None)
    weight_spec = P('expert', None, None)
    grad_spec = P(('data', 'expert'), None, None)

    def device_pass(x_in, expert_idx, gate_weight, grad_y, w_in, w_out):
        tok, top_k = expert_idx.shape
        n_exp, dm, ff = w_in.shape
        n_pairs = tok * top_k
        cap = (CAP_NUM * n_pairs) // (CAP_DEN * n_exp)
        rows = n_exp * cap
        chips = groups // 2
        hbm = pl.BlockSpec(memory_space=pl.ANY)
        dma = pltpu.SemaphoreType.DMA
        shape = jax.ShapeDtypeStruct
        outs = (shape((tok, dm), BF16), shape((tok, dm), BF16), shape((top_k, tok), F32),
                shape((n_exp, dm, ff), BF16), shape((n_exp, ff, dm), BF16))
        vmem = pl.BlockSpec(memory_space=pltpu.VMEM)
        mids = (pltpu.VMEM((tok, dm), BF16), pltpu.VMEM((tok, dm), BF16), pltpu.VMEM((chips, top_k, tok), F32),
                pltpu.VMEM((chips, 2 * tok, dm), BF16), pltpu.VMEM((chips, 2 * tok, dm), BF16))
        held = pl.pallas_call(
            functools.partial(moe_kernel, chips, cap, n_exp),
            name='moe',
            out_shape=mids,
            in_specs=[hbm] * 6,
            out_specs=(vmem,) * 5,
            scratch_shapes=[
                pltpu.VMEM((2, chips, top_k, tok), jnp.int32),
                pltpu.VMEM((2, chips, top_k, tok), F32),
                pltpu.VMEM((2 * chips, 8, tok), F32),
                pltpu.VMEM((2 * chips, 8, tok), F32),
                pltpu.VMEM((chips, 48, 2 * tok), BF16),
                pltpu.VMEM((48, rows), F32),
                pltpu.VMEM((8, rows), F32),
                pltpu.VMEM((8, rows), F32),
                pltpu.VMEM((rows, tok), F32),
                pltpu.VMEM((3, rows, tok), BF16),
                pltpu.VMEM((rows, dm), BF16),
                pltpu.VMEM((rows, dm), BF16),
                pltpu.VMEM((rows, ff), BF16),
                pltpu.VMEM((rows, ff), F32),
                pltpu.VMEM((rows, dm), BF16),
                pltpu.VMEM((rows, ff), BF16),
                pltpu.VMEM((chips, rows, 2 * tok), BF16),
                pltpu.VMEM((dm, rows), BF16),
                pltpu.VMEM((chips, dm, tok), F32),
                pltpu.VMEM((4, dm, tok), F32),
                pltpu.VMEM((2, chips, dm, tok), F32),
                pltpu.VMEM((2, 2, chips - 1, dm // 2, tok), F32),
                pltpu.VMEM((32, rows), BF16),
                pltpu.VMEM((chips, 8, tok), F32),
                pltpu.VMEM((chips, 8, tok), F32),
                pltpu.VMEM((chips, 8, tok), F32),
                pltpu.VMEM((n_exp, dm, ff), BF16),
                pltpu.VMEM((n_exp, ff, dm), BF16),
                dma((2, 2, chips - 1)), dma((2, 2, chips - 1)),
                dma((2, chips, 2)), dma((2, chips, 2)),
                dma((2, chips)), dma((2, chips)), dma((2,)), dma((2,)),
                dma((2, 2, chips - 1)), dma((2, 2, chips - 1)),
                dma((2, chips, 2)), dma((2, chips, 2)),
                dma((chips,)), dma((chips,)), dma((1,)), dma((1,)),
                dma((6,)), dma((2, n_exp)),
            ],
            compiler_params=pltpu.CompilerParams(collective_id=0, has_side_effects=True,
                                                 vmem_limit_bytes=VMEM_BYTES),
        )(expert_idx.T, gate_weight.T, x_in, grad_y, w_in, w_out)
        y, dx, dg, dw1, dw2 = pl.pallas_call(
            copy_kernel,
            name='outputs',
            out_shape=outs,
            in_specs=[vmem] * len(mids),
            out_specs=(hbm,) * len(outs),
            scratch_shapes=[dma((3 + n_exp * (dm + ff) // (2 * tok),))],
            compiler_params=pltpu.CompilerParams(vmem_limit_bytes=1 << 20),
        )(*[pltpu.with_memory_space_constraint(v, pltpu.VMEM) for v in held])
        return y, dx, dg.T, dw1, dw2

    return jax.shard_map(device_pass, mesh=mesh,
                         in_specs=(tok_spec, tok_spec, tok_spec, tok_spec, weight_spec, weight_spec),
                         out_specs=(tok_spec, tok_spec, tok_spec, grad_spec, grad_spec), check_vma=False)
```
